16 devices in a mesh: ep: 16 (over z, y, x, core).
Axes of the slice: x: 2, y: 2, z: 2, core: 2. Of those that a mesh axis runs over, the one named last changes fastest.
Arguments:
- hidden: bfloat16 [32768, 768], P('ep')
- w_router: float32 [768, 32], replicated
- expert_ids: int32 [32768, 2], P('ep')
- w_one: bfloat16 [32, 768, 3072], P('ep')
- w_three: bfloat16 [32, 768, 3072], P('ep')
- w_two: bfloat16 [32, 3072, 768], P('ep')
Outputs:
- output: bfloat16 [32768, 768], P('ep')
All inputs are finite; a program needn't handle non-finite values.
Results may differ from the reference program's by a relative error of at most 0.0086898.
Values are sent between devices in bfloat16 or wider.
A program may use at most 1 GiB of HBM per device.

```python
import jax
import jax.numpy as jnp
from jax import lax

TOK_DEV = 2048
GROUP = 16
D = 768
FF = 3072
EXPERTS = 32
ROW_BLOCK = 32


def route_ids(key):
    key_hot, key_src = jax.random.split(key)
    dev_order = jax.random.permutation(key_hot, GROUP)
    n_hot = GROUP // 4
    n_cold = GROUP - n_hot
    row_cap = 4 * TOK_DEV // GROUP
    per_dev = EXPERTS // GROUP
    hot_devs = dev_order[:n_hot]
    cold_devs = dev_order[n_hot:]
    slot_idx = jnp.arange(TOK_DEV)

    def one_source(src_key):
        key_shift, key_first, key_second, key_flip, key_perm = jax.random.split(src_key, 5)
        shift_val = jax.random.randint(key_shift, (), 0, n_cold)
        first_dev = hot_devs[slot_idx // row_cap]
        second_dev = cold_devs[(slot_idx + shift_val) % n_cold]
        first_exp = first_dev * per_dev + jax.random.randint(key_first, (TOK_DEV,), 0, per_dev)
        second_exp = second_dev * per_dev + jax.random.randint(key_second, (TOK_DEV,), 0, per_dev)
        pair_ids = jnp.stack([first_exp, second_exp], axis=1)
        flip_bit = jax.random.randint(key_flip, (TOK_DEV, 1), 0, 2)
        pair_ids = jnp.where(flip_bit == 1, pair_ids[:, ::-1], pair_ids)
        token_perm = jax.random.permutation(key_perm, TOK_DEV)
        return pair_ids[token_perm]

    src_keys = jax.random.split(key_src, GROUP)
    return jax.vmap(one_source)(src_keys).reshape(GROUP * TOK_DEV, 2).astype(jnp.int32)


def setup_inputs(seed: int = 0) -> dict:
    key = jax.random.key(seed)
    key_hidden, key_router, key_ids, key_one, key_three, key_two = jax.random.split(key, 6)
    tok_count = GROUP * TOK_DEV
    hidden = jax.random.normal(key_hidden, (tok_count, D), jnp.float32).astype(jnp.bfloat16)
    w_router = jax.random.normal(key_router, (D, EXPERTS), jnp.float32) * D ** -0.5
    expert_ids = route_ids(key_ids)
    w_one = (jax.random.normal(key_one, (EXPERTS, D, FF), jnp.float32) * D ** -0.5).astype(jnp.bfloat16)
    w_three = (jax.random.normal(key_three, (EXPERTS, D, FF), jnp.float32) * D ** -0.5).astype(jnp.bfloat16)
    w_two = (jax.random.normal(key_two, (EXPERTS, FF, D), jnp.float32) * FF ** -0.5).astype(jnp.bfloat16)
    return {"hidden": hidden, "w_router": w_router, "expert_ids": expert_ids, "w_one": w_one, "w_three": w_three, "w_two": w_two}


def reference(hidden, w_router, expert_ids, w_one, w_three, w_two):
    tok_count = hidden.shape[0]
    model_dim = hidden.shape[1]
    logits = jnp.dot(hidden.astype(jnp.float32), w_router, preferred_element_type=jnp.float32)
    prob_vals = jax.nn.softmax(logits, axis=-1)
    picked = jnp.take_along_axis(prob_vals, expert_ids, axis=1)
    gate_vals = picked / jnp.sum(picked, axis=1, keepdims=True)
    flat_ids = expert_ids.reshape(-1)
    assign_count = flat_ids.shape[0]
    sort_order = jnp.argsort(flat_ids, stable=True)
    sorted_ids = flat_ids[sort_order]
    counts = jnp.zeros((EXPERTS,), jnp.int32).at[flat_ids].add(1)
    padded = (counts + ROW_BLOCK - 1) // ROW_BLOCK * ROW_BLOCK
    pad_end = jnp.cumsum(padded)
    pad_start = pad_end - padded
    first_row = jnp.cumsum(counts) - counts
    rank_in = jnp.arange(assign_count) - first_row[sorted_ids]
    dest_row = pad_start[sorted_ids] + rank_in
    row_total = assign_count + EXPERTS * ROW_BLOCK
    block_count = row_total // ROW_BLOCK
    row_tok = jnp.zeros((row_total,), jnp.int32).at[dest_row].set((sort_order // 2).astype(jnp.int32))
    block_start = jnp.arange(block_count) * ROW_BLOCK
    block_exp = jnp.minimum(jnp.sum((block_start[:, None] >= pad_end[None, :]).astype(jnp.int32), axis=1), EXPERTS - 1)
    hidden_blocks = hidden[row_tok].reshape(block_count, ROW_BLOCK, model_dim)

    def block_ffn(block_args):
        hid_blk, exp_idx = block_args
        h_one = jnp.dot(hid_blk, w_one[exp_idx], preferred_element_type=jnp.float32)
        h_three = jnp.dot(hid_blk, w_three[exp_idx], preferred_element_type=jnp.float32)
        act_rows = (jax.nn.silu(h_one) * h_three).astype(jnp.bfloat16)
        return jnp.dot(act_rows, w_two[exp_idx], preferred_element_type=jnp.float32).astype(jnp.bfloat16)

    out_blocks = lax.map(block_ffn, (hidden_blocks, block_exp))
    out_rows = out_blocks.reshape(row_total, model_dim)
    sorted_out = out_rows[dest_row]
    assign_out = jnp.zeros((assign_count, model_dim), jnp.bfloat16).at[sort_order].set(sorted_out)
    both_out = assign_out.reshape(tok_count, 2, model_dim).astype(jnp.float32)
    out_sum = jnp.sum(gate_vals[:, :, None] * both_out, axis=1)
    return out_sum.astype(jnp.bfloat16)
```

```python
import functools

import jax
import jax.numpy as jnp
from jax import lax
from jax.experimental import pallas as pl
from jax.experimental.pallas import tpu as pltpu
from jax.sharding import PartitionSpec as P

F32 = jnp.float32
BF16 = jnp.bfloat16
I32 = jnp.int32
TILE = 32
CHUNKS = ((0, 128), (128, 128), (256, 128), (384, 128))
VMEM_BYTES = 60 * 1024 * 1024


def _dot(a, b):
    return jnp.dot(a, b, preferred_element_type=F32)


def route_kernel(local_count, row_cap, x_ref, wr_ref, ids_ref, slot_ref, cols_ref, cnt_ref):
    tok = x_ref.shape[0]
    n_exp = wr_ref.shape[0]
    w = wr_ref[...]
    w_hi = w.astype(BF16)
    rest = w - w_hi.astype(F32)
    w_mid = rest.astype(BF16)
    w_lo = (rest - w_mid.astype(F32)).astype(BF16)
    x = x_ref[...]
    nt = (((1,), (1,)), ((), ()))
    w_all = jnp.concatenate([w_hi, w_mid, w_lo], axis=0)
    parts = lax.dot_general(w_all, x, nt, preferred_element_type=F32)
    logits = parts[:n_exp] + (parts[n_exp : 2 * n_exp] + parts[2 * n_exp :])
    ids = ids_ref[...]
    id_a, id_b = ids[0:1], ids[1:2]
    row = lax.broadcasted_iota(I32, (n_exp, tok), 0)
    oh_a, oh_b = row == id_a, row == id_b
    zero = jnp.zeros((), F32)
    l_a = jnp.sum(jnp.where(oh_a, logits, zero), axis=0, keepdims=True)
    l_b = jnp.sum(jnp.where(oh_b, logits, zero), axis=0, keepdims=True)
    top = jnp.maximum(l_a, l_b)
    e_a, e_b = jnp.exp(l_a - top), jnp.exp(l_b - top)
    g_a, g_b = e_a / (e_a + e_b), e_b / (e_a + e_b)
    chosen = jnp.where(oh_a | oh_b, 1.0, 0.0).astype(F32)
    width = 256
    tri = (lax.broadcasted_iota(I32, (width, width), 0) < lax.broadcasted_iota(I32, (width, width), 1))
    tri = jnp.where(tri, 1.0, 0.0).astype(BF16)
    before = jnp.zeros((n_exp, 1), F32)
    ranks = []
    for k in range(tok // width):
        blk = chosen[:, k * width : (k + 1) * width]
        ranks.append(_dot(blk.astype(BF16), tri) + before)
        before = before + jnp.sum(blk, axis=1, keepdims=True)
    rank = jnp.concatenate(ranks, axis=1)
    cnt_ref[...] = jnp.broadcast_to(before, cnt_ref.shape).astype(I32)

    def slot_of(ident, onehot):
        here = jnp.sum(jnp.where(onehot, rank, zero), axis=0, keepdims=True)
        dev = ident // local_count
        lower = (row < ident) & (row >= dev * local_count)
        base = jnp.sum(jnp.where(lower, jnp.broadcast_to(before, (n_exp, tok)), zero), axis=0, keepdims=True)
        return dev.astype(F32) * row_cap + here + base

    s_a, s_b = slot_of(id_a, oh_a), slot_of(id_b, oh_b)
    both = jnp.concatenate([s_a, s_b, g_a, g_b, s_a, s_b, g_a, g_b], axis=0)
    slot_ref[...] = both.astype(I32)
    cols_ref[...] = both.T


def pack_kernel(row_cap, start, size, group, slot_ref, x_ref, out_ref):
    first_dev = pl.program_id(0) * group
    tok = x_ref.shape[0]
    rows = group * size
    r = lax.broadcasted_iota(I32, (rows, tok), 0)
    want = (first_dev + r // size) * row_cap + start + r % size
    hit = (want == slot_ref[0:1, :]) | (want == slot_ref[1:2, :])
    pick = jnp.where(hit, 1.0, 0.0).astype(BF16)
    out_ref[...] = _dot(pick, x_ref[...]).astype(BF16).reshape(out_ref.shape)


def ffn_kernel(start, size, n_src, bound_ref, x_ref, w1_ref, w3_ref, w2_ref, out_ref, xbuf, hbuf, ybuf, list_ref):
    e = pl.program_id(0)
    step = 256
    per = size // TILE

    @pl.when(e == 0)
    def _():
        out_ref[...] = jnp.zeros_like(out_ref)

    def collect(i, cnt):
        s = i // per
        t0 = start + (i % per) * TILE
        lo = bound_ref[e, s]
        hi = bound_ref[e + 1, s]
        hit = (lo < t0 + TILE) & (hi > t0)

        @pl.when(hit)
        def _():
            list_ref[cnt] = i
            xbuf[pl.ds(pl.multiple_of(cnt * TILE, TILE), TILE), :] = x_ref[pl.ds(pl.multiple_of(i * TILE, TILE), TILE), :]

        return cnt + hit.astype(I32)

    cnt = lax.fori_loop(0, n_src * per, collect, jnp.int32(0))
    ff = w1_ref.shape[1]
    wide = 512

    def block(g, _):
        r0 = pl.multiple_of(g * step, step)
        xb = xbuf[pl.ds(r0, step), :]
        for f in range(0, ff, wide):
            u = _dot(xb, w1_ref[:, f : f + wide])
            v = _dot(xb, w3_ref[:, f : f + wide])
            hbuf[:, f : f + wide] = (u * jax.nn.sigmoid(u) * v).astype(BF16)
        ybuf[pl.ds(r0, step), :] = _dot(hbuf[...], w2_ref[...]).astype(BF16)
        return 0

    lax.fori_loop(0, (cnt * TILE + step - 1) // step, block, 0)

    def put(k, _):
        i = list_ref[k]
        s = i // per
        t0 = start + (i % per) * TILE
        pos = t0 + lax.broadcasted_iota(I32, (TILE, 1), 0)
        own = (pos >= bound_ref[e, s]) & (pos < bound_ref[e + 1, s])
        at = pl.ds(pl.multiple_of(i * TILE, TILE), TILE)
        y = ybuf[pl.ds(pl.multiple_of(k * TILE, TILE), TILE), :]
        out_ref[at, :] = jnp.where(own, y, out_ref[at, :])
        return 0

    lax.fori_loop(0, cnt, put, 0)


def combine_kernel(row_cap, start, size, has_acc, last, *refs):
    if has_acc:
        cols_ref, back_ref, acc_ref, out_ref = refs
    else:
        cols_ref, back_ref, out_ref = refs
    rows = back_ref.shape[0]
    toks = cols_ref.shape[0]
    r = lax.broadcasted_iota(I32, (toks, rows), 1)
    slot = (r // size) * row_cap + start + r % size
    c = cols_ref[...]
    total = acc_ref[...] if has_acc else 0.0
    for k in range(2):
        pick = jnp.where(slot == c[:, k : k + 1].astype(I32), 1.0, 0.0).astype(BF16)
        total = total + c[:, 2 + k : 3 + k] * _dot(pick, back_ref[...])
    out_ref[...] = total.astype(out_ref.dtype)


def _params(**kw):
    return pltpu.CompilerParams(vmem_limit_bytes=VMEM_BYTES, **kw)


def solution(mesh):
    n = mesh.shape["ep"]

    def body(x, w_router, ids, w1, w3, w2):
        tok, dim = x.shape
        local = w1.shape[0]
        ff = w1.shape[2]
        n_exp = n * local
        cap = 4 * tok // n
        slots, cols, counts = pl.pallas_call(
            functools.partial(route_kernel, local, cap),
            out_shape=(
                jax.ShapeDtypeStruct((8, tok), I32),
                jax.ShapeDtypeStruct((tok, 8), F32),
                jax.ShapeDtypeStruct((n_exp, 128), I32),
            ),
            compiler_params=_params(),
            name="route",
        )(x, w_router.T, ids.T)
        per_exp = lax.all_to_all(counts[:, 0].reshape(n, local), "ep", 0, 0, tiled=True)
        ends = jnp.cumsum(per_exp, axis=1).T
        bounds = jnp.concatenate([jnp.zeros((1, n), I32), ends], axis=0)
        acc = None
        for index, (start, size) in enumerate(CHUNKS):
            group = 4
            send = pl.pallas_call(
                functools.partial(pack_kernel, cap, start, size, group),
                grid=(n // group,),
                in_specs=[pl.BlockSpec((8, tok), lambda i: (0, 0)), pl.BlockSpec((tok, dim), lambda i: (0, 0))],
                out_specs=pl.BlockSpec((group, size, dim), lambda i: (i, 0, 0)),
                out_shape=jax.ShapeDtypeStruct((n, size, dim), BF16),
                compiler_params=_params(),
                cost_estimate=pl.CostEstimate(flops=2 * n * size * tok * dim, bytes_accessed=1, transcendentals=0),
                name=f"pack{index}",
            )(slots, x)
            got = lax.all_to_all(send, "ep", 0, 0, tiled=True)
            rows = n * size
            made = pl.pallas_call(
                functools.partial(ffn_kernel, start, size, n),
                grid_spec=pltpu.PrefetchScalarGridSpec(
                    num_scalar_prefetch=1,
                    grid=(local,),
                    in_specs=[
                        pl.BlockSpec((rows, dim), lambda e, b: (0, 0)),
                        pl.BlockSpec((None, dim, ff), lambda e, b: (e, 0, 0)),
                        pl.BlockSpec((None, dim, ff), lambda e, b: (e, 0, 0)),
                        pl.BlockSpec((None, ff, dim), lambda e, b: (e, 0, 0)),
                    ],
                    out_specs=pl.BlockSpec((rows, dim), lambda e, b: (0, 0)),
                    scratch_shapes=[
                        pltpu.VMEM((rows, dim), BF16),
                        pltpu.VMEM((256, ff), BF16),
                        pltpu.VMEM((rows, dim), BF16),
                        pltpu.SMEM((rows // TILE,), I32),
                    ],
                ),
                out_shape=jax.ShapeDtypeStruct((rows, dim), BF16),
                compiler_params=_params(),
                cost_estimate=pl.CostEstimate(flops=6 * rows * dim * ff, bytes_accessed=1, transcendentals=0),
                name=f"ffn{index}",
            )(bounds, got.reshape(rows, dim), w1, w3, w2)
            back = lax.all_to_all(made.reshape(n, size, dim), "ep", 0, 0, tiled=True).reshape(rows, dim)
            last = index == len(CHUNKS) - 1
            tb = 512
            tile_spec = pl.BlockSpec((tb, dim), lambda i: (i, 0))
            ins = [cols, back] + ([] if acc is None else [acc])
            specs = [pl.BlockSpec((tb, 8), lambda i: (i, 0)), pl.BlockSpec((rows, dim), lambda i: (0, 0))]
            acc = pl.pallas_call(
                functools.partial(combine_kernel, cap, start, size, acc is not None, last),
                grid=(tok // tb,),
                in_specs=specs + ([] if acc is None else [tile_spec]),
                out_specs=tile_spec,
                out_shape=jax.ShapeDtypeStruct((tok, dim), BF16 if last else F32),
                compiler_params=_params(),
                cost_estimate=pl.CostEstimate(flops=4 * rows * tok * dim, bytes_accessed=1, transcendentals=0),
                name=f"combine{index}",
            )(*ins)
        return acc

    return jax.shard_map(
        body,
        mesh=mesh,
        in_specs=(P("ep", None), P(None, None), P("ep", None), P("ep", None, None), P("ep", None, None), P("ep", None, None)),
        out_specs=P("ep", None),
        check_vma=False,
    )
```

```python
import functools

import jax
import jax.numpy as jnp
from jax import lax
from jax.experimental import pallas as pl
from jax.experimental.pallas import tpu as pltpu
from jax.sharding import PartitionSpec as P


F32 = jnp.float32
BF16 = jnp.bfloat16
I32 = jnp.int32
TILE = 16
CHUNKS = ((0, 176), (176, 176), (352, 160))
VMEM_BYTES = 60 * 1024 * 1024


def _dot(a, b):
    return jnp.dot(a, b, preferred_element_type=F32)


def route_kernel(local_count, row_cap, x_ref, wr_ref, ids_ref, slot_ref, cols_ref, cnt_ref):
    tok = x_ref.shape[0]
    n_exp = wr_ref.shape[0]
    w = wr_ref[...]
    w_hi = w.astype(BF16)
    rest = w - w_hi.astype(F32)
    w_mid = rest.astype(BF16)
    w_lo = (rest - w_mid.astype(F32)).astype(BF16)
    x = x_ref[...]
    nt = (((1,), (1,)), ((), ()))
    w_all = jnp.concatenate([w_hi, w_mid, w_lo], axis=0)
    parts = lax.dot_general(w_all, x, nt, preferred_element_type=F32)
    logits = parts[:n_exp] + (parts[n_exp : 2 * n_exp] + parts[2 * n_exp :])
    ids = ids_ref[...]
    id_a, id_b = ids[0:1], ids[1:2]
    row = lax.broadcasted_iota(I32, (n_exp, tok), 0)
    oh_a, oh_b = row == id_a, row == id_b
    zero = jnp.zeros((), F32)
    l_a = jnp.sum(jnp.where(oh_a, logits, zero), axis=0, keepdims=True)
    l_b = jnp.sum(jnp.where(oh_b, logits, zero), axis=0, keepdims=True)
    top = jnp.maximum(l_a, l_b)
    e_a, e_b = jnp.exp(l_a - top), jnp.exp(l_b - top)
    g_a, g_b = e_a / (e_a + e_b), e_b / (e_a + e_b)
    chosen = jnp.where(oh_a | oh_b, 1.0, 0.0).astype(F32)
    width = 256
    tri = (lax.broadcasted_iota(I32, (width, width), 0) < lax.broadcasted_iota(I32, (width, width), 1))
    tri = jnp.where(tri, 1.0, 0.0).astype(BF16)
    before = jnp.zeros((n_exp, 1), F32)
    ranks = []
    for k in range(tok // width):
        blk = chosen[:, k * width : (k + 1) * width]
        ranks.append(_dot(blk.astype(BF16), tri) + before)
        before = before + jnp.sum(blk, axis=1, keepdims=True)
    rank = jnp.concatenate(ranks, axis=1)
    cnt_ref[...] = jnp.broadcast_to(before, cnt_ref.shape).astype(I32)

    def slot_of(ident, onehot):
        here = jnp.sum(jnp.where(onehot, rank, zero), axis=0, keepdims=True)
        dev = ident // local_count
        lower = (row < ident) & (row >= dev * local_count)
        base = jnp.sum(jnp.where(lower, jnp.broadcast_to(before, (n_exp, tok)), zero), axis=0, keepdims=True)
        return dev.astype(F32) * row_cap + here + base

    s_a, s_b = slot_of(id_a, oh_a), slot_of(id_b, oh_b)
    both = jnp.concatenate([s_a, s_b, g_a, g_b, s_a, s_b, g_a, g_b], axis=0)
    slot_ref[...] = both.astype(I32)
    cols_ref[...] = both.T


def pack_kernel(row_cap, chunks, counts_ref, slot_ref, x_ref, *refs):
    out_refs, list_ref = refs[:-1], refs[-1]
    tok = x_ref.shape[0]
    n_dev = out_refs[0].shape[0]
    for (start, size), out_ref in zip(chunks, out_refs):

        def collect(d, cnt):
            list_ref[cnt] = d
            return cnt + (counts_ref[d] > start).astype(I32)

        list_ref[n_dev] = 0
        cnt = lax.fori_loop(0, n_dev, collect, jnp.int32(0))
        last = jnp.maximum(cnt - 1, 0)

        def pair(i, _):
            d0, d1 = list_ref[2 * i], list_ref[jnp.minimum(2 * i + 1, last)]
            pos = lax.broadcasted_iota(I32, (size, tok), 0) + start
            want = jnp.concatenate([pos + d0 * row_cap, pos + d1 * row_cap], axis=0)
            hit = (want == slot_ref[0:1, :]) | (want == slot_ref[1:2, :])
            pick = jnp.where(hit, 1.0, 0.0).astype(BF16)
            rows = _dot(pick, x_ref[...]).astype(BF16)
            out_ref[d0] = rows[:size]
            out_ref[d1] = rows[size:]
            return 0

        lax.fori_loop(0, (cnt + 1) // 2, pair, 0)


WIDE = 512
STEP = 256


def ffn_kernel(start, size, n_src, bound_ref, x_ref, w1_hbm, w3_hbm, w2_hbm, out_ref, w1, w3, w2, xbuf, hbuf, ybuf, list_ref, sems):
    n_loc, _, ff = w1.shape
    n_f = ff // WIDE
    per = size // TILE

    def copy(e, which, f):
        cut = pl.ds(f * WIDE, WIDE)
        at = (e, cut) if which == 2 else (e, slice(None), cut)
        src, dst = ((w1_hbm, w1), (w3_hbm, w3), (w2_hbm, w2))[which]
        return pltpu.make_async_copy(src.at[at], dst.at[at], sems.at[e, which, f])

    counts = []
    for e in range(n_loc):

        def need(s, any_):
            lo, hi = bound_ref[e, s], bound_ref[e + 1, s]
            return any_ | ((lo < start + size) & (hi > start) & (hi > lo)).astype(I32)

        used = lax.fori_loop(0, n_src, need, jnp.int32(0))
        counts.append(used)

        @pl.when(used > 0)
        def _():
            for f in range(n_f):
                copy(e, 0, f).start()
                copy(e, 1, f).start()
            for f in range(n_f):
                copy(e, 2, f).start()

    out_ref[...] = jnp.zeros_like(out_ref)
    for e in range(n_loc):

        @pl.when(counts[e] > 0)
        def _():
            def collect(i, cnt):
                s = i // per
                t0 = start + (i % per) * TILE
                lo = bound_ref[e, s]
                hi = bound_ref[e + 1, s]
                hit = (lo < t0 + TILE) & (hi > t0) & (hi > lo)

                @pl.when(hit)
                def _():
                    list_ref[cnt] = i
                    here = pl.ds(pl.multiple_of(i * TILE, TILE), TILE)
                    xbuf[pl.ds(pl.multiple_of(cnt * TILE, TILE), TILE), :] = x_ref[here, :]

                return cnt + hit.astype(I32)

            cnt = lax.fori_loop(0, n_src * per, collect, jnp.int32(0))

            def block(g, _):
                at = pl.ds(pl.multiple_of(g * STEP, STEP), STEP)
                xb = xbuf[at, :]
                for f in range(n_f):

                    @pl.when(g == 0)
                    def _():
                        copy(e, 0, f).wait()
                        copy(e, 1, f).wait()

                    cut = slice(f * WIDE, (f + 1) * WIDE)
                    u = _dot(xb, w1[e, :, cut])
                    v = _dot(xb, w3[e, :, cut])
                    hbuf[:, cut] = (u * jax.nn.sigmoid(u) * v).astype(BF16)

                @pl.when(g == 0)
                def _():
                    for f in range(n_f):
                        copy(e, 2, f).wait()

                ybuf[at, :] = _dot(hbuf[...], w2[e]).astype(BF16)
                return 0

            lax.fori_loop(0, (cnt * TILE + STEP - 1) // STEP, block, 0)

            def put(k, _):
                i = list_ref[k]
                s = i // per
                t0 = start + (i % per) * TILE
                pos = t0 + lax.broadcasted_iota(I32, (TILE, 1), 0)
                own = (pos >= bound_ref[e, s]) & (pos < bound_ref[e + 1, s])
                at = pl.ds(pl.multiple_of(i * TILE, TILE), TILE)
                y = ybuf[pl.ds(pl.multiple_of(k * TILE, TILE), TILE), :]
                out_ref[at, :] = jnp.where(own, y, out_ref[at, :])
                return 0

            lax.fori_loop(0, cnt, put, 0)


def combine_kernel(row_cap, start, size, n_dev, has_acc, counts_ref, cols_ref, back_ref, *refs):
    if has_acc:
        acc_ref, out_ref, rows_ref, slot_ref, cnt_ref = refs
    else:
        out_ref, rows_ref, slot_ref, cnt_ref = refs

    @pl.when(pl.program_id(0) == 0)
    def _():
        slot_ref[...] = jnp.full_like(slot_ref, -1.0)

        def collect(d, cnt):
            @pl.when(counts_ref[d] > start)
            def _():
                pos = lax.broadcasted_iota(I32, (1, size), 1) + (d * row_cap + start)
                rows_ref[pl.ds(pl.multiple_of(cnt * size, TILE), size), :] = back_ref[d]
                slot_ref[cnt] = jnp.broadcast_to(pos.astype(F32), (8, size))

            return cnt + (counts_ref[d] > start).astype(I32)

        cnt = lax.fori_loop(0, n_dev, collect, jnp.int32(0))
        cnt_ref[0] = cnt

        @pl.when(cnt % 2 == 1)
        def _():
            rows_ref[pl.ds(pl.multiple_of(cnt * size, TILE), size), :] = jnp.zeros((size, rows_ref.shape[1]), BF16)

    c = cols_ref[...]
    toks, dim = out_ref.shape

    def pair(i, total):
        rows = rows_ref[pl.ds(pl.multiple_of(i * 2 * size, TILE), 2 * size), :]
        ids = jnp.concatenate([slot_ref[2 * i, 0:1], slot_ref[2 * i + 1, 0:1]], axis=1)
        for k in range(2):
            pick = jnp.where(ids == c[:, k : k + 1], 1.0, 0.0).astype(BF16)
            total = total + c[:, 2 + k : 3 + k] * _dot(pick, rows)
        return total

    first = acc_ref[...] if has_acc else jnp.zeros((toks, dim), F32)
    total = lax.fori_loop(0, (cnt_ref[0] + 1) // 2, pair, first)
    out_ref[...] = total.astype(out_ref.dtype)


def _params(**kw):
    return pltpu.CompilerParams(vmem_limit_bytes=VMEM_BYTES, **kw)


def solution(mesh):
    n = mesh.shape["ep"]

    def body(x, w_router, ids, w1, w3, w2):
        tok, dim = x.shape
        local = w1.shape[0]
        ff = w1.shape[2]
        n_exp = n * local
        cap = 4 * tok // n
        slots, cols, counts = pl.pallas_call(
            functools.partial(route_kernel, local, cap),
            out_shape=(
                jax.ShapeDtypeStruct((8, tok), I32),
                jax.ShapeDtypeStruct((tok, 8), F32),
                jax.ShapeDtypeStruct((n_exp, 128), I32),
            ),
            compiler_params=_params(),
            name="route",
        )(x, w_router.T, ids.T)
        per_exp = lax.all_to_all(counts[:, 0].reshape(n, local), "ep", 0, 0, tiled=True)
        ends = jnp.cumsum(per_exp, axis=1).T
        bounds = jnp.concatenate([jnp.zeros((1, n), I32), ends], axis=0)
        dev_counts = jnp.sum(counts[:, 0].reshape(n, local), axis=1)
        smem = pl.BlockSpec(memory_space=pltpu.SMEM)
        vmem = pl.BlockSpec(memory_space=pltpu.VMEM)
        hbm = pl.BlockSpec(memory_space=pl.ANY)
        sends = []
        for part in (CHUNKS[:1], CHUNKS[1:]):
            total = sum(size for _, size in part)
            pack = pl.pallas_call(
                functools.partial(pack_kernel, cap, part),
                in_specs=[smem, vmem, vmem],
                out_specs=[vmem] * len(part),
                out_shape=[jax.ShapeDtypeStruct((n, size, dim), BF16) for _, size in part],
                scratch_shapes=[pltpu.SMEM((n + 1,), I32)],
                compiler_params=_params(),
                cost_estimate=pl.CostEstimate(flops=2 * n * total * tok * dim, bytes_accessed=1, transcendentals=0),
            )
            sends += pack(dev_counts, slots, x)
        acc = None
        for index, (start, size) in enumerate(CHUNKS):
            got = lax.all_to_all(sends[index], "ep", 0, 0, tiled=True)
            rows = n * size
            made = pl.pallas_call(
                functools.partial(ffn_kernel, start, size, n),
                in_specs=[smem, vmem, hbm, hbm, hbm],
                out_specs=vmem,
                scratch_shapes=[
                    pltpu.VMEM((local, dim, ff), BF16),
                    pltpu.VMEM((local, dim, ff), BF16),
                    pltpu.VMEM((local, ff, dim), BF16),
                    pltpu.VMEM((rows, dim), BF16),
                    pltpu.VMEM((STEP, ff), BF16),
                    pltpu.VMEM((rows, dim), BF16),
                    pltpu.SMEM((rows // TILE,), I32),
                    pltpu.SemaphoreType.DMA((local, 3, ff // WIDE)),
                ],
                out_shape=jax.ShapeDtypeStruct((rows, dim), BF16),
                compiler_params=_params(),
                cost_estimate=pl.CostEstimate(flops=6 * rows * dim * ff, bytes_accessed=1, transcendentals=0),
            )
            made = made(bounds, got.reshape(rows, dim), w1, w3, w2)
            back = lax.all_to_all(made.reshape(n, size, dim), "ep", 0, 0, tiled=True)
            last = index == len(CHUNKS) - 1
            tb = 512
            tile_spec = pl.BlockSpec((tb, dim), lambda i, c: (i, 0))
            ins = [cols, back] + ([] if acc is None else [acc])
            specs = [pl.BlockSpec((tb, 8), lambda i, c: (i, 0)), pl.BlockSpec((n, size, dim), lambda i, c: (0, 0, 0))]
            combine = pl.pallas_call(
                functools.partial(combine_kernel, cap, start, size, n, acc is not None),
                grid_spec=pltpu.PrefetchScalarGridSpec(
                    num_scalar_prefetch=1,
                    grid=(tok // tb,),
                    in_specs=specs + ([] if acc is None else [tile_spec]),
                    out_specs=tile_spec,
                    scratch_shapes=[
                        pltpu.VMEM((rows + size, dim), BF16),
                        pltpu.VMEM((n + 1, 8, size), F32),
                        pltpu.SMEM((1,), I32),
                    ],
                ),
                out_shape=jax.ShapeDtypeStruct((tok, dim), BF16 if last else F32),
                compiler_params=_params(),
                cost_estimate=pl.CostEstimate(flops=4 * rows * tok * dim, bytes_accessed=1, transcendentals=0),
            )
            acc = combine(dev_counts, *ins)
        return acc

    return jax.shard_map(
        body,
        mesh=mesh,
        in_specs=(P("ep", None), P(None, None), P("ep", None), P("ep", None, None), P("ep", None, None), P("ep", None, None)),
        out_specs=P("ep", None),
        check_vma=False,
    )
```

```python
import functools

import jax
import jax.numpy as jnp
from jax import lax
from jax.experimental import pallas as pl
from jax.experimental.pallas import tpu as pltpu
from jax.sharding import PartitionSpec as P


F32 = jnp.float32
BF16 = jnp.bfloat16
I32 = jnp.int32
TILE = 16
CHUNKS = ((0, 128), (128, 128), (256, 128), (384, 128))
VMEM_BYTES = 60 * 1024 * 1024


def _dot(a, b):
    return jnp.dot(a, b, preferred_element_type=F32)


def route_kernel(local_count, row_cap, x_ref, wr_ref, ids_ref, slot_ref, cols_ref, cnt_ref):
    tok = x_ref.shape[0]
    n_exp = wr_ref.shape[0]
    w = wr_ref[...]
    w_hi = w.astype(BF16)
    rest = w - w_hi.astype(F32)
    w_mid = rest.astype(BF16)
    w_lo = (rest - w_mid.astype(F32)).astype(BF16)
    x = x_ref[...]
    nt = (((1,), (1,)), ((), ()))
    w_all = jnp.concatenate([w_hi, w_mid, w_lo], axis=0)
    parts = lax.dot_general(w_all, x, nt, preferred_element_type=F32)
    logits = parts[:n_exp] + (parts[n_exp : 2 * n_exp] + parts[2 * n_exp :])
    ids = ids_ref[...]
    id_a, id_b = ids[0:1], ids[1:2]
    row = lax.broadcasted_iota(I32, (n_exp, tok), 0)
    oh_a, oh_b = row == id_a, row == id_b
    zero = jnp.zeros((), F32)
    l_a = jnp.sum(jnp.where(oh_a, logits, zero), axis=0, keepdims=True)
    l_b = jnp.sum(jnp.where(oh_b, logits, zero), axis=0, keepdims=True)
    top = jnp.maximum(l_a, l_b)
    e_a, e_b = jnp.exp(l_a - top), jnp.exp(l_b - top)
    g_a, g_b = e_a / (e_a + e_b), e_b / (e_a + e_b)
    chosen = jnp.where(oh_a | oh_b, 1.0, 0.0).astype(F32)
    width = 256
    tri = (lax.broadcasted_iota(I32, (width, width), 0) < lax.broadcasted_iota(I32, (width, width), 1))
    tri = jnp.where(tri, 1.0, 0.0).astype(BF16)
    before = jnp.zeros((n_exp, 1), F32)
    ranks = []
    for k in range(tok // width):
        blk = chosen[:, k * width : (k + 1) * width]
        ranks.append(_dot(blk.astype(BF16), tri) + before)
        before = before + jnp.sum(blk, axis=1, keepdims=True)
    rank = jnp.concatenate(ranks, axis=1)
    cnt_ref[...] = jnp.broadcast_to(before, cnt_ref.shape).astype(I32)

    def slot_of(ident, onehot):
        here = jnp.sum(jnp.where(onehot, rank, zero), axis=0, keepdims=True)
        dev = ident // local_count
        lower = (row < ident) & (row >= dev * local_count)
        base = jnp.sum(jnp.where(lower, jnp.broadcast_to(before, (n_exp, tok)), zero), axis=0, keepdims=True)
        return dev.astype(F32) * row_cap + here + base

    s_a, s_b = slot_of(id_a, oh_a), slot_of(id_b, oh_b)
    both = jnp.concatenate([s_a, s_b, g_a, g_b, s_a, s_b, g_a, g_b], axis=0)
    slot_ref[...] = both.astype(I32)
    cols_ref[...] = both.T


SLOT_TILE = 32
PACK_GROUP = 8
SUM_GROUP = 16


def list_tiles(n_dev, size, start, counts_ref, list_ref, visit=None):
    per = size // SLOT_TILE

    def collect(i, cnt):
        hit = counts_ref[i // per] > start + (i % per) * SLOT_TILE

        @pl.when(hit)
        def _():
            list_ref[cnt] = i
            if visit is not None:
                visit(i, cnt)

        return cnt + hit.astype(I32)

    return lax.fori_loop(0, n_dev * per, collect, jnp.int32(0))


def first_slot(i, size, start, row_cap):
    per = size // SLOT_TILE
    return (i // per) * row_cap + start + (i % per) * SLOT_TILE


def pack_kernel(row_cap, chunks, counts_ref, slot_ref, x_ref, *refs):
    out_refs, list_ref = refs[:-1], refs[-1]
    tok = x_ref.shape[0]
    for (start, size), out_ref in zip(chunks, out_refs):
        n_dev = out_ref.shape[0] // size
        list_ref[0] = 0
        cnt = list_tiles(n_dev, size, start, counts_ref, list_ref)
        last = jnp.maximum(cnt - 1, 0)

        @pl.loop(0, (cnt + PACK_GROUP - 1) // PACK_GROUP)
        def _(g):
            tiles = [list_ref[jnp.minimum(g * PACK_GROUP + j, last)] for j in range(PACK_GROUP)]
            pos = lax.broadcasted_iota(I32, (SLOT_TILE, tok), 0)
            want = jnp.concatenate([pos + first_slot(i, size, start, row_cap) for i in tiles], axis=0)
            hit = (want == slot_ref[0:1, :]) | (want == slot_ref[1:2, :])
            pick = jnp.where(hit, 1.0, 0.0).astype(BF16)
            rows = _dot(pick, x_ref[...]).astype(BF16)
            for j, i in enumerate(tiles):
                at = pl.ds(pl.multiple_of(i * SLOT_TILE, SLOT_TILE), SLOT_TILE)
                out_ref[at, :] = rows[j * SLOT_TILE : (j + 1) * SLOT_TILE]


WIDE = 512
STEP = 256


def ffn_kernel(start, size, n_src, bound_ref, x_ref, w1_hbm, w3_hbm, w2_hbm, out_ref, w1, w3, w2, xbuf, hbuf, ybuf, list_ref, sems):
    n_loc, _, ff = w1.shape
    n_f = ff // WIDE
    per = size // TILE

    def copy(e, which, f):
        cut = pl.ds(f * WIDE, WIDE)
        at = (e, cut) if which == 2 else (e, slice(None), cut)
        src, dst = ((w1_hbm, w1), (w3_hbm, w3), (w2_hbm, w2))[which]
        return pltpu.make_async_copy(src.at[at], dst.at[at], sems.at[e, which, f])

    counts = []
    for e in range(n_loc):

        def need(s, any_):
            lo, hi = bound_ref[e, s], bound_ref[e + 1, s]
            return any_ | ((lo < start + size) & (hi > start) & (hi > lo)).astype(I32)

        used = lax.fori_loop(0, n_src, need, jnp.int32(0))
        counts.append(used)

        @pl.when(used > 0)
        def _():
            for f in range(n_f):
                copy(e, 0, f).start()
                copy(e, 1, f).start()
            for f in range(n_f):
                copy(e, 2, f).start()

    out_ref[...] = jnp.zeros_like(out_ref)
    for e in range(n_loc):

        @pl.when(counts[e] > 0)
        def _():
            def collect(i, cnt):
                s = i // per
                t0 = start + (i % per) * TILE
                lo = bound_ref[e, s]
                hi = bound_ref[e + 1, s]
                hit = (lo < t0 + TILE) & (hi > t0) & (hi > lo)

                @pl.when(hit)
                def _():
                    list_ref[cnt] = i
                    here = pl.ds(pl.multiple_of(i * TILE, TILE), TILE)
                    xbuf[pl.ds(pl.multiple_of(cnt * TILE, TILE), TILE), :] = x_ref[here, :]

                return cnt + hit.astype(I32)

            cnt = lax.fori_loop(0, n_src * per, collect, jnp.int32(0))

            def block(g, fresh):
                at = pl.ds(pl.multiple_of(g * STEP, STEP), STEP)
                xb = xbuf[at, :]
                for f in range(n_f):
                    if fresh:
                        copy(e, 0, f).wait()
                        copy(e, 1, f).wait()
                    cut = slice(f * WIDE, (f + 1) * WIDE)
                    u = _dot(xb, w1[e, :, cut])
                    v = _dot(xb, w3[e, :, cut])
                    hbuf[:, cut] = (u * jax.nn.sigmoid(u) * v).astype(BF16)
                if fresh:
                    for f in range(n_f):
                        copy(e, 2, f).wait()
                ybuf[at, :] = _dot(hbuf[...], w2[e]).astype(BF16)

            block(0, True)

            @pl.loop(1, (cnt * TILE + STEP - 1) // STEP)
            def _(g):
                block(g, False)

            def put(k, _):
                i = list_ref[k]
                s = i // per
                t0 = start + (i % per) * TILE
                pos = t0 + lax.broadcasted_iota(I32, (TILE, 1), 0)
                own = (pos >= bound_ref[e, s]) & (pos < bound_ref[e + 1, s])
                at = pl.ds(pl.multiple_of(i * TILE, TILE), TILE)
                y = ybuf[pl.ds(pl.multiple_of(k * TILE, TILE), TILE), :]
                out_ref[at, :] = jnp.where(own, y, out_ref[at, :])
                return 0

            lax.fori_loop(0, cnt, put, 0)


def combine_kernel(row_cap, start, size, n_dev, has_acc, counts_ref, cols_ref, back_ref, *refs):
    if has_acc:
        acc_ref, out_ref, rows_ref, sum_ref, list_ref, cnt_ref = refs
    else:
        out_ref, rows_ref, sum_ref, list_ref, cnt_ref = refs
    group = SUM_GROUP * SLOT_TILE
    toks, dim = out_ref.shape

    @pl.when(pl.program_id(0) == 0)
    def _():
        def bring(i, k):
            src = pl.ds(pl.multiple_of(i * SLOT_TILE, SLOT_TILE), SLOT_TILE)
            rows_ref[pl.ds(pl.multiple_of(k * SLOT_TILE, SLOT_TILE), SLOT_TILE), :] = back_ref[src, :]

        cnt = list_tiles(n_dev, size, start, counts_ref, list_ref, bring)
        groups = (cnt + SUM_GROUP - 1) // SUM_GROUP
        cnt_ref[0] = groups

        @pl.loop(cnt, groups * SUM_GROUP)
        def _(k):
            list_ref[k] = -1
            rows_ref[pl.ds(pl.multiple_of(k * SLOT_TILE, SLOT_TILE), SLOT_TILE), :] = jnp.zeros((SLOT_TILE, dim), BF16)

    c = cols_ref[...]
    sum_ref[...] = acc_ref[...] if has_acc else jnp.zeros((toks, dim), F32)
    lane = lax.broadcasted_iota(I32, (1, group), 1)

    @pl.loop(0, cnt_ref[0])
    def _(g):
        rows = rows_ref[pl.ds(pl.multiple_of(g * group, group), group), :]
        ids = jnp.full((1, group), -1, I32)
        for j in range(SUM_GROUP):
            i = list_ref[g * SUM_GROUP + j]
            base = jnp.where(i < 0, -1 - group, first_slot(i, size, start, row_cap))
            ids = jnp.where(lane // SLOT_TILE == j, base + lane % SLOT_TILE, ids)
        ids = ids.astype(F32)
        add = 0.0
        for k in range(2):
            pick = jnp.where(ids == c[:, k : k + 1], 1.0, 0.0).astype(BF16)
            add = add + c[:, 2 + k : 3 + k] * _dot(pick, rows)
        sum_ref[...] += add

    out_ref[...] = sum_ref[...].astype(out_ref.dtype)


def _params(**kw):
    return pltpu.CompilerParams(vmem_limit_bytes=VMEM_BYTES, **kw)


def solution(mesh):
    n = mesh.shape["ep"]

    def body(x, w_router, ids, w1, w3, w2):
        tok, dim = x.shape
        local = w1.shape[0]
        ff = w1.shape[2]
        n_exp = n * local
        cap = 4 * tok // n
        slots, cols, counts = pl.pallas_call(
            functools.partial(route_kernel, local, cap),
            out_shape=(
                jax.ShapeDtypeStruct((8, tok), I32),
                jax.ShapeDtypeStruct((tok, 8), F32),
                jax.ShapeDtypeStruct((n_exp, 128), I32),
            ),
            compiler_params=_params(),
            name="route",
        )(x, w_router.T, ids.T)
        per_exp = lax.all_to_all(counts[:, 0].reshape(n, local), "ep", 0, 0, tiled=True)
        ends = jnp.cumsum(per_exp, axis=1).T
        bounds = jnp.concatenate([jnp.zeros((1, n), I32), ends], axis=0)
        dev_counts = jnp.sum(counts[:, 0].reshape(n, local), axis=1)
        smem = pl.BlockSpec(memory_space=pltpu.SMEM)
        vmem = pl.BlockSpec(memory_space=pltpu.VMEM)
        hbm = pl.BlockSpec(memory_space=pl.ANY)
        sends = []
        for part in (CHUNKS[:1], CHUNKS[1:]):
            total = sum(size for _, size in part)
            pack = pl.pallas_call(
                functools.partial(pack_kernel, cap, part),
                in_specs=[smem, vmem, vmem],
                out_specs=[vmem] * len(part),
                out_shape=[jax.ShapeDtypeStruct((n * size, dim), BF16) for _, size in part],
                scratch_shapes=[pltpu.SMEM((cap * n // SLOT_TILE,), I32)],
                compiler_params=_params(),
                cost_estimate=pl.CostEstimate(flops=2 * n * total * tok * dim, bytes_accessed=1, transcendentals=0),
            )
            sends += pack(dev_counts, slots, x)
        acc = None
        for index, (start, size) in enumerate(CHUNKS):
            got = lax.all_to_all(sends[index].reshape(n, size, dim), "ep", 0, 0, tiled=True)
            rows = n * size
            made = pl.pallas_call(
                functools.partial(ffn_kernel, start, size, n),
                in_specs=[smem, vmem, hbm, hbm, hbm],
                out_specs=vmem,
                scratch_shapes=[
                    pltpu.VMEM((local, dim, ff), BF16),
                    pltpu.VMEM((local, dim, ff), BF16),
                    pltpu.VMEM((local, ff, dim), BF16),
                    pltpu.VMEM((rows, dim), BF16),
                    pltpu.VMEM((STEP, ff), BF16),
                    pltpu.VMEM((rows, dim), BF16),
                    pltpu.SMEM((rows // TILE,), I32),
                    pltpu.SemaphoreType.DMA((local, 3, ff // WIDE)),
                ],
                out_shape=jax.ShapeDtypeStruct((rows, dim), BF16),
                compiler_params=_params(),
                cost_estimate=pl.CostEstimate(flops=6 * rows * dim * ff, bytes_accessed=1, transcendentals=0),
            )
            made = made(bounds, got.reshape(rows, dim), w1, w3, w2)
            back = lax.all_to_all(made.reshape(n, size, dim), "ep", 0, 0, tiled=True).reshape(rows, dim)
            last = index == len(CHUNKS) - 1
            tb = 512
            tile_spec = pl.BlockSpec((tb, dim), lambda i, c: (i, 0))
            ins = [cols, back] + ([] if acc is None else [acc])
            specs = [pl.BlockSpec((tb, 8), lambda i, c: (i, 0)), pl.BlockSpec((rows, dim), lambda i, c: (0, 0))]
            combine = pl.pallas_call(
                functools.partial(combine_kernel, cap, start, size, n, acc is not None),
                grid_spec=pltpu.PrefetchScalarGridSpec(
                    num_scalar_prefetch=1,
                    grid=(tok // tb,),
                    in_specs=specs + ([] if acc is None else [tile_spec]),
                    out_specs=tile_spec,
                    scratch_shapes=[
                        pltpu.VMEM((rows, dim), BF16),
                        pltpu.VMEM((tb, dim), F32),
                        pltpu.SMEM((rows // SLOT_TILE,), I32),
                        pltpu.SMEM((1,), I32),
                    ],
                ),
                out_shape=jax.ShapeDtypeStruct((tok, dim), BF16 if last else F32),
                compiler_params=_params(),
                cost_estimate=pl.CostEstimate(flops=4 * rows * tok * dim, bytes_accessed=1, transcendentals=0),
            )
            acc = combine(dev_counts, *ins)
        return acc

    return jax.shard_map(
        body,
        mesh=mesh,
        in_specs=(P("ep", None), P(None, None), P("ep", None), P("ep", None, None), P("ep", None, None), P("ep", None, None)),
        out_specs=P("ep", None),
        check_vma=False,
    )
```

```python
import functools

import jax
import jax.numpy as jnp
from jax import lax
from jax.experimental import pallas as pl
from jax.experimental.pallas import tpu as pltpu
from jax.sharding import PartitionSpec as P


F32 = jnp.float32
BF16 = jnp.bfloat16
I32 = jnp.int32
TILE = 16
CHUNKS = ((0, 128), (128, 128), (256, 128), (384, 128))
VMEM_BYTES = 60 * 1024 * 1024
FFN_VMEM = 44 * 1024 * 1024


def _dot(a, b):
    return jnp.dot(a, b, preferred_element_type=F32)


def route_kernel(local_count, row_cap, x_ref, wr_ref, ids_ref, slot_ref, cols_ref, cnt_ref):
    tok = x_ref.shape[0]
    n_exp = wr_ref.shape[0]
    w = wr_ref[...]
    w_hi = w.astype(BF16)
    rest = w - w_hi.astype(F32)
    w_mid = rest.astype(BF16)
    w_lo = (rest - w_mid.astype(F32)).astype(BF16)
    x = x_ref[...]
    nt = (((1,), (1,)), ((), ()))
    w_all = jnp.concatenate([w_hi, w_mid, w_lo], axis=0)
    parts = lax.dot_general(w_all, x, nt, preferred_element_type=F32)
    logits = parts[:n_exp] + (parts[n_exp : 2 * n_exp] + parts[2 * n_exp :])
    ids = ids_ref[...]
    id_a, id_b = ids[0:1], ids[1:2]
    row = lax.broadcasted_iota(I32, (n_exp, tok), 0)
    oh_a, oh_b = row == id_a, row == id_b
    zero = jnp.zeros((), F32)
    l_a = jnp.sum(jnp.where(oh_a, logits, zero), axis=0, keepdims=True)
    l_b = jnp.sum(jnp.where(oh_b, logits, zero), axis=0, keepdims=True)
    top = jnp.maximum(l_a, l_b)
    e_a, e_b = jnp.exp(l_a - top), jnp.exp(l_b - top)
    g_a, g_b = e_a / (e_a + e_b), e_b / (e_a + e_b)
    chosen = jnp.where(oh_a | oh_b, 1.0, 0.0).astype(F32)
    width = 256
    tri = (lax.broadcasted_iota(I32, (width, width), 0) < lax.broadcasted_iota(I32, (width, width), 1))
    tri = jnp.where(tri, 1.0, 0.0).astype(BF16)
    before = jnp.zeros((n_exp, 1), F32)
    ranks = []
    for k in range(tok // width):
        blk = chosen[:, k * width : (k + 1) * width]
        ranks.append(_dot(blk.astype(BF16), tri) + before)
        before = before + jnp.sum(blk, axis=1, keepdims=True)
    rank = jnp.concatenate(ranks, axis=1)
    cnt_ref[...] = jnp.broadcast_to(before, cnt_ref.shape).astype(I32)

    def slot_of(ident, onehot):
        here = jnp.sum(jnp.where(onehot, rank, zero), axis=0, keepdims=True)
        dev = ident // local_count
        lower = (row < ident) & (row >= dev * local_count)
        base = jnp.sum(jnp.where(lower, jnp.broadcast_to(before, (n_exp, tok)), zero), axis=0, keepdims=True)
        return dev.astype(F32) * row_cap + here + base

    s_a, s_b = slot_of(id_a, oh_a), slot_of(id_b, oh_b)
    both = jnp.concatenate([s_a, s_b, g_a, g_b, s_a, s_b, g_a, g_b], axis=0)
    slot_ref[...] = both.astype(I32)
    cols_ref[...] = both.T


SLOT_TILE = 32
PACK_GROUP = 8
SUM_GROUP = 16


def list_tiles(n_dev, size, start, counts_ref, list_ref, visit=None):
    per = size // SLOT_TILE

    def collect(i, cnt):
        hit = counts_ref[i // per] > start + (i % per) * SLOT_TILE

        @pl.when(hit)
        def _():
            list_ref[cnt] = i
            if visit is not None:
                visit(i, cnt)

        return cnt + hit.astype(I32)

    return lax.fori_loop(0, n_dev * per, collect, jnp.int32(0))


def first_slot(i, size, start, row_cap):
    per = size // SLOT_TILE
    return (i // per) * row_cap + start + (i % per) * SLOT_TILE


def pack_kernel(row_cap, chunks, counts_ref, slot_ref, x_ref, *refs):
    out_refs, list_ref = refs[:-1], refs[-1]
    tok = x_ref.shape[0]
    for (start, size), out_ref in zip(chunks, out_refs):
        n_dev = out_ref.shape[0] // size
        list_ref[0] = 0
        cnt = list_tiles(n_dev, size, start, counts_ref, list_ref)
        last = jnp.maximum(cnt - 1, 0)

        @pl.loop(0, (cnt + PACK_GROUP - 1) // PACK_GROUP)
        def _(g):
            tiles = [list_ref[jnp.minimum(g * PACK_GROUP + j, last)] for j in range(PACK_GROUP)]
            pos = lax.broadcasted_iota(I32, (SLOT_TILE, tok), 0)
            want = jnp.concatenate([pos + first_slot(i, size, start, row_cap) for i in tiles], axis=0)
            hit = (want == slot_ref[0:1, :]) | (want == slot_ref[1:2, :])
            pick = jnp.where(hit, 1.0, 0.0).astype(BF16)
            rows = _dot(pick, x_ref[...]).astype(BF16)
            for j, i in enumerate(tiles):
                at = pl.ds(pl.multiple_of(i * SLOT_TILE, SLOT_TILE), SLOT_TILE)
                out_ref[at, :] = rows[j * SLOT_TILE : (j + 1) * SLOT_TILE]


WIDE = 512
STEP = 256


def ffn_kernel(start, size, n_src, bound_ref, x_ref, w1_hbm, w3_hbm, w2_hbm, out_ref, w1, w3, w2, xbuf, hbuf, ybuf, list_ref, used_ref, sems):
    n_loc, _, ff = w1.shape
    n_f = ff // WIDE
    per = size // TILE

    def copy(e, which, f):
        cut = pl.ds(f * WIDE, WIDE)
        at = (e, cut) if which == 2 else (e, slice(None), cut)
        src, dst = ((w1_hbm, w1), (w3_hbm, w3), (w2_hbm, w2))[which]
        return pltpu.make_async_copy(src.at[at], dst.at[at], sems.at[e, which, f])

    @pl.loop(0, n_loc)
    def _(e):
        def need(s, any_):
            lo, hi = bound_ref[e, s], bound_ref[e + 1, s]
            return any_ | ((lo < start + size) & (hi > start) & (hi > lo)).astype(I32)

        used = lax.fori_loop(0, n_src, need, jnp.int32(0))
        used_ref[e] = used

        @pl.when(used > 0)
        def _():
            @pl.loop(0, n_f)
            def _(f):
                copy(e, 0, f).start()
                copy(e, 1, f).start()

            @pl.loop(0, n_f)
            def _(f):
                copy(e, 2, f).start()

    out_ref[...] = jnp.zeros_like(out_ref)

    @pl.loop(0, n_loc)
    def _(e):
        @pl.when(used_ref[e] > 0)
        def _():
            def collect(i, cnt):
                s = i // per
                t0 = start + (i % per) * TILE
                lo = bound_ref[e, s]
                hi = bound_ref[e + 1, s]
                hit = (lo < t0 + TILE) & (hi > t0) & (hi > lo)

                @pl.when(hit)
                def _():
                    list_ref[cnt] = i
                    here = pl.ds(pl.multiple_of(i * TILE, TILE), TILE)
                    xbuf[pl.ds(pl.multiple_of(cnt * TILE, TILE), TILE), :] = x_ref[here, :]

                return cnt + hit.astype(I32)

            cnt = lax.fori_loop(0, n_src * per, collect, jnp.int32(0))

            def columns(at, f):
                cut = pl.ds(f * WIDE if isinstance(f, int) else pl.multiple_of(f * WIDE, WIDE), WIDE)
                xb = xbuf[at, :]
                u = _dot(xb, w1[e, :, cut])
                v = _dot(xb, w3[e, :, cut])
                hbuf[:, cut] = (u * jax.nn.sigmoid(u) * v).astype(BF16)

            @pl.loop(0, n_f)
            def _(f):
                copy(e, 0, f).wait()
                copy(e, 1, f).wait()
                columns(pl.ds(0, STEP), f)

            @pl.loop(0, n_f)
            def _(f):
                copy(e, 2, f).wait()

            @pl.loop(0, (cnt * TILE + STEP - 1) // STEP)
            def _(g):
                at = pl.ds(pl.multiple_of(g * STEP, STEP), STEP)

                @pl.when(g > 0)
                def _():
                    for f in range(n_f):
                        columns(at, f)

                ybuf[at, :] = _dot(hbuf[...], w2[e]).astype(BF16)

            def put(k, _):
                i = list_ref[k]
                s = i // per
                t0 = start + (i % per) * TILE
                pos = t0 + lax.broadcasted_iota(I32, (TILE, 1), 0)
                own = (pos >= bound_ref[e, s]) & (pos < bound_ref[e + 1, s])
                at = pl.ds(pl.multiple_of(i * TILE, TILE), TILE)
                y = ybuf[pl.ds(pl.multiple_of(k * TILE, TILE), TILE), :]
                out_ref[at, :] = jnp.where(own, y, out_ref[at, :])
                return 0

            lax.fori_loop(0, cnt, put, 0)


def combine_kernel(row_cap, start, size, n_dev, has_acc, counts_ref, cols_ref, back_ref, *refs):
    if has_acc:
        acc_ref, out_ref, rows_ref, sum_ref, list_ref, cnt_ref = refs
    else:
        out_ref, rows_ref, sum_ref, list_ref, cnt_ref = refs
    group = SUM_GROUP * SLOT_TILE
    toks, dim = out_ref.shape

    @pl.when(pl.program_id(0) == 0)
    def _():
        def bring(i, k):
            src = pl.ds(pl.multiple_of(i * SLOT_TILE, SLOT_TILE), SLOT_TILE)
            rows_ref[pl.ds(pl.multiple_of(k * SLOT_TILE, SLOT_TILE), SLOT_TILE), :] = back_ref[src, :]

        cnt = list_tiles(n_dev, size, start, counts_ref, list_ref, bring)
        groups = (cnt + SUM_GROUP - 1) // SUM_GROUP
        cnt_ref[0] = groups

        @pl.loop(cnt, groups * SUM_GROUP)
        def _(k):
            list_ref[k] = -1
            rows_ref[pl.ds(pl.multiple_of(k * SLOT_TILE, SLOT_TILE), SLOT_TILE), :] = jnp.zeros((SLOT_TILE, dim), BF16)

    c = cols_ref[...]
    sum_ref[...] = acc_ref[...] if has_acc else jnp.zeros((toks, dim), F32)
    lane = lax.broadcasted_iota(I32, (1, group), 1)

    @pl.loop(0, cnt_ref[0])
    def _(g):
        rows = rows_ref[pl.ds(pl.multiple_of(g * group, group), group), :]
        ids = jnp.full((1, group), -1, I32)
        for j in range(SUM_GROUP):
            i = list_ref[g * SUM_GROUP + j]
            base = jnp.where(i < 0, -1 - group, first_slot(i, size, start, row_cap))
            ids = jnp.where(lane // SLOT_TILE == j, base + lane % SLOT_TILE, ids)
        ids = ids.astype(F32)
        add = 0.0
        for k in range(2):
            pick = jnp.where(ids == c[:, k : k + 1], 1.0, 0.0).astype(BF16)
            add = add + c[:, 2 + k : 3 + k] * _dot(pick, rows)
        sum_ref[...] += add

    out_ref[...] = sum_ref[...].astype(out_ref.dtype)


def _params(vmem_limit_bytes=VMEM_BYTES):
    return pltpu.CompilerParams(vmem_limit_bytes=vmem_limit_bytes)


def solution(mesh):
    n = mesh.shape["ep"]

    def body(x, w_router, ids, w1, w3, w2):
        tok, dim = x.shape
        local = w1.shape[0]
        ff = w1.shape[2]
        n_exp = n * local
        cap = 4 * tok // n
        slots, cols, counts = pl.pallas_call(
            functools.partial(route_kernel, local, cap),
            out_shape=(
                jax.ShapeDtypeStruct((8, tok), I32),
                jax.ShapeDtypeStruct((tok, 8), F32),
                jax.ShapeDtypeStruct((n_exp, 128), I32),
            ),
            compiler_params=_params(),
            name="route",
        )(x, w_router.T, ids.T)
        per_exp = lax.all_to_all(counts[:, 0].reshape(n, local), "ep", 0, 0, tiled=True)
        ends = jnp.cumsum(per_exp, axis=1).T
        bounds = jnp.concatenate([jnp.zeros((1, n), I32), ends], axis=0)
        dev_counts = jnp.sum(counts[:, 0].reshape(n, local), axis=1)
        smem = pl.BlockSpec(memory_space=pltpu.SMEM)
        vmem = pl.BlockSpec(memory_space=pltpu.VMEM)
        hbm = pl.BlockSpec(memory_space=pl.ANY)
        sends = []
        for part in (CHUNKS[:1], CHUNKS[1:]):
            total = sum(size for _, size in part)
            pack = pl.pallas_call(
                functools.partial(pack_kernel, cap, part),
                in_specs=[smem, vmem, vmem],
                out_specs=[vmem] * len(part),
                out_shape=[jax.ShapeDtypeStruct((n * size, dim), BF16) for _, size in part],
                scratch_shapes=[pltpu.SMEM((cap * n // SLOT_TILE,), I32)],
                compiler_params=_params(),
                cost_estimate=pl.CostEstimate(flops=2 * n * total * tok * dim, bytes_accessed=1, transcendentals=0),
            )
            sends += pack(dev_counts, slots, x)
        acc = None
        for index, (start, size) in enumerate(CHUNKS):
            got = lax.all_to_all(sends[index].reshape(n, size, dim), "ep", 0, 0, tiled=True)
            rows = n * size
            made = pl.pallas_call(
                functools.partial(ffn_kernel, start, size, n),
                in_specs=[smem, vmem, hbm, hbm, hbm],
                out_specs=vmem,
                scratch_shapes=[
                    pltpu.VMEM((local, dim, ff), BF16),
                    pltpu.VMEM((local, dim, ff), BF16),
                    pltpu.VMEM((local, ff, dim), BF16),
                    pltpu.VMEM((rows, dim), BF16),
                    pltpu.VMEM((STEP, ff), BF16),
                    pltpu.VMEM((rows, dim), BF16),
                    pltpu.SMEM((rows // TILE,), I32),
                    pltpu.SMEM((local,), I32),
                    pltpu.SemaphoreType.DMA((local, 3, ff // WIDE)),
                ],
                out_shape=pltpu.VMEM((rows, dim), BF16),
                compiler_params=_params(FFN_VMEM),
                cost_estimate=pl.CostEstimate(flops=6 * rows * dim * ff, bytes_accessed=1, transcendentals=0),
            )
            got = pltpu.with_memory_space_constraint(got.reshape(rows, dim), pltpu.VMEM)
            made = made(bounds, got, *[pltpu.with_memory_space_constraint(w, pltpu.HBM) for w in (w1, w3, w2)])
            back = lax.all_to_all(made.reshape(n, size, dim), "ep", 0, 0, tiled=True).reshape(rows, dim)
            last = index == len(CHUNKS) - 1
            tb = 512
            tile_spec = pl.BlockSpec((tb, dim), lambda i, c: (i, 0))
            ins = [cols, back] + ([] if acc is None else [acc])
            specs = [pl.BlockSpec((tb, 8), lambda i, c: (i, 0)), pl.BlockSpec((rows, dim), lambda i, c: (0, 0))]
            combine = pl.pallas_call(
                functools.partial(combine_kernel, cap, start, size, n, acc is not None),
                grid_spec=pltpu.PrefetchScalarGridSpec(
                    num_scalar_prefetch=1,
                    grid=(tok // tb,),
                    in_specs=specs + ([] if acc is None else [tile_spec]),
                    out_specs=tile_spec,
                    scratch_shapes=[
                        pltpu.VMEM((rows, dim), BF16),
                        pltpu.VMEM((tb, dim), F32),
                        pltpu.SMEM((rows // SLOT_TILE,), I32),
                        pltpu.SMEM((1,), I32),
                    ],
                ),
                out_shape=jax.ShapeDtypeStruct((tok, dim), BF16 if last else F32),
                compiler_params=_params(),
                cost_estimate=pl.CostEstimate(flops=4 * rows * tok * dim, bytes_accessed=1, transcendentals=0),
            )
            acc = combine(dev_counts, *ins)
        return acc

    return jax.shard_map(
        body,
        mesh=mesh,
        in_specs=(P("ep", None), P(None, None), P("ep", None), P("ep", None, None), P("ep", None, None), P("ep", None, None)),
        out_specs=P("ep", None),
        check_vma=False,
    )
```

```python
import functools

import jax
import jax.numpy as jnp
from jax import lax
from jax.experimental import pallas as pl
from jax.experimental.pallas import tpu as pltpu
from jax.sharding import PartitionSpec as P


F32 = jnp.float32
BF16 = jnp.bfloat16
I32 = jnp.int32
TILE = 16
CHUNKS = ((0, 256), (256, 256))
VMEM_BYTES = 60 * 1024 * 1024
FFN_VMEM = 50 * 1024 * 1024


def _dot(a, b):
    return jnp.dot(a, b, preferred_element_type=F32)


def route_kernel(local_count, row_cap, x_ref, wr_ref, ids_ref, slot_ref, cols_ref, cnt_ref):
    tok = x_ref.shape[0]
    n_exp = wr_ref.shape[0]
    w = wr_ref[...]
    w_hi = w.astype(BF16)
    rest = w - w_hi.astype(F32)
    w_mid = rest.astype(BF16)
    w_lo = (rest - w_mid.astype(F32)).astype(BF16)
    x = x_ref[...]
    nt = (((1,), (1,)), ((), ()))
    w_all = jnp.concatenate([w_hi, w_mid, w_lo], axis=0)
    parts = lax.dot_general(w_all, x, nt, preferred_element_type=F32)
    logits = parts[:n_exp] + (parts[n_exp : 2 * n_exp] + parts[2 * n_exp :])
    ids = ids_ref[...]
    id_a, id_b = ids[0:1], ids[1:2]
    row = lax.broadcasted_iota(I32, (n_exp, tok), 0)
    oh_a, oh_b = row == id_a, row == id_b
    zero = jnp.zeros((), F32)
    l_a = jnp.sum(jnp.where(oh_a, logits, zero), axis=0, keepdims=True)
    l_b = jnp.sum(jnp.where(oh_b, logits, zero), axis=0, keepdims=True)
    top = jnp.maximum(l_a, l_b)
    e_a, e_b = jnp.exp(l_a - top), jnp.exp(l_b - top)
    g_a, g_b = e_a / (e_a + e_b), e_b / (e_a + e_b)
    chosen = jnp.where(oh_a | oh_b, 1.0, 0.0).astype(F32)
    width = 256
    tri = (lax.broadcasted_iota(I32, (width, width), 0) < lax.broadcasted_iota(I32, (width, width), 1))
    tri = jnp.where(tri, 1.0, 0.0).astype(BF16)
    before = jnp.zeros((n_exp, 1), F32)
    ranks = []
    for k in range(tok // width):
        blk = chosen[:, k * width : (k + 1) * width]
        ranks.append(_dot(blk.astype(BF16), tri) + before)
        before = before + jnp.sum(blk, axis=1, keepdims=True)
    rank = jnp.concatenate(ranks, axis=1)
    cnt_ref[...] = jnp.broadcast_to(before, cnt_ref.shape).astype(I32)

    def slot_of(ident, onehot):
        here = jnp.sum(jnp.where(onehot, rank, zero), axis=0, keepdims=True)
        dev = ident // local_count
        lower = (row < ident) & (row >= dev * local_count)
        base = jnp.sum(jnp.where(lower, jnp.broadcast_to(before, (n_exp, tok)), zero), axis=0, keepdims=True)
        return dev.astype(F32) * row_cap + here + base

    s_a, s_b = slot_of(id_a, oh_a), slot_of(id_b, oh_b)
    both = jnp.concatenate([s_a, s_b, g_a, g_b, s_a, s_b, g_a, g_b], axis=0)
    slot_ref[...] = both.astype(I32)
    cols_ref[...] = both.T


SLOT_TILE = 32
PACK_GROUP = 8
SUM_GROUP = 16


def list_tiles(n_dev, size, start, counts_ref, list_ref, visit=None):
    per = size // SLOT_TILE

    def collect(i, cnt):
        hit = counts_ref[i // per] > start + (i % per) * SLOT_TILE

        @pl.when(hit)
        def _():
            list_ref[cnt] = i
            if visit is not None:
                visit(i, cnt)

        return cnt + hit.astype(I32)

    return lax.fori_loop(0, n_dev * per, collect, jnp.int32(0))


def first_slot(i, size, start, row_cap):
    per = size // SLOT_TILE
    return (i // per) * row_cap + start + (i % per) * SLOT_TILE


def pack_kernel(row_cap, chunks, counts_ref, slot_ref, x_ref, *refs):
    out_refs, list_ref = refs[:-1], refs[-1]
    tok = x_ref.shape[0]
    for (start, size), out_ref in zip(chunks, out_refs):
        n_dev = out_ref.shape[0] // size
        list_ref[0] = 0
        cnt = list_tiles(n_dev, size, start, counts_ref, list_ref)
        last = jnp.maximum(cnt - 1, 0)

        @pl.loop(0, (cnt + PACK_GROUP - 1) // PACK_GROUP)
        def _(g):
            tiles = [list_ref[jnp.minimum(g * PACK_GROUP + j, last)] for j in range(PACK_GROUP)]
            pos = lax.broadcasted_iota(I32, (SLOT_TILE, tok), 0)
            want = jnp.concatenate([pos + first_slot(i, size, start, row_cap) for i in tiles], axis=0)
            hit = (want == slot_ref[0:1, :]) | (want == slot_ref[1:2, :])
            pick = jnp.where(hit, 1.0, 0.0).astype(BF16)
            rows = _dot(pick, x_ref[...]).astype(BF16)
            for j, i in enumerate(tiles):
                at = pl.ds(pl.multiple_of(i * SLOT_TILE, SLOT_TILE), SLOT_TILE)
                out_ref[at, :] = rows[j * SLOT_TILE : (j + 1) * SLOT_TILE]


WIDE = 512
STEP = 256


def ffn_kernel(start, size, n_src, bound_ref, x_ref, w1_hbm, w3_hbm, w2_hbm, out_ref, w1, w3, w2, xbuf, hbuf, list_ref, used_ref, sems):
    n_loc, _, ff = w1.shape
    n_f = ff // WIDE
    per = size // TILE

    def copy(e, which, f):
        cut = pl.ds(f * WIDE, WIDE)
        at = (e, cut) if which == 2 else (e, slice(None), cut)
        src, dst = ((w1_hbm, w1), (w3_hbm, w3), (w2_hbm, w2))[which]
        return pltpu.make_async_copy(src.at[at], dst.at[at], sems.at[e, which, f])

    @pl.loop(0, n_loc)
    def _(e):
        def need(s, any_):
            lo, hi = bound_ref[e, s], bound_ref[e + 1, s]
            return any_ | ((lo < start + size) & (hi > start) & (hi > lo)).astype(I32)

        used = lax.fori_loop(0, n_src, need, jnp.int32(0))
        used_ref[e] = used

        @pl.when(used > 0)
        def _():
            @pl.loop(0, n_f)
            def _(f):
                copy(e, 0, f).start()
                copy(e, 1, f).start()

            @pl.loop(0, n_f)
            def _(f):
                copy(e, 2, f).start()

    out_ref[...] = jnp.zeros_like(out_ref)

    @pl.loop(0, n_loc)
    def _(e):
        @pl.when(used_ref[e] > 0)
        def _():
            def collect(i, cnt):
                s = i // per
                t0 = start + (i % per) * TILE
                lo = bound_ref[e, s]
                hi = bound_ref[e + 1, s]
                hit = (lo < t0 + TILE) & (hi > t0) & (hi > lo)

                @pl.when(hit)
                def _():
                    list_ref[cnt] = i
                    here = pl.ds(pl.multiple_of(i * TILE, TILE), TILE)
                    xbuf[pl.ds(pl.multiple_of(cnt * TILE, TILE), TILE), :] = x_ref[here, :]

                return cnt + hit.astype(I32)

            cnt = lax.fori_loop(0, n_src * per, collect, jnp.int32(0))

            def columns(at, f):
                cut = pl.ds(f * WIDE if isinstance(f, int) else pl.multiple_of(f * WIDE, WIDE), WIDE)
                xb = xbuf[at, :]
                u = _dot(xb, w1[e, :, cut])
                v = _dot(xb, w3[e, :, cut])
                hbuf[:, cut] = (u * jax.nn.sigmoid(u) * v).astype(BF16)

            @pl.loop(0, n_f)
            def _(f):
                copy(e, 0, f).wait()
                copy(e, 1, f).wait()
                columns(pl.ds(0, STEP), f)

            @pl.loop(0, n_f)
            def _(f):
                copy(e, 2, f).wait()

            @pl.loop(0, (cnt * TILE + STEP - 1) // STEP)
            def _(g):
                at = pl.ds(pl.multiple_of(g * STEP, STEP), STEP)

                @pl.when(g > 0)
                def _():
                    for f in range(n_f):
                        columns(at, f)

                xbuf[at, :] = _dot(hbuf[...], w2[e]).astype(BF16)

            def put(k, _):
                i = list_ref[k]
                s = i // per
                t0 = start + (i % per) * TILE
                pos = t0 + lax.broadcasted_iota(I32, (TILE, 1), 0)
                own = (pos >= bound_ref[e, s]) & (pos < bound_ref[e + 1, s])
                at = pl.ds(pl.multiple_of(i * TILE, TILE), TILE)
                y = xbuf[pl.ds(pl.multiple_of(k * TILE, TILE), TILE), :]
                out_ref[at, :] = jnp.where(own, y, out_ref[at, :])
                return 0

            lax.fori_loop(0, cnt, put, 0)


def combine_kernel(row_cap, start, size, n_dev, has_acc, counts_ref, cols_ref, back_ref, *refs):
    if has_acc:
        acc_ref, out_ref, rows_ref, sum_ref, list_ref, cnt_ref = refs
    else:
        out_ref, rows_ref, sum_ref, list_ref, cnt_ref = refs
    group = SUM_GROUP * SLOT_TILE
    toks, dim = out_ref.shape

    @pl.when(pl.program_id(0) == 0)
    def _():
        def bring(i, k):
            src = pl.ds(pl.multiple_of(i * SLOT_TILE, SLOT_TILE), SLOT_TILE)
            rows_ref[pl.ds(pl.multiple_of(k * SLOT_TILE, SLOT_TILE), SLOT_TILE), :] = back_ref[src, :]

        cnt = list_tiles(n_dev, size, start, counts_ref, list_ref, bring)
        groups = (cnt + SUM_GROUP - 1) // SUM_GROUP
        cnt_ref[0] = groups

        @pl.loop(cnt, groups * SUM_GROUP)
        def _(k):
            list_ref[k] = -1
            rows_ref[pl.ds(pl.multiple_of(k * SLOT_TILE, SLOT_TILE), SLOT_TILE), :] = jnp.zeros((SLOT_TILE, dim), BF16)

    c = cols_ref[...]
    sum_ref[...] = acc_ref[...] if has_acc else jnp.zeros((toks, dim), F32)
    lane = lax.broadcasted_iota(I32, (1, group), 1)

    @pl.loop(0, cnt_ref[0])
    def _(g):
        rows = rows_ref[pl.ds(pl.multiple_of(g * group, group), group), :]
        ids = jnp.full((1, group), -1, I32)
        for j in range(SUM_GROUP):
            i = list_ref[g * SUM_GROUP + j]
            base = jnp.where(i < 0, -1 - group, first_slot(i, size, start, row_cap))
            ids = jnp.where(lane // SLOT_TILE == j, base + lane % SLOT_TILE, ids)
        ids = ids.astype(F32)
        add = 0.0
        for k in range(2):
            pick = jnp.where(ids == c[:, k : k + 1], 1.0, 0.0).astype(BF16)
            add = add + c[:, 2 + k : 3 + k] * _dot(pick, rows)
        sum_ref[...] += add

    out_ref[...] = sum_ref[...].astype(out_ref.dtype)


def _params(vmem_limit_bytes=VMEM_BYTES):
    return pltpu.CompilerParams(vmem_limit_bytes=vmem_limit_bytes)


def solution(mesh):
    n = mesh.shape["ep"]

    def body(x, w_router, ids, w1, w3, w2):
        tok, dim = x.shape
        local = w1.shape[0]
        ff = w1.shape[2]
        n_exp = n * local
        cap = 4 * tok // n
        slots, cols, counts = pl.pallas_call(
            functools.partial(route_kernel, local, cap),
            out_shape=(
                jax.ShapeDtypeStruct((8, tok), I32),
                jax.ShapeDtypeStruct((tok, 8), F32),
                jax.ShapeDtypeStruct((n_exp, 128), I32),
            ),
            compiler_params=_params(),
            name="route",
        )(x, w_router.T, ids.T)
        per_exp = lax.all_to_all(counts[:, 0].reshape(n, local), "ep", 0, 0, tiled=True)
        ends = jnp.cumsum(per_exp, axis=1).T
        bounds = jnp.concatenate([jnp.zeros((1, n), I32), ends], axis=0)
        dev_counts = jnp.sum(counts[:, 0].reshape(n, local), axis=1)
        smem = pl.BlockSpec(memory_space=pltpu.SMEM)
        vmem = pl.BlockSpec(memory_space=pltpu.VMEM)
        hbm = pl.BlockSpec(memory_space=pl.ANY)
        sends = []
        for part in (CHUNKS[:1], CHUNKS[1:]):
            total = sum(size for _, size in part)
            pack = pl.pallas_call(
                functools.partial(pack_kernel, cap, part),
                in_specs=[smem, vmem, vmem],
                out_specs=[vmem] * len(part),
                out_shape=[jax.ShapeDtypeStruct((n * size, dim), BF16) for _, size in part],
                scratch_shapes=[pltpu.SMEM((cap * n // SLOT_TILE,), I32)],
                compiler_params=_params(),
                cost_estimate=pl.CostEstimate(flops=2 * n * total * tok * dim, bytes_accessed=1, transcendentals=0),
            )
            sends += pack(dev_counts, slots, x)
        acc = None
        for index, (start, size) in enumerate(CHUNKS):
            got = lax.all_to_all(sends[index].reshape(n, size, dim), "ep", 0, 0, tiled=True)
            rows = n * size
            made = pl.pallas_call(
                functools.partial(ffn_kernel, start, size, n),
                in_specs=[smem, vmem, hbm, hbm, hbm],
                out_specs=vmem,
                scratch_shapes=[
                    pltpu.VMEM((local, dim, ff), BF16),
                    pltpu.VMEM((local, dim, ff), BF16),
                    pltpu.VMEM((local, ff, dim), BF16),
                    pltpu.VMEM((rows, dim), BF16),
                    pltpu.VMEM((STEP, ff), BF16),
                    pltpu.SMEM((rows // TILE,), I32),
                    pltpu.SMEM((local,), I32),
                    pltpu.SemaphoreType.DMA((local, 3, ff // WIDE)),
                ],
                out_shape=pltpu.VMEM((rows, dim), BF16),
                compiler_params=_params(FFN_VMEM),
                cost_estimate=pl.CostEstimate(flops=6 * rows * dim * ff, bytes_accessed=1, transcendentals=0),
            )
            got = pltpu.with_memory_space_constraint(got.reshape(rows, dim), pltpu.VMEM)
            made = made(bounds, got, *[pltpu.with_memory_space_constraint(w, pltpu.HBM) for w in (w1, w3, w2)])
            back = lax.all_to_all(made.reshape(n, size, dim), "ep", 0, 0, tiled=True).reshape(rows, dim)
            last = index == len(CHUNKS) - 1
            tb = 512
            tile_spec = pl.BlockSpec((tb, dim), lambda i, c: (i, 0))
            ins = [cols, back] + ([] if acc is None else [acc])
            specs = [pl.BlockSpec((tb, 8), lambda i, c: (i, 0)), pl.BlockSpec((rows, dim), lambda i, c: (0, 0))]
            combine = pl.pallas_call(
                functools.partial(combine_kernel, cap, start, size, n, acc is not None),
                grid_spec=pltpu.PrefetchScalarGridSpec(
                    num_scalar_prefetch=1,
                    grid=(tok // tb,),
                    in_specs=specs + ([] if acc is None else [tile_spec]),
                    out_specs=tile_spec,
                    scratch_shapes=[
                        pltpu.VMEM((rows, dim), BF16),
                        pltpu.VMEM((tb, dim), F32),
                        pltpu.SMEM((rows // SLOT_TILE,), I32),
                        pltpu.SMEM((1,), I32),
                    ],
                ),
                out_shape=jax.ShapeDtypeStruct((tok, dim), BF16 if last else F32),
                compiler_params=_params(),
                cost_estimate=pl.CostEstimate(flops=4 * rows * tok * dim, bytes_accessed=1, transcendentals=0),
            )
            acc = combine(dev_counts, *ins)
        return acc

    return jax.shard_map(
        body,
        mesh=mesh,
        in_specs=(P("ep", None), P(None, None), P("ep", None), P("ep", None, None), P("ep", None, None), P("ep", None, None)),
        out_specs=P("ep", None),
        check_vma=False,
    )
```

```python
import functools

import jax
import jax.numpy as jnp
from jax import lax
from jax.experimental import pallas as pl
from jax.experimental.pallas import tpu as pltpu
from jax.sharding import PartitionSpec as P


F32 = jnp.float32
BF16 = jnp.bfloat16
I32 = jnp.int32
TILE = 16
CHUNKS = ((0, 256), (256, 256))
VMEM_BYTES = 60 * 1024 * 1024


def _dot(a, b):
    return jnp.dot(a, b, preferred_element_type=F32)


def route_kernel(local_count, row_cap, x_ref, wr_ref, ids_ref, slot_ref, cols_ref, cnt_ref):
    tok = x_ref.shape[0]
    n_exp = wr_ref.shape[0]
    w = wr_ref[...]
    w_hi = w.astype(BF16)
    rest = w - w_hi.astype(F32)
    w_mid = rest.astype(BF16)
    w_lo = (rest - w_mid.astype(F32)).astype(BF16)
    x = x_ref[...]
    nt = (((1,), (1,)), ((), ()))
    w_all = jnp.concatenate([w_hi, w_mid, w_lo], axis=0)
    parts = lax.dot_general(w_all, x, nt, preferred_element_type=F32)
    logits = parts[:n_exp] + (parts[n_exp : 2 * n_exp] + parts[2 * n_exp :])
    ids = ids_ref[...]
    id_a, id_b = ids[0:1], ids[1:2]
    row = lax.broadcasted_iota(I32, (n_exp, tok), 0)
    oh_a, oh_b = row == id_a, row == id_b
    zero = jnp.zeros((), F32)
    l_a = jnp.sum(jnp.where(oh_a, logits, zero), axis=0, keepdims=True)
    l_b = jnp.sum(jnp.where(oh_b, logits, zero), axis=0, keepdims=True)
    top = jnp.maximum(l_a, l_b)
    e_a, e_b = jnp.exp(l_a - top), jnp.exp(l_b - top)
    g_a, g_b = e_a / (e_a + e_b), e_b / (e_a + e_b)
    chosen = jnp.where(oh_a | oh_b, 1.0, 0.0).astype(F32)
    width = 256
    tri = (lax.broadcasted_iota(I32, (width, width), 0) < lax.broadcasted_iota(I32, (width, width), 1))
    tri = jnp.where(tri, 1.0, 0.0).astype(BF16)
    before = jnp.zeros((n_exp, 1), F32)
    ranks = []
    for k in range(tok // width):
        blk = chosen[:, k * width : (k + 1) * width]
        ranks.append(_dot(blk.astype(BF16), tri) + before)
        before = before + jnp.sum(blk, axis=1, keepdims=True)
    rank = jnp.concatenate(ranks, axis=1)
    cnt_ref[...] = jnp.broadcast_to(before, cnt_ref.shape).astype(I32)

    def slot_of(ident, onehot):
        here = jnp.sum(jnp.where(onehot, rank, zero), axis=0, keepdims=True)
        dev = ident // local_count
        lower = (row < ident) & (row >= dev * local_count)
        base = jnp.sum(jnp.where(lower, jnp.broadcast_to(before, (n_exp, tok)), zero), axis=0, keepdims=True)
        return dev.astype(F32) * row_cap + here + base

    s_a, s_b = slot_of(id_a, oh_a), slot_of(id_b, oh_b)
    both = jnp.concatenate([s_a, s_b, g_a, g_b, s_a, s_b, g_a, g_b], axis=0)
    slot_ref[...] = both.astype(I32)
    cols_ref[...] = both.T


SLOT_TILE = 32
PACK_GROUP = 8
SUM_GROUP = 16


def list_tiles(n_dev, size, start, counts_ref, list_ref, visit=None):
    per = size // SLOT_TILE

    def collect(i, cnt):
        hit = counts_ref[i // per] > start + (i % per) * SLOT_TILE

        @pl.when(hit)
        def _():
            list_ref[cnt] = i
            if visit is not None:
                visit(i, cnt)

        return cnt + hit.astype(I32)

    return lax.fori_loop(0, n_dev * per, collect, jnp.int32(0))


def first_slot(i, size, start, row_cap):
    per = size // SLOT_TILE
    return (i // per) * row_cap + start + (i % per) * SLOT_TILE


def pack_kernel(row_cap, chunks, counts_ref, slot_ref, x_ref, *refs):
    out_refs, list_ref = refs[:-1], refs[-1]
    tok = x_ref.shape[0]
    for (start, size), out_ref in zip(chunks, out_refs):
        n_dev = out_ref.shape[0] // size
        list_ref[0] = 0
        cnt = list_tiles(n_dev, size, start, counts_ref, list_ref)
        last = jnp.maximum(cnt - 1, 0)

        @pl.loop(0, (cnt + PACK_GROUP - 1) // PACK_GROUP)
        def _(g):
            tiles = [list_ref[jnp.minimum(g * PACK_GROUP + j, last)] for j in range(PACK_GROUP)]
            pos = lax.broadcasted_iota(I32, (SLOT_TILE, tok), 0)
            want = jnp.concatenate([pos + first_slot(i, size, start, row_cap) for i in tiles], axis=0)
            hit = (want == slot_ref[0:1, :]) | (want == slot_ref[1:2, :])
            pick = jnp.where(hit, 1.0, 0.0).astype(BF16)
            rows = _dot(pick, x_ref[...]).astype(BF16)
            for j, i in enumerate(tiles):
                at = pl.ds(pl.multiple_of(i * SLOT_TILE, SLOT_TILE), SLOT_TILE)
                out_ref[at, :] = rows[j * SLOT_TILE : (j + 1) * SLOT_TILE]


WIDE = 512
GROUP = 16
STEP = GROUP * TILE


def ffn_kernel(start, size, n_src, bound_ref, x_hbm, w1_hbm, w3_hbm, w2_hbm, out_ref, x_ref, w1, w3, w2, xbuf, hbuf, list_ref, low_ref, high_ref, used_ref, sems, x_sems):
    n_loc, _, ff = w1.shape
    n_f = ff // WIDE
    per = size // TILE

    def copy(e, which, f):
        cut = pl.ds(f * WIDE, WIDE)
        at = (e, cut) if which == 2 else (e, slice(None), cut)
        src, dst = ((w1_hbm, w1), (w3_hbm, w3), (w2_hbm, w2))[which]
        return pltpu.make_async_copy(src.at[at], dst.at[at], sems.at[e, which, f])

    quarter = x_ref.shape[0] // 4

    def row_copy(q):
        at = pl.ds(q * quarter, quarter)
        return pltpu.make_async_copy(x_hbm.at[at], x_ref.at[at], x_sems.at[q])

    for q in range(4):
        row_copy(q).start()

    @pl.loop(0, n_loc)
    def _(e):
        def need(s, any_):
            lo, hi = bound_ref[e, s], bound_ref[e + 1, s]
            return any_ | ((lo < start + size) & (hi > start) & (hi > lo)).astype(I32)

        used = lax.fori_loop(0, n_src, need, jnp.int32(0))
        used_ref[e] = used

        @pl.when(used > 0)
        def _():
            @pl.loop(0, n_f)
            def _(f):
                copy(e, 0, f).start()
                copy(e, 1, f).start()

            @pl.loop(0, n_f)
            def _(f):
                copy(e, 2, f).start()

    out_ref[...] = jnp.zeros_like(out_ref)
    for q in range(4):
        row_copy(q).wait()

    @pl.loop(0, n_loc)
    def _(e):
        @pl.when(used_ref[e] > 0)
        def _():
            def collect(s, cnt):
                lo = jnp.clip(bound_ref[e, s] - start, 0, size)
                hi = jnp.clip(bound_ref[e + 1, s] - start, 0, size)
                t_lo = lo // TILE
                t_hi = jnp.where(hi > lo, (hi + TILE - 1) // TILE, t_lo)

                def add(t, k):
                    list_ref[k] = s * per + t
                    low_ref[k] = lo - t * TILE
                    high_ref[k] = hi - t * TILE
                    return k + 1

                return lax.fori_loop(t_lo, t_hi, add, cnt)

            cnt = lax.fori_loop(0, n_src, collect, jnp.int32(0))
            groups = (cnt + GROUP - 1) // GROUP

            @pl.loop(cnt, groups * GROUP)
            def _(k):
                list_ref[k] = 0
                low_ref[k] = 0
                high_ref[k] = 0

            def tile_of(g, j):
                return pl.ds(pl.multiple_of(list_ref[g * GROUP + j] * TILE, TILE), TILE)

            def columns(f):
                cut = pl.ds(f * WIDE if isinstance(f, int) else pl.multiple_of(f * WIDE, WIDE), WIDE)
                xb = xbuf[...]
                u = _dot(xb, w1[e, :, cut])
                v = _dot(xb, w3[e, :, cut])
                hbuf[:, cut] = (u * jax.nn.sigmoid(u) * v).astype(BF16)

            @pl.loop(0, groups)
            def _(g):
                for j in range(GROUP):
                    xbuf[j * TILE : (j + 1) * TILE, :] = x_ref[tile_of(g, j), :]

                @pl.when(g == 0)
                def _():
                    @pl.loop(0, n_f)
                    def _(f):
                        copy(e, 0, f).wait()
                        copy(e, 1, f).wait()
                        columns(f)

                    @pl.loop(0, n_f)
                    def _(f):
                        copy(e, 2, f).wait()

                @pl.when(g > 0)
                def _():
                    for f in range(n_f):
                        columns(f)

                y = _dot(hbuf[...], w2[e]).astype(BF16)
                row = lax.broadcasted_iota(I32, (TILE, 1), 0)
                for j in range(GROUP):
                    own = (row >= low_ref[g * GROUP + j]) & (row < high_ref[g * GROUP + j])
                    at = tile_of(g, j)
                    out_ref[at, :] = jnp.where(own, y[j * TILE : (j + 1) * TILE], out_ref[at, :])


def combine_kernel(row_cap, start, size, n_dev, has_acc, counts_ref, cols_ref, back_ref, *refs):
    if has_acc:
        acc_ref, out_ref, rows_ref, sum_ref, list_ref, cnt_ref = refs
    else:
        out_ref, rows_ref, sum_ref, list_ref, cnt_ref = refs
    group = SUM_GROUP * SLOT_TILE
    toks, dim = out_ref.shape

    @pl.when(pl.program_id(0) == 0)
    def _():
        cnt = list_tiles(n_dev, size, start, counts_ref, list_ref)
        groups = (cnt + SUM_GROUP - 1) // SUM_GROUP
        cnt_ref[0] = groups

        @pl.loop(cnt, groups * SUM_GROUP)
        def _(k):
            list_ref[k] = -1

    c = cols_ref[...]
    sum_ref[...] = acc_ref[...] if has_acc else jnp.zeros((toks, dim), F32)
    lane = lax.broadcasted_iota(I32, (1, group), 1)

    @pl.loop(0, cnt_ref[0])
    def _(g):
        ids = jnp.full((1, group), -1, I32)
        for j in range(SUM_GROUP):
            i = list_ref[g * SUM_GROUP + j]
            base = jnp.where(i < 0, -1 - group, first_slot(i, size, start, row_cap))
            ids = jnp.where(lane // SLOT_TILE == j, base + lane % SLOT_TILE, ids)
            src = pl.ds(pl.multiple_of(jnp.maximum(i, 0) * SLOT_TILE, SLOT_TILE), SLOT_TILE)
            rows_ref[j * SLOT_TILE : (j + 1) * SLOT_TILE, :] = back_ref[src, :]
        rows = rows_ref[...]
        ids = ids.astype(F32)
        add = 0.0
        for k in range(2):
            pick = jnp.where(ids == c[:, k : k + 1], 1.0, 0.0).astype(BF16)
            add = add + c[:, 2 + k : 3 + k] * _dot(pick, rows)
        sum_ref[...] += add

    out_ref[...] = sum_ref[...].astype(out_ref.dtype)


def _params(vmem_limit_bytes=VMEM_BYTES):
    return pltpu.CompilerParams(vmem_limit_bytes=vmem_limit_bytes)


def solution(mesh):
    n = mesh.shape["ep"]

    def body(x, w_router, ids, w1, w3, w2):
        tok, dim = x.shape
        local = w1.shape[0]
        ff = w1.shape[2]
        n_exp = n * local
        cap = 4 * tok // n
        slots, cols, counts = pl.pallas_call(
            functools.partial(route_kernel, local, cap),
            out_shape=(
                jax.ShapeDtypeStruct((8, tok), I32),
                jax.ShapeDtypeStruct((tok, 8), F32),
                jax.ShapeDtypeStruct((n_exp, 128), I32),
            ),
            compiler_params=_params(),
            name="route",
        )(x, w_router.T, ids.T)
        per_exp = lax.all_to_all(counts[:, 0].reshape(n, local), "ep", 0, 0, tiled=True)
        ends = jnp.cumsum(per_exp, axis=1).T
        bounds = jnp.concatenate([jnp.zeros((1, n), I32), ends], axis=0)
        dev_counts = jnp.sum(counts[:, 0].reshape(n, local), axis=1)
        smem = pl.BlockSpec(memory_space=pltpu.SMEM)
        vmem = pl.BlockSpec(memory_space=pltpu.VMEM)
        hbm = pl.BlockSpec(memory_space=pl.ANY)
        sends = []
        for part in (CHUNKS[:1], CHUNKS[1:]):
            total = sum(size for _, size in part)
            pack = pl.pallas_call(
                functools.partial(pack_kernel, cap, part),
                in_specs=[smem, vmem, vmem],
                out_specs=[vmem] * len(part),
                out_shape=[jax.ShapeDtypeStruct((n * size, dim), BF16) for _, size in part],
                scratch_shapes=[pltpu.SMEM((cap * n // SLOT_TILE,), I32)],
                compiler_params=_params(),
                cost_estimate=pl.CostEstimate(flops=2 * n * total * tok * dim, bytes_accessed=1, transcendentals=0),
            )
            sends += pack(dev_counts, slots, x)
        acc = None
        for index, (start, size) in enumerate(CHUNKS):
            got = lax.all_to_all(sends[index].reshape(n, size, dim), "ep", 0, 0, tiled=True)
            rows = n * size
            made = pl.pallas_call(
                functools.partial(ffn_kernel, start, size, n),
                in_specs=[smem, hbm, hbm, hbm, hbm],
                out_specs=vmem,
                scratch_shapes=[
                    pltpu.VMEM((rows, dim), BF16),
                    pltpu.VMEM((local, dim, ff), BF16),
                    pltpu.VMEM((local, dim, ff), BF16),
                    pltpu.VMEM((local, ff, dim), BF16),
                    pltpu.VMEM((STEP, dim), BF16),
                    pltpu.VMEM((STEP, ff), BF16),
                    pltpu.SMEM((rows // TILE + GROUP,), I32),
                    pltpu.SMEM((rows // TILE + GROUP,), I32),
                    pltpu.SMEM((rows // TILE + GROUP,), I32),
                    pltpu.SMEM((local,), I32),
                    pltpu.SemaphoreType.DMA((local, 3, ff // WIDE)),
                    pltpu.SemaphoreType.DMA((4,)),
                ],
                out_shape=jax.ShapeDtypeStruct((rows, dim), BF16),
                compiler_params=_params(),
                cost_estimate=pl.CostEstimate(flops=6 * rows * dim * ff, bytes_accessed=1, transcendentals=0),
            )
            made = made(bounds, got.reshape(rows, dim), w1, w3, w2)
            back = lax.all_to_all(made.reshape(n, size, dim), "ep", 0, 0, tiled=True).reshape(rows, dim)
            last = index == len(CHUNKS) - 1
            tb = 512
            tile_spec = pl.BlockSpec((tb, dim), lambda i, c: (i, 0))
            ins = [cols, back] + ([] if acc is None else [acc])
            specs = [pl.BlockSpec((tb, 8), lambda i, c: (i, 0)), pl.BlockSpec((rows, dim), lambda i, c: (0, 0))]
            combine = pl.pallas_call(
                functools.partial(combine_kernel, cap, start, size, n, acc is not None),
                grid_spec=pltpu.PrefetchScalarGridSpec(
                    num_scalar_prefetch=1,
                    grid=(tok // tb,),
                    in_specs=specs + ([] if acc is None else [tile_spec]),
                    out_specs=tile_spec,
                    scratch_shapes=[
                        pltpu.VMEM((SUM_GROUP * SLOT_TILE, dim), BF16),
                        pltpu.VMEM((tb, dim), F32),
                        pltpu.SMEM((rows // SLOT_TILE,), I32),
                        pltpu.SMEM((1,), I32),
                    ],
                ),
                out_shape=jax.ShapeDtypeStruct((tok, dim), BF16 if last else F32),
                compiler_params=_params(),
                cost_estimate=pl.CostEstimate(flops=4 * rows * tok * dim, bytes_accessed=1, transcendentals=0),
            )
            acc = combine(dev_counts, *ins)
        return acc

    return jax.shard_map(
        body,
        mesh=mesh,
        in_specs=(P("ep", None), P(None, None), P("ep", None), P("ep", None, None), P("ep", None, None), P("ep", None, None)),
        out_specs=P("ep", None),
        check_vma=False,
    )
```

```python
import functools

import jax
import jax.numpy as jnp
from jax import lax
from jax.experimental import pallas as pl
from jax.experimental.pallas import tpu as pltpu
from jax.sharding import PartitionSpec as P


F32 = jnp.float32
BF16 = jnp.bfloat16
I32 = jnp.int32
TILE = 16
CHUNKS = ((0, 256), (256, 256))
VMEM_BYTES = 60 * 1024 * 1024


def _dot(a, b):
    return jnp.dot(a, b, preferred_element_type=F32)


def route_kernel(local_count, row_cap, x_ref, wr_ref, ids_ref, slot_ref, cols_ref, cnt_ref):
    tok = x_ref.shape[0]
    n_exp = wr_ref.shape[0]
    w = wr_ref[...]
    w_hi = w.astype(BF16)
    rest = w - w_hi.astype(F32)
    w_mid = rest.astype(BF16)
    w_lo = (rest - w_mid.astype(F32)).astype(BF16)
    x = x_ref[...]
    nt = (((1,), (1,)), ((), ()))
    w_all = jnp.concatenate([w_hi, w_mid, w_lo], axis=0)
    parts = lax.dot_general(w_all, x, nt, preferred_element_type=F32)
    logits = parts[:n_exp] + (parts[n_exp : 2 * n_exp] + parts[2 * n_exp :])
    ids = ids_ref[...]
    id_a, id_b = ids[0:1], ids[1:2]
    row = lax.broadcasted_iota(I32, (n_exp, tok), 0)
    oh_a, oh_b = row == id_a, row == id_b
    zero = jnp.zeros((), F32)
    l_a = jnp.sum(jnp.where(oh_a, logits, zero), axis=0, keepdims=True)
    l_b = jnp.sum(jnp.where(oh_b, logits, zero), axis=0, keepdims=True)
    top = jnp.maximum(l_a, l_b)
    e_a, e_b = jnp.exp(l_a - top), jnp.exp(l_b - top)
    g_a, g_b = e_a / (e_a + e_b), e_b / (e_a + e_b)
    chosen = jnp.where(oh_a | oh_b, 1.0, 0.0).astype(F32)
    width = 256
    tri = (lax.broadcasted_iota(I32, (width, width), 0) < lax.broadcasted_iota(I32, (width, width), 1))
    tri = jnp.where(tri, 1.0, 0.0).astype(BF16)
    before = jnp.zeros((n_exp, 1), F32)
    ranks = []
    for k in range(tok // width):
        blk = chosen[:, k * width : (k + 1) * width]
        ranks.append(_dot(blk.astype(BF16), tri) + before)
        before = before + jnp.sum(blk, axis=1, keepdims=True)
    rank = jnp.concatenate(ranks, axis=1)
    cnt_ref[...] = jnp.broadcast_to(before, cnt_ref.shape).astype(I32)

    def slot_of(ident, onehot):
        here = jnp.sum(jnp.where(onehot, rank, zero), axis=0, keepdims=True)
        dev = ident // local_count
        lower = (row < ident) & (row >= dev * local_count)
        base = jnp.sum(jnp.where(lower, jnp.broadcast_to(before, (n_exp, tok)), zero), axis=0, keepdims=True)
        return dev.astype(F32) * row_cap + here + base

    s_a, s_b = slot_of(id_a, oh_a), slot_of(id_b, oh_b)
    both = jnp.concatenate([s_a, s_b, g_a, g_b, s_a, s_b, g_a, g_b], axis=0)
    slot_ref[...] = both.astype(I32)
    cols_ref[...] = both.T


SLOT_TILE = 32
SUM_GROUP = 16


def list_tiles(n_dev, size, start, counts_ref, list_ref, visit=None):
    per = size // SLOT_TILE

    def collect(i, cnt):
        hit = counts_ref[i // per] > start + (i % per) * SLOT_TILE

        @pl.when(hit)
        def _():
            list_ref[cnt] = i
            if visit is not None:
                visit(i, cnt)

        return cnt + hit.astype(I32)

    return lax.fori_loop(0, n_dev * per, collect, jnp.int32(0))


def first_slot(i, size, start, row_cap):
    per = size // SLOT_TILE
    return (i // per) * row_cap + start + (i % per) * SLOT_TILE


WIDE = 512
GROUP = 16
STEP = GROUP * TILE


MESH = pl.DeviceIdType.MESH


def partner(me, offset):
    other = me
    for bit in (1, 2, 4, 8):
        other = other + ((offset // bit) % 2) * (bit - 2 * bit * ((me // bit) % 2))
    return other


def pair_of(p):
    j, r = (p - 1) // 2, (p - 1) % 2
    near = 8 - 4 * j + 2 * (j // 2)
    return 14 - near + r, near + r


def ship_kernel(row_cap, n_dev, chunks, slot_ref, x_ref, got_ref, next_ref, sbuf, vbuf, send_sems, recv_sems, own_sem, next_sems):
    me = lax.axis_index("ep")
    tok = x_ref.shape[0]
    (start, size), (start1, size1) = chunks

    def pack(dev, first, rows):
        want = lax.broadcasted_iota(I32, (rows, tok), 0) + (dev * row_cap + first)
        hit = (want == slot_ref[0:1, :]) | (want == slot_ref[1:2, :])
        pick = jnp.where(hit, 1.0, 0.0).astype(BF16)
        return _dot(pick, x_ref[...]).astype(BF16)

    def send(k):
        return pltpu.make_async_remote_copy(
            src_ref=sbuf.at[k],
            dst_ref=got_ref.at[me],
            send_sem=send_sems.at[k],
            recv_sem=recv_sems.at[k],
            device_id=(partner(me, k),),
            device_id_type=MESH,
        )

    def keep(d):
        return pltpu.make_async_copy(vbuf.at[d], next_ref.at[d], next_sems.at[d])

    def pack_first(k0, k1):
        @pl.loop(0, 2)
        def _(r):
            k = k0 + r * (k1 - k0)
            sbuf[k] = pack(partner(me, k), start, size)

    barrier = pltpu.get_barrier_semaphore()
    for k in range(1, n_dev):
        pl.semaphore_signal(barrier, inc=1, device_id=(partner(me, k),), device_id_type=MESH)
    pack_first(14, 15)
    pl.semaphore_wait(barrier, n_dev - 1)
    send(14).start()
    send(15).start()
    pack_first(6, 8)
    pack_first(0, 1)

    @pl.loop(1, 7)
    def _(p):
        k0, k1 = pair_of(p)

        @pl.when(p <= 2)
        def _():
            send(13 + p).wait_send()

        @pl.when(p >= 3)
        def _():
            for k in pair_of(p - 2):
                send(k).wait_send()

        send(k0).start()
        send(k1).start()

        @pl.when(p < 6)
        def _():
            pack_first(*pair_of(p + 1))

        @pl.loop((n_dev * (p - 1)) // 6, (n_dev * p) // 6)
        def _(d):
            vbuf[d] = pack(d, start1, size1)

            @pl.when(d > 0)
            def _():
                keep(d - 1).start()

    keep(n_dev - 1).start()
    send(1).start()
    own = pltpu.make_async_copy(sbuf.at[0], got_ref.at[me], own_sem)
    own.start()
    for p in (5, 6):
        for k in pair_of(p):
            send(k).wait_send()
    send(1).wait_send()
    own.wait()

    @pl.loop(0, n_dev)
    def _(d):
        keep(d).wait()

    @pl.loop(1, n_dev)
    def _(k):
        send(k).wait_recv()


def ffn_kernel(start, size, n_src, bound_ref, x_hbm, w1_hbm, w3_hbm, w2_hbm, out_ref, x_ref, w1, w3, w2, xbuf, hbuf, list_ref, low_ref, high_ref, used_ref, sems, x_sems):
    n_loc, _, ff = w1.shape
    n_f = ff // WIDE
    per = size // TILE

    def copy(e, which, f):
        cut = pl.ds(f * WIDE, WIDE)
        at = (e, cut) if which == 2 else (e, slice(None), cut)
        src, dst = ((w1_hbm, w1), (w3_hbm, w3), (w2_hbm, w2))[which]
        return pltpu.make_async_copy(src.at[at], dst.at[at], sems.at[e, which, f])

    quarter = x_ref.shape[0] // 4

    def row_copy(q):
        at = pl.ds(q * quarter, quarter)
        return pltpu.make_async_copy(x_hbm.at[at], x_ref.at[at], x_sems.at[q])

    for q in range(4):
        row_copy(q).start()

    @pl.loop(0, n_loc)
    def _(e):
        def need(s, any_):
            lo, hi = bound_ref[e, s], bound_ref[e + 1, s]
            return any_ | ((lo < start + size) & (hi > start) & (hi > lo)).astype(I32)

        used = lax.fori_loop(0, n_src, need, jnp.int32(0))
        used_ref[e] = used

        @pl.when(used > 0)
        def _():
            @pl.loop(0, n_f)
            def _(f):
                copy(e, 0, f).start()
                copy(e, 1, f).start()

            @pl.loop(0, n_f)
            def _(f):
                copy(e, 2, f).start()

    out_ref[...] = jnp.zeros_like(out_ref)
    for q in range(4):
        row_copy(q).wait()

    @pl.loop(0, n_loc)
    def _(e):
        @pl.when(used_ref[e] > 0)
        def _():
            def collect(s, cnt):
                lo = jnp.clip(bound_ref[e, s] - start, 0, size)
                hi = jnp.clip(bound_ref[e + 1, s] - start, 0, size)
                t_lo = lo // TILE
                t_hi = jnp.where(hi > lo, (hi + TILE - 1) // TILE, t_lo)

                def add(t, k):
                    list_ref[k] = s * per + t
                    low_ref[k] = lo - t * TILE
                    high_ref[k] = hi - t * TILE
                    return k + 1

                return lax.fori_loop(t_lo, t_hi, add, cnt)

            cnt = lax.fori_loop(0, n_src, collect, jnp.int32(0))
            groups = (cnt + GROUP - 1) // GROUP

            @pl.loop(cnt, groups * GROUP)
            def _(k):
                list_ref[k] = 0
                low_ref[k] = 0
                high_ref[k] = 0

            def tile_of(g, j):
                return pl.ds(pl.multiple_of(list_ref[g * GROUP + j] * TILE, TILE), TILE)

            def columns(f):
                cut = pl.ds(f * WIDE if isinstance(f, int) else pl.multiple_of(f * WIDE, WIDE), WIDE)
                xb = xbuf[...]
                u = _dot(xb, w1[e, :, cut])
                v = _dot(xb, w3[e, :, cut])
                hbuf[:, cut] = (u * jax.nn.sigmoid(u) * v).astype(BF16)

            @pl.loop(0, groups)
            def _(g):
                for j in range(GROUP):
                    xbuf[j * TILE : (j + 1) * TILE, :] = x_ref[tile_of(g, j), :]

                @pl.when(g == 0)
                def _():
                    @pl.loop(0, n_f)
                    def _(f):
                        copy(e, 0, f).wait()
                        copy(e, 1, f).wait()
                        columns(f)

                    @pl.loop(0, n_f)
                    def _(f):
                        copy(e, 2, f).wait()

                @pl.when(g > 0)
                def _():
                    for f in range(n_f):
                        columns(f)

                y = _dot(hbuf[...], w2[e]).astype(BF16)
                row = lax.broadcasted_iota(I32, (TILE, 1), 0)
                for j in range(GROUP):
                    own = (row >= low_ref[g * GROUP + j]) & (row < high_ref[g * GROUP + j])
                    at = tile_of(g, j)
                    out_ref[at, :] = jnp.where(own, y[j * TILE : (j + 1) * TILE], out_ref[at, :])


def combine_kernel(row_cap, start, size, n_dev, has_acc, counts_ref, cols_ref, back_ref, *refs):
    if has_acc:
        acc_ref, out_ref, rows_ref, sum_ref, list_ref, cnt_ref = refs
    else:
        out_ref, rows_ref, sum_ref, list_ref, cnt_ref = refs
    group = SUM_GROUP * SLOT_TILE
    toks, dim = out_ref.shape

    @pl.when(pl.program_id(0) == 0)
    def _():
        cnt = list_tiles(n_dev, size, start, counts_ref, list_ref)
        groups = (cnt + SUM_GROUP - 1) // SUM_GROUP
        cnt_ref[0] = groups

        @pl.loop(cnt, groups * SUM_GROUP)
        def _(k):
            list_ref[k] = -1

    c = cols_ref[...]
    sum_ref[...] = acc_ref[...] if has_acc else jnp.zeros((toks, dim), F32)
    lane = lax.broadcasted_iota(I32, (1, group), 1)

    @pl.loop(0, cnt_ref[0])
    def _(g):
        ids = jnp.full((1, group), -1, I32)
        for j in range(SUM_GROUP):
            i = list_ref[g * SUM_GROUP + j]
            base = jnp.where(i < 0, -1 - group, first_slot(i, size, start, row_cap))
            ids = jnp.where(lane // SLOT_TILE == j, base + lane % SLOT_TILE, ids)
            src = pl.ds(pl.multiple_of(jnp.maximum(i, 0) * SLOT_TILE, SLOT_TILE), SLOT_TILE)
            rows_ref[j * SLOT_TILE : (j + 1) * SLOT_TILE, :] = back_ref[src, :]
        rows = rows_ref[...]
        ids = ids.astype(F32)
        add = 0.0
        for k in range(2):
            pick = jnp.where(ids == c[:, k : k + 1], 1.0, 0.0).astype(BF16)
            add = add + c[:, 2 + k : 3 + k] * _dot(pick, rows)
        sum_ref[...] += add

    out_ref[...] = sum_ref[...].astype(out_ref.dtype)


def _params(vmem_limit_bytes=VMEM_BYTES):
    return pltpu.CompilerParams(vmem_limit_bytes=vmem_limit_bytes)


def solution(mesh):
    n = mesh.shape["ep"]

    def body(x, w_router, ids, w1, w3, w2):
        tok, dim = x.shape
        local = w1.shape[0]
        ff = w1.shape[2]
        n_exp = n * local
        cap = 4 * tok // n
        slots, cols, counts = pl.pallas_call(
            functools.partial(route_kernel, local, cap),
            out_shape=(
                jax.ShapeDtypeStruct((8, tok), I32),
                jax.ShapeDtypeStruct((tok, 8), F32),
                jax.ShapeDtypeStruct((n_exp, 128), I32),
            ),
            compiler_params=_params(),
            name="route",
        )(x, w_router.T, ids.T)
        every = lax.all_gather(counts[:, :1].reshape(n, local), "ep", axis=0)
        per_exp = lax.dynamic_index_in_dim(every, lax.axis_index("ep"), axis=1, keepdims=False)
        ends = jnp.cumsum(per_exp, axis=1).T
        bounds = jnp.concatenate([jnp.zeros((1, n), I32), ends], axis=0)
        dev_counts = jnp.sum(counts[:, 0].reshape(n, local), axis=1)
        smem = pl.BlockSpec(memory_space=pltpu.SMEM)
        vmem = pl.BlockSpec(memory_space=pltpu.VMEM)
        hbm = pl.BlockSpec(memory_space=pl.ANY)
        ship = pl.pallas_call(
            functools.partial(ship_kernel, cap, n, CHUNKS),
            in_specs=[vmem, vmem],
            out_specs=[hbm, hbm],
            out_shape=[jax.ShapeDtypeStruct((n, size, dim), BF16) for _, size in CHUNKS],
            scratch_shapes=[
                pltpu.VMEM((n, CHUNKS[0][1], dim), BF16),
                pltpu.VMEM((n, CHUNKS[1][1], dim), BF16),
                pltpu.SemaphoreType.DMA((n,)),
                pltpu.SemaphoreType.DMA((n,)),
                pltpu.SemaphoreType.DMA,
                pltpu.SemaphoreType.DMA((n,)),
            ],
            compiler_params=pltpu.CompilerParams(
                vmem_limit_bytes=VMEM_BYTES, collective_id=0, has_side_effects=True
            ),
            cost_estimate=pl.CostEstimate(flops=10**11, bytes_accessed=1, transcendentals=0),
            name="ship",
        )
        first_rows, second_rows = ship(slots, x)
        acc = None
        for index, (start, size) in enumerate(CHUNKS):
            if index == 0:
                got = first_rows
            else:
                got = lax.all_to_all(second_rows, "ep", 0, 0, tiled=True)
            rows = n * size
            made = pl.pallas_call(
                functools.partial(ffn_kernel, start, size, n),
                in_specs=[smem, hbm, hbm, hbm, hbm],
                out_specs=vmem,
                scratch_shapes=[
                    pltpu.VMEM((rows, dim), BF16),
                    pltpu.VMEM((local, dim, ff), BF16),
                    pltpu.VMEM((local, dim, ff), BF16),
                    pltpu.VMEM((local, ff, dim), BF16),
                    pltpu.VMEM((STEP, dim), BF16),
                    pltpu.VMEM((STEP, ff), BF16),
                    pltpu.SMEM((rows // TILE + GROUP,), I32),
                    pltpu.SMEM((rows // TILE + GROUP,), I32),
                    pltpu.SMEM((rows // TILE + GROUP,), I32),
                    pltpu.SMEM((local,), I32),
                    pltpu.SemaphoreType.DMA((local, 3, ff // WIDE)),
                    pltpu.SemaphoreType.DMA((4,)),
                ],
                out_shape=jax.ShapeDtypeStruct((rows, dim), BF16),
                compiler_params=_params(),
                cost_estimate=pl.CostEstimate(flops=6 * rows * dim * ff, bytes_accessed=1, transcendentals=0),
            )
            made = made(bounds, got.reshape(rows, dim), w1, w3, w2)
            back = lax.all_to_all(made.reshape(n, size, dim), "ep", 0, 0, tiled=True).reshape(rows, dim)
            last = index == len(CHUNKS) - 1
            tb = 512
            tile_spec = pl.BlockSpec((tb, dim), lambda i, c: (i, 0))
            ins = [cols, back] + ([] if acc is None else [acc])
            specs = [pl.BlockSpec((tb, 8), lambda i, c: (i, 0)), pl.BlockSpec((rows, dim), lambda i, c: (0, 0))]
            combine = pl.pallas_call(
                functools.partial(combine_kernel, cap, start, size, n, acc is not None),
                grid_spec=pltpu.PrefetchScalarGridSpec(
                    num_scalar_prefetch=1,
                    grid=(tok // tb,),
                    in_specs=specs + ([] if acc is None else [tile_spec]),
                    out_specs=tile_spec,
                    scratch_shapes=[
                        pltpu.VMEM((SUM_GROUP * SLOT_TILE, dim), BF16),
                        pltpu.VMEM((tb, dim), F32),
                        pltpu.SMEM((rows // SLOT_TILE,), I32),
                        pltpu.SMEM((1,), I32),
                    ],
                ),
                out_shape=jax.ShapeDtypeStruct((tok, dim), BF16 if last else F32),
                compiler_params=_params(),
                cost_estimate=pl.CostEstimate(flops=4 * rows * tok * dim, bytes_accessed=1, transcendentals=0),
            )
            acc = combine(dev_counts, *ins)
        return acc

    return jax.shard_map(
        body,
        mesh=mesh,
        in_specs=(P("ep", None), P(None, None), P("ep", None), P("ep", None, None), P("ep", None, None), P("ep", None, None)),
        out_specs=P("ep", None),
        check_vma=False,
    )
```

```python
import functools

import jax
import jax.numpy as jnp
from jax import lax
from jax.experimental import pallas as pl
from jax.experimental.pallas import tpu as pltpu
from jax.sharding import PartitionSpec as P


F32 = jnp.float32
BF16 = jnp.bfloat16
I32 = jnp.int32
TILE = 16
CHUNKS = ((0, 256), (256, 256))
VMEM_BYTES = 60 * 1024 * 1024


def _dot(a, b):
    return jnp.dot(a, b, preferred_element_type=F32)


def route_kernel(local_count, row_cap, x_ref, wr_ref, ids_ref, slot_ref, cols_ref, cnt_ref):
    tok = x_ref.shape[0]
    n_exp = wr_ref.shape[0]
    w = wr_ref[...]
    w_hi = w.astype(BF16)
    rest = w - w_hi.astype(F32)
    w_mid = rest.astype(BF16)
    w_lo = (rest - w_mid.astype(F32)).astype(BF16)
    x = x_ref[...]
    nt = (((1,), (1,)), ((), ()))
    w_all = jnp.concatenate([w_hi, w_mid, w_lo], axis=0)
    parts = lax.dot_general(w_all, x, nt, preferred_element_type=F32)
    logits = parts[:n_exp] + (parts[n_exp : 2 * n_exp] + parts[2 * n_exp :])
    ids = ids_ref[...]
    id_a, id_b = ids[0:1], ids[1:2]
    row = lax.broadcasted_iota(I32, (n_exp, tok), 0)
    oh_a, oh_b = row == id_a, row == id_b
    zero = jnp.zeros((), F32)
    l_a = jnp.sum(jnp.where(oh_a, logits, zero), axis=0, keepdims=True)
    l_b = jnp.sum(jnp.where(oh_b, logits, zero), axis=0, keepdims=True)
    top = jnp.maximum(l_a, l_b)
    e_a, e_b = jnp.exp(l_a - top), jnp.exp(l_b - top)
    g_a, g_b = e_a / (e_a + e_b), e_b / (e_a + e_b)
    chosen = jnp.where(oh_a | oh_b, 1.0, 0.0).astype(F32)
    width = 256
    tri = (lax.broadcasted_iota(I32, (width, width), 0) < lax.broadcasted_iota(I32, (width, width), 1))
    tri = jnp.where(tri, 1.0, 0.0).astype(BF16)
    before = jnp.zeros((n_exp, 1), F32)
    ranks = []
    for k in range(tok // width):
        blk = chosen[:, k * width : (k + 1) * width]
        ranks.append(_dot(blk.astype(BF16), tri) + before)
        before = before + jnp.sum(blk, axis=1, keepdims=True)
    rank = jnp.concatenate(ranks, axis=1)
    cnt_ref[...] = jnp.broadcast_to(before, cnt_ref.shape).astype(I32)

    def slot_of(ident, onehot):
        here = jnp.sum(jnp.where(onehot, rank, zero), axis=0, keepdims=True)
        dev = ident // local_count
        lower = (row < ident) & (row >= dev * local_count)
        base = jnp.sum(jnp.where(lower, jnp.broadcast_to(before, (n_exp, tok)), zero), axis=0, keepdims=True)
        return dev.astype(F32) * row_cap + here + base

    s_a, s_b = slot_of(id_a, oh_a), slot_of(id_b, oh_b)
    both = jnp.concatenate([s_a, s_b, g_a, g_b, s_a, s_b, g_a, g_b], axis=0)
    slot_ref[...] = both.astype(I32)
    cols_ref[...] = both.T


SLOT_TILE = 32
SUM_GROUP = 16


def list_tiles(n_dev, size, start, counts_ref, list_ref, visit=None):
    per = size // SLOT_TILE

    def collect(i, cnt):
        hit = counts_ref[i // per] > start + (i % per) * SLOT_TILE

        @pl.when(hit)
        def _():
            list_ref[cnt] = i
            if visit is not None:
                visit(i, cnt)

        return cnt + hit.astype(I32)

    return lax.fori_loop(0, n_dev * per, collect, jnp.int32(0))


def first_slot(i, size, start, row_cap):
    per = size // SLOT_TILE
    return (i // per) * row_cap + start + (i % per) * SLOT_TILE


WIDE = 512
GROUP = 16
STEP = GROUP * TILE


MESH = pl.DeviceIdType.MESH


def partner(me, offset):
    other = me
    for bit in (1, 2, 4, 8):
        other = other + ((offset // bit) % 2) * (bit - 2 * bit * ((me // bit) % 2))
    return other


def pair_of(p):
    j, r = (p - 1) // 2, (p - 1) % 2
    near = 8 - 4 * j + 2 * (j // 2)
    return 14 - near + r, near + r


def ship_kernel(row_cap, n_dev, chunks, slot_ref, cnt_ref, x_ref, got_ref, next_ref, all_ref, sbuf, vbuf, send_sems, recv_sems, own_sem, next_sems, cs_sems, cr_sems, co_sem):
    me = lax.axis_index("ep")
    tok = x_ref.shape[0]
    (start, size), (start1, size1) = chunks

    def pack(dev, first, rows):
        want = lax.broadcasted_iota(I32, (rows, tok), 0) + (dev * row_cap + first)
        hit = (want == slot_ref[0:1, :]) | (want == slot_ref[1:2, :])
        pick = jnp.where(hit, 1.0, 0.0).astype(BF16)
        return _dot(pick, x_ref[...]).astype(BF16)

    def send(k):
        return pltpu.make_async_remote_copy(
            src_ref=sbuf.at[k],
            dst_ref=got_ref.at[me],
            send_sem=send_sems.at[k],
            recv_sem=recv_sems.at[k],
            device_id=(partner(me, k),),
            device_id_type=MESH,
        )

    def tell(k):
        return pltpu.make_async_remote_copy(
            src_ref=cnt_ref,
            dst_ref=all_ref.at[me],
            send_sem=cs_sems.at[k],
            recv_sem=cr_sems.at[k],
            device_id=(partner(me, k),),
            device_id_type=MESH,
        )

    own_counts = pltpu.make_async_copy(cnt_ref, all_ref.at[me], co_sem)

    def keep(d):
        return pltpu.make_async_copy(vbuf.at[d], next_ref.at[d], next_sems.at[d])

    def pack_first(k0, k1):
        @pl.loop(0, 2)
        def _(r):
            k = k0 + r * (k1 - k0)
            sbuf[k] = pack(partner(me, k), start, size)

    barrier = pltpu.get_barrier_semaphore()
    for k in range(1, n_dev):
        pl.semaphore_signal(barrier, inc=1, device_id=(partner(me, k),), device_id_type=MESH)
    pack_first(14, 15)
    pl.semaphore_wait(barrier, n_dev - 1)
    send(14).start()
    send(15).start()
    own_counts.start()

    @pl.loop(1, n_dev)
    def _(k):
        tell(k).start()

    pack_first(6, 8)
    pack_first(0, 1)

    @pl.loop(1, 7)
    def _(p):
        k0, k1 = pair_of(p)

        @pl.when(p <= 2)
        def _():
            send(13 + p).wait_send()

        @pl.when(p >= 3)
        def _():
            for k in pair_of(p - 2):
                send(k).wait_send()

        send(k0).start()
        send(k1).start()

        @pl.when(p < 6)
        def _():
            pack_first(*pair_of(p + 1))

        @pl.loop((n_dev * (p - 1)) // 6, (n_dev * p) // 6)
        def _(d):
            vbuf[d] = pack(d, start1, size1)

            @pl.when(d > 0)
            def _():
                keep(d - 1).start()

    keep(n_dev - 1).start()
    send(1).start()
    own = pltpu.make_async_copy(sbuf.at[0], got_ref.at[me], own_sem)
    own.start()
    for p in (5, 6):
        for k in pair_of(p):
            send(k).wait_send()
    send(1).wait_send()
    own.wait()
    own_counts.wait()

    @pl.loop(0, n_dev)
    def _(d):
        keep(d).wait()

    @pl.loop(1, n_dev)
    def _(k):
        tell(k).wait_send()
        tell(k).wait_recv()
        send(k).wait_recv()


def ffn_kernel(start, size, n_src, bound_ref, x_hbm, w1_hbm, w3_hbm, w2_hbm, out_ref, x_ref, w1, w3, w2, xbuf, hbuf, list_ref, low_ref, high_ref, used_ref, sems, x_sems):
    n_loc, _, ff = w1.shape
    n_f = ff // WIDE
    per = size // TILE

    def copy(e, which, f):
        cut = pl.ds(f * WIDE, WIDE)
        at = (e, cut) if which == 2 else (e, slice(None), cut)
        src, dst = ((w1_hbm, w1), (w3_hbm, w3), (w2_hbm, w2))[which]
        return pltpu.make_async_copy(src.at[at], dst.at[at], sems.at[e, which, f])

    quarter = x_ref.shape[0] // 4

    def row_copy(q):
        at = pl.ds(q * quarter, quarter)
        return pltpu.make_async_copy(x_hbm.at[at], x_ref.at[at], x_sems.at[q])

    for q in range(4):
        row_copy(q).start()

    @pl.loop(0, n_loc)
    def _(e):
        def need(s, any_):
            lo, hi = bound_ref[e, s], bound_ref[e + 1, s]
            return any_ | ((lo < start + size) & (hi > start) & (hi > lo)).astype(I32)

        used = lax.fori_loop(0, n_src, need, jnp.int32(0))
        used_ref[e] = used

        @pl.when(used > 0)
        def _():
            @pl.loop(0, n_f)
            def _(f):
                copy(e, 0, f).start()
                copy(e, 1, f).start()

            @pl.loop(0, n_f)
            def _(f):
                copy(e, 2, f).start()

    out_ref[...] = jnp.zeros_like(out_ref)
    for q in range(4):
        row_copy(q).wait()

    @pl.loop(0, n_loc)
    def _(e):
        @pl.when(used_ref[e] > 0)
        def _():
            def collect(s, cnt):
                lo = jnp.clip(bound_ref[e, s] - start, 0, size)
                hi = jnp.clip(bound_ref[e + 1, s] - start, 0, size)
                t_lo = lo // TILE
                t_hi = jnp.where(hi > lo, (hi + TILE - 1) // TILE, t_lo)

                def add(t, k):
                    list_ref[k] = s * per + t
                    low_ref[k] = lo - t * TILE
                    high_ref[k] = hi - t * TILE
                    return k + 1

                return lax.fori_loop(t_lo, t_hi, add, cnt)

            cnt = lax.fori_loop(0, n_src, collect, jnp.int32(0))
            groups = (cnt + GROUP - 1) // GROUP

            @pl.loop(cnt, groups * GROUP)
            def _(k):
                list_ref[k] = 0
                low_ref[k] = 0
                high_ref[k] = 0

            def tile_of(g, j):
                return pl.ds(pl.multiple_of(list_ref[g * GROUP + j] * TILE, TILE), TILE)

            def columns(f):
                cut = pl.ds(f * WIDE if isinstance(f, int) else pl.multiple_of(f * WIDE, WIDE), WIDE)
                xb = xbuf[...]
                u = _dot(xb, w1[e, :, cut])
                v = _dot(xb, w3[e, :, cut])
                hbuf[:, cut] = (u * jax.nn.sigmoid(u) * v).astype(BF16)

            @pl.loop(0, groups)
            def _(g):
                for j in range(GROUP):
                    xbuf[j * TILE : (j + 1) * TILE, :] = x_ref[tile_of(g, j), :]

                @pl.when(g == 0)
                def _():
                    @pl.loop(0, n_f)
                    def _(f):
                        copy(e, 0, f).wait()
                        copy(e, 1, f).wait()
                        columns(f)

                    @pl.loop(0, n_f)
                    def _(f):
                        copy(e, 2, f).wait()

                @pl.when(g > 0)
                def _():
                    for f in range(n_f):
                        columns(f)

                y = _dot(hbuf[...], w2[e]).astype(BF16)
                row = lax.broadcasted_iota(I32, (TILE, 1), 0)
                for j in range(GROUP):
                    own = (row >= low_ref[g * GROUP + j]) & (row < high_ref[g * GROUP + j])
                    at = tile_of(g, j)
                    out_ref[at, :] = jnp.where(own, y[j * TILE : (j + 1) * TILE], out_ref[at, :])


def combine_kernel(row_cap, start, size, n_dev, has_acc, counts_ref, cols_ref, back_ref, *refs):
    if has_acc:
        acc_ref, out_ref, rows_ref, sum_ref, list_ref, cnt_ref = refs
    else:
        out_ref, rows_ref, sum_ref, list_ref, cnt_ref = refs
    group = SUM_GROUP * SLOT_TILE
    toks, dim = out_ref.shape

    @pl.when(pl.program_id(0) == 0)
    def _():
        cnt = list_tiles(n_dev, size, start, counts_ref, list_ref)
        groups = (cnt + SUM_GROUP - 1) // SUM_GROUP
        cnt_ref[0] = groups

        @pl.loop(cnt, groups * SUM_GROUP)
        def _(k):
            list_ref[k] = -1

    c = cols_ref[...]
    sum_ref[...] = acc_ref[...] if has_acc else jnp.zeros((toks, dim), F32)
    lane = lax.broadcasted_iota(I32, (1, group), 1)

    @pl.loop(0, cnt_ref[0])
    def _(g):
        ids = jnp.full((1, group), -1, I32)
        for j in range(SUM_GROUP):
            i = list_ref[g * SUM_GROUP + j]
            base = jnp.where(i < 0, -1 - group, first_slot(i, size, start, row_cap))
            ids = jnp.where(lane // SLOT_TILE == j, base + lane % SLOT_TILE, ids)
            src = pl.ds(pl.multiple_of(jnp.maximum(i, 0) * SLOT_TILE, SLOT_TILE), SLOT_TILE)
            rows_ref[j * SLOT_TILE : (j + 1) * SLOT_TILE, :] = back_ref[src, :]
        rows = rows_ref[...]
        ids = ids.astype(F32)
        add = 0.0
        for k in range(2):
            pick = jnp.where(ids == c[:, k : k + 1], 1.0, 0.0).astype(BF16)
            add = add + c[:, 2 + k : 3 + k] * _dot(pick, rows)
        sum_ref[...] += add

    out_ref[...] = sum_ref[...].astype(out_ref.dtype)


def _params(vmem_limit_bytes=VMEM_BYTES):
    return pltpu.CompilerParams(vmem_limit_bytes=vmem_limit_bytes)


def solution(mesh):
    n = mesh.shape["ep"]

    def body(x, w_router, ids, w1, w3, w2):
        tok, dim = x.shape
        local = w1.shape[0]
        ff = w1.shape[2]
        n_exp = n * local
        cap = 4 * tok // n
        slots, cols, counts = pl.pallas_call(
            functools.partial(route_kernel, local, cap),
            out_shape=(
                jax.ShapeDtypeStruct((8, tok), I32),
                jax.ShapeDtypeStruct((tok, 8), F32),
                jax.ShapeDtypeStruct((n_exp, 128), I32),
            ),
            compiler_params=_params(),
            name="route",
        )(x, w_router.T, ids.T)
        dev_counts = jnp.sum(counts[:, 0].reshape(n, local), axis=1)
        smem = pl.BlockSpec(memory_space=pltpu.SMEM)
        vmem = pl.BlockSpec(memory_space=pltpu.VMEM)
        hbm = pl.BlockSpec(memory_space=pl.ANY)
        ship = pl.pallas_call(
            functools.partial(ship_kernel, cap, n, CHUNKS),
            in_specs=[vmem, vmem, vmem],
            out_specs=[hbm, hbm, hbm],
            out_shape=[jax.ShapeDtypeStruct((n, size, dim), BF16) for _, size in CHUNKS]
            + [jax.ShapeDtypeStruct((n,) + counts.shape, I32)],
            scratch_shapes=[
                pltpu.VMEM((n, CHUNKS[0][1], dim), BF16),
                pltpu.VMEM((n, CHUNKS[1][1], dim), BF16),
                pltpu.SemaphoreType.DMA((n,)),
                pltpu.SemaphoreType.DMA((n,)),
                pltpu.SemaphoreType.DMA,
                pltpu.SemaphoreType.DMA((n,)),
                pltpu.SemaphoreType.DMA((n,)),
                pltpu.SemaphoreType.DMA((n,)),
                pltpu.SemaphoreType.DMA,
            ],
            compiler_params=pltpu.CompilerParams(
                vmem_limit_bytes=VMEM_BYTES, collective_id=0, has_side_effects=True
            ),
            cost_estimate=pl.CostEstimate(flops=10**11, bytes_accessed=1, transcendentals=0),
            name="ship",
        )
        first_rows, second_rows, every = ship(slots, counts, x)
        at = lax.axis_index("ep") * local
        per_exp = lax.dynamic_slice(every, (0, at, 0), (n, local, 1))[:, :, 0]
        ends = jnp.cumsum(per_exp, axis=1).T
        bounds = jnp.concatenate([jnp.zeros((1, n), I32), ends], axis=0)
        acc = None
        for index, (start, size) in enumerate(CHUNKS):
            if index == 0:
                got = first_rows
            else:
                got = lax.all_to_all(second_rows, "ep", 0, 0, tiled=True)
            rows = n * size
            made = pl.pallas_call(
                functools.partial(ffn_kernel, start, size, n),
                in_specs=[smem, hbm, hbm, hbm, hbm],
                out_specs=vmem,
                scratch_shapes=[
                    pltpu.VMEM((rows, dim), BF16),
                    pltpu.VMEM((local, dim, ff), BF16),
                    pltpu.VMEM((local, dim, ff), BF16),
                    pltpu.VMEM((local, ff, dim), BF16),
                    pltpu.VMEM((STEP, dim), BF16),
                    pltpu.VMEM((STEP, ff), BF16),
                    pltpu.SMEM((rows // TILE + GROUP,), I32),
                    pltpu.SMEM((rows // TILE + GROUP,), I32),
                    pltpu.SMEM((rows // TILE + GROUP,), I32),
                    pltpu.SMEM((local,), I32),
                    pltpu.SemaphoreType.DMA((local, 3, ff // WIDE)),
                    pltpu.SemaphoreType.DMA((4,)),
                ],
                out_shape=jax.ShapeDtypeStruct((rows, dim), BF16),
                compiler_params=_params(),
                cost_estimate=pl.CostEstimate(flops=6 * rows * dim * ff, bytes_accessed=1, transcendentals=0),
            )
            made = made(bounds, got.reshape(rows, dim), w1, w3, w2)
            back = lax.all_to_all(made.reshape(n, size, dim), "ep", 0, 0, tiled=True).reshape(rows, dim)
            last = index == len(CHUNKS) - 1
            tb = 512
            tile_spec = pl.BlockSpec((tb, dim), lambda i, c: (i, 0))
            ins = [cols, back] + ([] if acc is None else [acc])
            specs = [pl.BlockSpec((tb, 8), lambda i, c: (i, 0)), pl.BlockSpec((rows, dim), lambda i, c: (0, 0))]
            combine = pl.pallas_call(
                functools.partial(combine_kernel, cap, start, size, n, acc is not None),
                grid_spec=pltpu.PrefetchScalarGridSpec(
                    num_scalar_prefetch=1,
                    grid=(tok // tb,),
                    in_specs=specs + ([] if acc is None else [tile_spec]),
                    out_specs=tile_spec,
                    scratch_shapes=[
                        pltpu.VMEM((SUM_GROUP * SLOT_TILE, dim), BF16),
                        pltpu.VMEM((tb, dim), F32),
                        pltpu.SMEM((rows // SLOT_TILE,), I32),
                        pltpu.SMEM((1,), I32),
                    ],
                ),
                out_shape=jax.ShapeDtypeStruct((tok, dim), BF16 if last else F32),
                compiler_params=_params(),
                cost_estimate=pl.CostEstimate(flops=4 * rows * tok * dim, bytes_accessed=1, transcendentals=0),
            )
            acc = combine(dev_counts, *ins)
        return acc

    return jax.shard_map(
        body,
        mesh=mesh,
        in_specs=(P("ep", None), P(None, None), P("ep", None), P("ep", None, None), P("ep", None, None), P("ep", None, None)),
        out_specs=P("ep", None),
        check_vma=False,
    )
```

```python
import functools

import jax
import jax.numpy as jnp
from jax import lax
from jax.experimental import pallas as pl
from jax.experimental.pallas import tpu as pltpu
from jax.sharding import PartitionSpec as P


F32 = jnp.float32
BF16 = jnp.bfloat16
I32 = jnp.int32
TILE = 16
CHUNKS = ((0, 256), (256, 256))
VMEM_BYTES = 60 * 1024 * 1024


def _dot(a, b):
    return jnp.dot(a, b, preferred_element_type=F32)


def route_kernel(local_count, row_cap, x_ref, wr_ref, ids_ref, slot_ref, cols_ref, cnt_ref):
    tok = x_ref.shape[0]
    n_exp = wr_ref.shape[0]
    w = wr_ref[...]
    w_hi = w.astype(BF16)
    rest = w - w_hi.astype(F32)
    w_mid = rest.astype(BF16)
    w_lo = (rest - w_mid.astype(F32)).astype(BF16)
    x = x_ref[...]
    nt = (((1,), (1,)), ((), ()))
    w_all = jnp.concatenate([w_hi, w_mid, w_lo], axis=0)
    parts = lax.dot_general(w_all, x, nt, preferred_element_type=F32)
    logits = parts[:n_exp] + (parts[n_exp : 2 * n_exp] + parts[2 * n_exp :])
    ids = ids_ref[...]
    id_a, id_b = ids[0:1], ids[1:2]
    row = lax.broadcasted_iota(I32, (n_exp, tok), 0)
    oh_a, oh_b = row == id_a, row == id_b
    zero = jnp.zeros((), F32)
    l_a = jnp.sum(jnp.where(oh_a, logits, zero), axis=0, keepdims=True)
    l_b = jnp.sum(jnp.where(oh_b, logits, zero), axis=0, keepdims=True)
    top = jnp.maximum(l_a, l_b)
    e_a, e_b = jnp.exp(l_a - top), jnp.exp(l_b - top)
    g_a, g_b = e_a / (e_a + e_b), e_b / (e_a + e_b)
    chosen = jnp.where(oh_a | oh_b, 1.0, 0.0).astype(F32)
    width = 256
    tri = (lax.broadcasted_iota(I32, (width, width), 0) < lax.broadcasted_iota(I32, (width, width), 1))
    tri = jnp.where(tri, 1.0, 0.0).astype(BF16)
    before = jnp.zeros((n_exp, 1), F32)
    ranks = []
    for k in range(tok // width):
        blk = chosen[:, k * width : (k + 1) * width]
        ranks.append(_dot(blk.astype(BF16), tri) + before)
        before = before + jnp.sum(blk, axis=1, keepdims=True)
    rank = jnp.concatenate(ranks, axis=1)
    cnt_ref[...] = jnp.broadcast_to(before, cnt_ref.shape).astype(I32)

    def slot_of(ident, onehot):
        here = jnp.sum(jnp.where(onehot, rank, zero), axis=0, keepdims=True)
        dev = ident // local_count
        lower = (row < ident) & (row >= dev * local_count)
        base = jnp.sum(jnp.where(lower, jnp.broadcast_to(before, (n_exp, tok)), zero), axis=0, keepdims=True)
        return dev.astype(F32) * row_cap + here + base

    s_a, s_b = slot_of(id_a, oh_a), slot_of(id_b, oh_b)
    both = jnp.concatenate([s_a, s_b, g_a, g_b, s_a, s_b, g_a, g_b], axis=0)
    slot_ref[...] = both.astype(I32)
    cols_ref[...] = both.T


SLOT_TILE = 32
SUM_GROUP = 16


def list_tiles(n_dev, size, start, counts_ref, list_ref, visit=None):
    per = size // SLOT_TILE

    def collect(i, cnt):
        hit = counts_ref[i // per] > start + (i % per) * SLOT_TILE

        @pl.when(hit)
        def _():
            list_ref[cnt] = i
            if visit is not None:
                visit(i, cnt)

        return cnt + hit.astype(I32)

    return lax.fori_loop(0, n_dev * per, collect, jnp.int32(0))


def first_slot(i, size, start, row_cap):
    per = size // SLOT_TILE
    return (i // per) * row_cap + start + (i % per) * SLOT_TILE


WIDE = 512
GROUP = 16
STEP = GROUP * TILE


MESH = pl.DeviceIdType.MESH


def partner(me, offset):
    other = me
    for bit in (1, 2, 4, 8):
        other = other + ((offset // bit) % 2) * (bit - 2 * bit * ((me // bit) % 2))
    return other


def pair_of(p):
    j, r = (p - 1) // 2, (p - 1) % 2
    near = 8 - 4 * j + 2 * (j // 2)
    return 14 - near + r, near + r


def ship_kernel(row_cap, n_dev, chunks, slot_ref, cnt_ref, x_ref, got_ref, next_ref, all_ref, sbuf, vbuf, send_sems, recv_sems, own_sem, next_sems, cs_sems, cr_sems, co_sem):
    me = lax.axis_index("ep")
    tok = x_ref.shape[0]
    (start, size), (start1, size1) = chunks

    def pack(dev, first, rows):
        want = lax.broadcasted_iota(I32, (rows, tok), 0) + (dev * row_cap + first)
        hit = (want == slot_ref[0:1, :]) | (want == slot_ref[1:2, :])
        pick = jnp.where(hit, 1.0, 0.0).astype(BF16)
        return _dot(pick, x_ref[...]).astype(BF16)

    def send(k):
        return pltpu.make_async_remote_copy(
            src_ref=sbuf.at[k],
            dst_ref=got_ref.at[me],
            send_sem=send_sems.at[k],
            recv_sem=recv_sems.at[k],
            device_id=(partner(me, k),),
            device_id_type=MESH,
        )

    def tell(k):
        return pltpu.make_async_remote_copy(
            src_ref=cnt_ref,
            dst_ref=all_ref.at[me],
            send_sem=cs_sems.at[k],
            recv_sem=cr_sems.at[k],
            device_id=(partner(me, k),),
            device_id_type=MESH,
        )

    own_counts = pltpu.make_async_copy(cnt_ref, all_ref.at[me], co_sem)

    def keep(d):
        return pltpu.make_async_copy(vbuf.at[d], next_ref.at[d], next_sems.at[d])

    def pack_first(k0, k1):
        @pl.loop(0, 2)
        def _(r):
            k = k0 + r * (k1 - k0)
            sbuf[k] = pack(partner(me, k), start, size)

    barrier = pltpu.get_barrier_semaphore()
    for k in range(1, n_dev):
        pl.semaphore_signal(barrier, inc=1, device_id=(partner(me, k),), device_id_type=MESH)
    pack_first(14, 15)
    pl.semaphore_wait(barrier, n_dev - 1)
    send(14).start()
    send(15).start()
    own_counts.start()

    @pl.loop(1, n_dev)
    def _(k):
        tell(k).start()

    pack_first(6, 8)
    pack_first(0, 1)

    @pl.loop(1, 7)
    def _(p):
        k0, k1 = pair_of(p)

        @pl.when(p <= 2)
        def _():
            send(13 + p).wait_send()

        @pl.when(p >= 3)
        def _():
            for k in pair_of(p - 2):
                send(k).wait_send()

        send(k0).start()
        send(k1).start()

        @pl.when(p < 6)
        def _():
            pack_first(*pair_of(p + 1))

        @pl.loop((n_dev * (p - 1)) // 6, (n_dev * p) // 6)
        def _(d):
            vbuf[d] = pack(d, start1, size1)

            @pl.when(d > 0)
            def _():
                keep(d - 1).start()

    keep(n_dev - 1).start()
    send(1).start()
    own = pltpu.make_async_copy(sbuf.at[0], got_ref.at[me], own_sem)
    own.start()
    for p in (5, 6):
        for k in pair_of(p):
            send(k).wait_send()
    send(1).wait_send()
    own.wait()
    own_counts.wait()

    @pl.loop(0, n_dev)
    def _(d):
        keep(d).wait()

    @pl.loop(1, n_dev)
    def _(k):
        tell(k).wait_send()
        tell(k).wait_recv()
        send(k).wait_recv()


def ffn_kernel(start, size, n_src, bound_ref, x_hbm, w1_hbm, w3_hbm, w2_hbm, out_ref, x_ref, w1, w3, w2, xbuf, hbuf, list_ref, low_ref, high_ref, used_ref, sems, x_sems):
    n_loc, _, ff = w1.shape
    n_f = ff // WIDE
    per = size // TILE

    def copy(e, which, f):
        cut = pl.ds(f * WIDE, WIDE)
        at = (e, cut) if which == 2 else (e, slice(None), cut)
        src, dst = ((w1_hbm, w1), (w3_hbm, w3), (w2_hbm, w2))[which]
        return pltpu.make_async_copy(src.at[at], dst.at[at], sems.at[e, which, f])

    quarter = x_ref.shape[0] // 4

    def row_copy(q):
        at = pl.ds(q * quarter, quarter)
        return pltpu.make_async_copy(x_hbm.at[at], x_ref.at[at], x_sems.at[q])

    for q in range(4):
        row_copy(q).start()

    @pl.loop(0, n_loc)
    def _(e):
        def need(s, any_):
            lo, hi = bound_ref[e, s], bound_ref[e + 1, s]
            return any_ | ((lo < start + size) & (hi > start) & (hi > lo)).astype(I32)

        used = lax.fori_loop(0, n_src, need, jnp.int32(0))
        used_ref[e] = used

        @pl.when(used > 0)
        def _():
            @pl.loop(0, n_f)
            def _(f):
                copy(e, 0, f).start()
                copy(e, 1, f).start()

            @pl.loop(0, n_f)
            def _(f):
                copy(e, 2, f).start()

    out_ref[...] = jnp.zeros_like(out_ref)
    for q in range(4):
        row_copy(q).wait()

    @pl.loop(0, n_loc)
    def _(e):
        @pl.when(used_ref[e] > 0)
        def _():
            def collect(s, cnt):
                lo = jnp.clip(bound_ref[e, s] - start, 0, size)
                hi = jnp.clip(bound_ref[e + 1, s] - start, 0, size)
                t_lo = lo // TILE
                t_hi = jnp.where(hi > lo, (hi + TILE - 1) // TILE, t_lo)

                def add(t, k):
                    list_ref[k] = s * per + t
                    low_ref[k] = lo - t * TILE
                    high_ref[k] = hi - t * TILE
                    return k + 1

                return lax.fori_loop(t_lo, t_hi, add, cnt)

            cnt = lax.fori_loop(0, n_src, collect, jnp.int32(0))
            groups = (cnt + GROUP - 1) // GROUP

            @pl.loop(cnt, groups * GROUP)
            def _(k):
                list_ref[k] = 0
                low_ref[k] = 0
                high_ref[k] = 0

            def tile_of(g, j):
                return pl.ds(pl.multiple_of(list_ref[g * GROUP + j] * TILE, TILE), TILE)

            def columns(f):
                cut = pl.ds(f * WIDE if isinstance(f, int) else pl.multiple_of(f * WIDE, WIDE), WIDE)
                xb = xbuf[...]
                u = _dot(xb, w1[e, :, cut])
                v = _dot(xb, w3[e, :, cut])
                hbuf[:, cut] = (u * jax.nn.sigmoid(u) * v).astype(BF16)

            @pl.loop(0, groups)
            def _(g):
                for j in range(GROUP):
                    xbuf[j * TILE : (j + 1) * TILE, :] = x_ref[tile_of(g, j), :]

                @pl.when(g == 0)
                def _():
                    @pl.loop(0, n_f)
                    def _(f):
                        copy(e, 0, f).wait()
                        copy(e, 1, f).wait()
                        columns(f)

                    @pl.loop(0, n_f)
                    def _(f):
                        copy(e, 2, f).wait()

                @pl.when(g > 0)
                def _():
                    for f in range(n_f):
                        columns(f)

                y = _dot(hbuf[...], w2[e]).astype(BF16)
                row = lax.broadcasted_iota(I32, (TILE, 1), 0)
                for j in range(GROUP):
                    own = (row >= low_ref[g * GROUP + j]) & (row < high_ref[g * GROUP + j])
                    at = tile_of(g, j)
                    out_ref[at, :] = jnp.where(own, y[j * TILE : (j + 1) * TILE], out_ref[at, :])


def gated(cols, ids, rows):
    add = 0.0
    for k in range(2):
        pick = jnp.where(ids == cols[:, k : k + 1], 1.0, 0.0).astype(BF16)
        add = add + cols[:, 2 + k : 3 + k] * _dot(pick, rows)
    return add


def bring_kernel(row_cap, n_dev, chunk, made_ref, back_hbm, cols_ref, got_ref, acc_ref, back, acc, send_sems, recv_sems, own_sem, back_sems, acc_sem):
    me = lax.axis_index("ep")
    start, size = chunk
    tok = cols_ref.shape[0]
    block = 512

    def send(k):
        return pltpu.make_async_remote_copy(
            src_ref=made_ref.at[partner(me, k)],
            dst_ref=got_ref.at[me],
            send_sem=send_sems.at[k],
            recv_sem=recv_sems.at[k],
            device_id=(partner(me, k),),
            device_id_type=MESH,
        )

    def fetch(g):
        at = pl.ds(pl.multiple_of(g * 2 * size, 2 * size), 2 * size)
        return pltpu.make_async_copy(back_hbm.at[at], back.at[at], back_sems.at[g])

    barrier = pltpu.get_barrier_semaphore()
    for k in range(1, n_dev):
        pl.semaphore_signal(barrier, inc=1, device_id=(partner(me, k),), device_id_type=MESH)
    acc[...] = jnp.zeros_like(acc)
    pl.semaphore_wait(barrier, n_dev - 1)
    send(14).start()
    send(15).start()
    send(1).start()
    own = pltpu.make_async_copy(made_ref.at[me], got_ref.at[me], own_sem)
    own.start()
    groups = n_dev // 2

    @pl.loop(0, groups)
    def _(g):
        fetch(g).start()

    @pl.loop(1, 7)
    def _(p):
        k0, k1 = pair_of(p)

        @pl.when(p <= 2)
        def _():
            send(13 + p).wait_send()

        @pl.when(p >= 3)
        def _():
            for k in pair_of(p - 2):
                send(k).wait_send()

        send(k0).start()
        send(k1).start()

        @pl.loop((groups * (p - 1)) // 6, (groups * p) // 6)
        def _(g):
            fetch(g).wait()
            rows = back[pl.ds(pl.multiple_of(g * 2 * size, 2 * size), 2 * size), :]
            lane = lax.broadcasted_iota(I32, (1, 2 * size), 1)
            ids = ((2 * g + lane // size) * row_cap + start + lane % size).astype(F32)

            @pl.loop(0, tok // block)
            def _(t):
                at = pl.ds(pl.multiple_of(t * block, block), block)
                acc[at, :] += gated(cols_ref[at, :], ids, rows)

    out = pltpu.make_async_copy(acc, acc_ref, acc_sem)
    for p in (5, 6):
        for k in pair_of(p):
            send(k).wait_send()
    out.start()
    send(1).wait_send()
    own.wait()

    @pl.loop(1, n_dev)
    def _(k):
        send(k).wait_recv()

    out.wait()


def combine_kernel(row_cap, start, size, n_dev, counts_ref, cols_ref, back_hbm, acc_ref, out_ref, rows_ref, sum_ref, list_ref, cnt_ref, sems):
    group = SUM_GROUP * SLOT_TILE

    def fetch(i, k):
        src = pl.ds(pl.multiple_of(i * SLOT_TILE, SLOT_TILE), SLOT_TILE)
        dst = pl.ds(pl.multiple_of(k * SLOT_TILE, SLOT_TILE), SLOT_TILE)
        return pltpu.make_async_copy(back_hbm.at[src], rows_ref.at[dst], sems.at[k])

    @pl.when(pl.program_id(0) == 0)
    def _():
        cnt = list_tiles(n_dev, size, start, counts_ref, list_ref, lambda i, k: fetch(i, k).start())
        groups = (cnt + SUM_GROUP - 1) // SUM_GROUP
        cnt_ref[0] = groups

        @pl.loop(cnt, groups * SUM_GROUP)
        def _(k):
            list_ref[k] = -1
            rows_ref[pl.ds(pl.multiple_of(k * SLOT_TILE, SLOT_TILE), SLOT_TILE), :] = jnp.zeros((SLOT_TILE, rows_ref.shape[1]), BF16)

        @pl.loop(0, cnt)
        def _(k):
            fetch(list_ref[k], k).wait()

    lane = lax.broadcasted_iota(I32, (1, group), 1)

    def one(g, total):
        ids = jnp.full((1, group), -1, I32)
        for j in range(SUM_GROUP):
            i = list_ref[g * SUM_GROUP + j]
            base = jnp.where(i < 0, -1 - group, first_slot(i, size, start, row_cap))
            ids = jnp.where(lane // SLOT_TILE == j, base + lane % SLOT_TILE, ids)
        rows = rows_ref[pl.ds(pl.multiple_of(g * group, group), group), :]
        return total + gated(cols_ref[...], ids.astype(F32), rows)

    sum_ref[...] = acc_ref[...]

    @pl.loop(0, cnt_ref[0])
    def _(g):
        sum_ref[...] = one(g, sum_ref[...])

    out_ref[...] = sum_ref[...].astype(out_ref.dtype)


def _params(vmem_limit_bytes=VMEM_BYTES):
    return pltpu.CompilerParams(vmem_limit_bytes=vmem_limit_bytes)


def solution(mesh):
    n = mesh.shape["ep"]

    def body(x, w_router, ids, w1, w3, w2):
        tok, dim = x.shape
        local = w1.shape[0]
        ff = w1.shape[2]
        n_exp = n * local
        cap = 4 * tok // n
        slots, cols, counts = pl.pallas_call(
            functools.partial(route_kernel, local, cap),
            out_shape=(
                jax.ShapeDtypeStruct((8, tok), I32),
                jax.ShapeDtypeStruct((tok, 8), F32),
                jax.ShapeDtypeStruct((n_exp, 128), I32),
            ),
            compiler_params=_params(),
            name="route",
        )(x, w_router.T, ids.T)
        dev_counts = jnp.sum(counts[:, 0].reshape(n, local), axis=1)
        smem = pl.BlockSpec(memory_space=pltpu.SMEM)
        vmem = pl.BlockSpec(memory_space=pltpu.VMEM)
        hbm = pl.BlockSpec(memory_space=pl.ANY)
        ship = pl.pallas_call(
            functools.partial(ship_kernel, cap, n, CHUNKS),
            in_specs=[vmem, vmem, vmem],
            out_specs=[hbm, hbm, hbm],
            out_shape=[jax.ShapeDtypeStruct((n, size, dim), BF16) for _, size in CHUNKS]
            + [jax.ShapeDtypeStruct((n,) + counts.shape, I32)],
            scratch_shapes=[
                pltpu.VMEM((n, CHUNKS[0][1], dim), BF16),
                pltpu.VMEM((n, CHUNKS[1][1], dim), BF16),
                pltpu.SemaphoreType.DMA((n,)),
                pltpu.SemaphoreType.DMA((n,)),
                pltpu.SemaphoreType.DMA,
                pltpu.SemaphoreType.DMA((n,)),
                pltpu.SemaphoreType.DMA((n,)),
                pltpu.SemaphoreType.DMA((n,)),
                pltpu.SemaphoreType.DMA,
            ],
            compiler_params=pltpu.CompilerParams(
                vmem_limit_bytes=VMEM_BYTES, collective_id=0, has_side_effects=True
            ),
            cost_estimate=pl.CostEstimate(flops=10**11, bytes_accessed=1, transcendentals=0),
            name="ship",
        )
        first_rows, second_rows, every = ship(slots, counts, x)
        at = lax.axis_index("ep") * local
        per_exp = lax.dynamic_slice(every, (0, at, 0), (n, local, 1))[:, :, 0]
        ends = jnp.cumsum(per_exp, axis=1).T
        bounds = jnp.concatenate([jnp.zeros((1, n), I32), ends], axis=0)
        for index, (start, size) in enumerate(CHUNKS):
            if index == 0:
                got = first_rows
            else:
                got = lax.all_to_all(second_rows, "ep", 0, 0, tiled=True)
            rows = n * size
            made = pl.pallas_call(
                functools.partial(ffn_kernel, start, size, n),
                in_specs=[smem, hbm, hbm, hbm, hbm],
                out_specs=vmem,
                scratch_shapes=[
                    pltpu.VMEM((rows, dim), BF16),
                    pltpu.VMEM((local, dim, ff), BF16),
                    pltpu.VMEM((local, dim, ff), BF16),
                    pltpu.VMEM((local, ff, dim), BF16),
                    pltpu.VMEM((STEP, dim), BF16),
                    pltpu.VMEM((STEP, ff), BF16),
                    pltpu.SMEM((rows // TILE + GROUP,), I32),
                    pltpu.SMEM((rows // TILE + GROUP,), I32),
                    pltpu.SMEM((rows // TILE + GROUP,), I32),
                    pltpu.SMEM((local,), I32),
                    pltpu.SemaphoreType.DMA((local, 3, ff // WIDE)),
                    pltpu.SemaphoreType.DMA((4,)),
                ],
                out_shape=jax.ShapeDtypeStruct((rows, dim), BF16),
                compiler_params=_params(),
                cost_estimate=pl.CostEstimate(flops=6 * rows * dim * ff, bytes_accessed=1, transcendentals=0),
            )
            made = made(bounds, got.reshape(rows, dim), w1, w3, w2)
            if index == 0:
                back = lax.all_to_all(made.reshape(n, size, dim), "ep", 0, 0, tiled=True)
        start, size = CHUNKS[1]
        rows = n * size
        got, acc = pl.pallas_call(
            functools.partial(bring_kernel, cap, n, CHUNKS[0]),
            in_specs=[hbm, hbm, vmem],
            out_specs=[hbm, hbm],
            out_shape=[jax.ShapeDtypeStruct((n, size, dim), BF16), jax.ShapeDtypeStruct((tok, dim), F32)],
            scratch_shapes=[
                pltpu.VMEM((n * CHUNKS[0][1], dim), BF16),
                pltpu.VMEM((tok, dim), F32),
                pltpu.SemaphoreType.DMA((n,)),
                pltpu.SemaphoreType.DMA((n,)),
                pltpu.SemaphoreType.DMA,
                pltpu.SemaphoreType.DMA((n // 2,)),
                pltpu.SemaphoreType.DMA,
            ],
            compiler_params=pltpu.CompilerParams(
                vmem_limit_bytes=VMEM_BYTES, collective_id=1, has_side_effects=True
            ),
            cost_estimate=pl.CostEstimate(flops=10**11, bytes_accessed=1, transcendentals=0),
            name="bring",
        )(made.reshape(n, size, dim), back.reshape(n * CHUNKS[0][1], dim), cols)
        tb = 512
        tile_spec = pl.BlockSpec((tb, dim), lambda i, c: (i, 0))
        return pl.pallas_call(
            functools.partial(combine_kernel, cap, start, size, n),
            grid_spec=pltpu.PrefetchScalarGridSpec(
                num_scalar_prefetch=1,
                grid=(tok // tb,),
                in_specs=[pl.BlockSpec((tb, 8), lambda i, c: (i, 0)), hbm, tile_spec],
                out_specs=tile_spec,
                scratch_shapes=[
                    pltpu.VMEM((rows, dim), BF16),
                    pltpu.VMEM((tb, dim), F32),
                    pltpu.SMEM((rows // SLOT_TILE,), I32),
                    pltpu.SMEM((1,), I32),
                    pltpu.SemaphoreType.DMA((rows // SLOT_TILE,)),
                ],
            ),
            out_shape=jax.ShapeDtypeStruct((tok, dim), BF16),
            compiler_params=_params(),
            name="combine",
        )(dev_counts, cols, got.reshape(rows, dim), acc)

    return jax.shard_map(
        body,
        mesh=mesh,
        in_specs=(P("ep", None), P(None, None), P("ep", None), P("ep", None, None), P("ep", None, None), P("ep", None, None)),
        out_specs=P("ep", None),
        check_vma=False,
    )
```

```python
import functools

import jax
import jax.numpy as jnp
from jax import lax
from jax.experimental import pallas as pl
from jax.experimental.pallas import tpu as pltpu
from jax.sharding import PartitionSpec as P


F32 = jnp.float32
BF16 = jnp.bfloat16
I32 = jnp.int32
TILE = 16
CHUNKS = ((0, 256), (256, 256))
VMEM_BYTES = 60 * 1024 * 1024


def _dot(a, b):
    return jnp.dot(a, b, preferred_element_type=F32)


def route_kernel(local_count, row_cap, x_ref, wr_ref, ids_ref, slot_ref, cols_ref, cnt_ref):
    tok = x_ref.shape[0]
    n_exp = wr_ref.shape[0]
    w = wr_ref[...]
    w_hi = w.astype(BF16)
    rest = w - w_hi.astype(F32)
    w_mid = rest.astype(BF16)
    w_lo = (rest - w_mid.astype(F32)).astype(BF16)
    x = x_ref[...]
    nt = (((1,), (1,)), ((), ()))
    w_all = jnp.concatenate([w_hi, w_mid, w_lo], axis=0)
    parts = lax.dot_general(w_all, x, nt, preferred_element_type=F32)
    logits = parts[:n_exp] + (parts[n_exp : 2 * n_exp] + parts[2 * n_exp :])
    ids = ids_ref[...]
    id_a, id_b = ids[0:1], ids[1:2]
    row = lax.broadcasted_iota(I32, (n_exp, tok), 0)
    oh_a, oh_b = row == id_a, row == id_b
    zero = jnp.zeros((), F32)
    l_a = jnp.sum(jnp.where(oh_a, logits, zero), axis=0, keepdims=True)
    l_b = jnp.sum(jnp.where(oh_b, logits, zero), axis=0, keepdims=True)
    top = jnp.maximum(l_a, l_b)
    e_a, e_b = jnp.exp(l_a - top), jnp.exp(l_b - top)
    g_a, g_b = e_a / (e_a + e_b), e_b / (e_a + e_b)
    chosen = jnp.where(oh_a | oh_b, 1.0, 0.0).astype(F32)
    width = 256
    tri = (lax.broadcasted_iota(I32, (width, width), 0) < lax.broadcasted_iota(I32, (width, width), 1))
    tri = jnp.where(tri, 1.0, 0.0).astype(BF16)
    before = jnp.zeros((n_exp, 1), F32)
    ranks = []
    for k in range(tok // width):
        blk = chosen[:, k * width : (k + 1) * width]
        ranks.append(_dot(blk.astype(BF16), tri) + before)
        before = before + jnp.sum(blk, axis=1, keepdims=True)
    rank = jnp.concatenate(ranks, axis=1)
    cnt_ref[...] = jnp.broadcast_to(before, cnt_ref.shape).astype(I32)

    def slot_of(ident, onehot):
        here = jnp.sum(jnp.where(onehot, rank, zero), axis=0, keepdims=True)
        dev = ident // local_count
        lower = (row < ident) & (row >= dev * local_count)
        base = jnp.sum(jnp.where(lower, jnp.broadcast_to(before, (n_exp, tok)), zero), axis=0, keepdims=True)
        return dev.astype(F32) * row_cap + here + base

    s_a, s_b = slot_of(id_a, oh_a), slot_of(id_b, oh_b)
    both = jnp.concatenate([s_a, s_b, g_a, g_b, s_a, s_b, g_a, g_b], axis=0)
    slot_ref[...] = both.astype(I32)
    cols_ref[...] = both.T


WIDE = 512
GROUP = 16
STEP = GROUP * TILE


MESH = pl.DeviceIdType.MESH


def partner(me, offset):
    other = me
    for bit in (1, 2, 4, 8):
        other = other + ((offset // bit) % 2) * (bit - 2 * bit * ((me // bit) % 2))
    return other


def pair_of(p):
    j, r = (p - 1) // 2, (p - 1) % 2
    near = 8 - 4 * j + 2 * (j // 2)
    return 14 - near + r, near + r


def ship_kernel(row_cap, n_dev, chunks, slot_ref, cnt_ref, x_ref, got_ref, next_ref, all_ref, sbuf, vbuf, send_sems, recv_sems, own_sem, next_sems, cs_sems, cr_sems, co_sem):
    me = lax.axis_index("ep")
    tok = x_ref.shape[0]
    (start, size), (start1, size1) = chunks

    def pack(dev, first, rows):
        want = lax.broadcasted_iota(I32, (rows, tok), 0) + (dev * row_cap + first)
        hit = (want == slot_ref[0:1, :]) | (want == slot_ref[1:2, :])
        pick = jnp.where(hit, 1.0, 0.0).astype(BF16)
        return _dot(pick, x_ref[...]).astype(BF16)

    def send(k):
        return pltpu.make_async_remote_copy(
            src_ref=sbuf.at[k],
            dst_ref=got_ref.at[me],
            send_sem=send_sems.at[k],
            recv_sem=recv_sems.at[k],
            device_id=(partner(me, k),),
            device_id_type=MESH,
        )

    def tell(k):
        return pltpu.make_async_remote_copy(
            src_ref=cnt_ref,
            dst_ref=all_ref.at[me],
            send_sem=cs_sems.at[k],
            recv_sem=cr_sems.at[k],
            device_id=(partner(me, k),),
            device_id_type=MESH,
        )

    own_counts = pltpu.make_async_copy(cnt_ref, all_ref.at[me], co_sem)

    def keep(d):
        return pltpu.make_async_copy(vbuf.at[d], next_ref.at[d], next_sems.at[d])

    def pack_first(k0, k1):
        @pl.loop(0, 2)
        def _(r):
            k = k0 + r * (k1 - k0)
            sbuf[k] = pack(partner(me, k), start, size)

    barrier = pltpu.get_barrier_semaphore()
    for k in range(1, n_dev):
        pl.semaphore_signal(barrier, inc=1, device_id=(partner(me, k),), device_id_type=MESH)
    pack_first(14, 15)
    pl.semaphore_wait(barrier, n_dev - 1)
    send(14).start()
    send(15).start()
    own_counts.start()

    @pl.loop(1, n_dev)
    def _(k):
        tell(k).start()

    pack_first(6, 8)
    pack_first(0, 1)

    @pl.loop(1, 7)
    def _(p):
        k0, k1 = pair_of(p)

        @pl.when(p <= 2)
        def _():
            send(13 + p).wait_send()

        @pl.when(p >= 3)
        def _():
            for k in pair_of(p - 2):
                send(k).wait_send()

        send(k0).start()
        send(k1).start()

        @pl.when(p < 6)
        def _():
            pack_first(*pair_of(p + 1))

        @pl.loop((n_dev * (p - 1)) // 6, (n_dev * p) // 6)
        def _(d):
            vbuf[d] = pack(d, start1, size1)

            @pl.when(d > 0)
            def _():
                keep(d - 1).start()

    keep(n_dev - 1).start()
    send(1).start()
    own = pltpu.make_async_copy(sbuf.at[0], got_ref.at[me], own_sem)
    own.start()
    for p in (5, 6):
        for k in pair_of(p):
            send(k).wait_send()
    send(1).wait_send()
    own.wait()
    own_counts.wait()

    @pl.loop(0, n_dev)
    def _(d):
        keep(d).wait()

    @pl.loop(1, n_dev)
    def _(k):
        tell(k).wait_send()
        tell(k).wait_recv()
        send(k).wait_recv()


def ffn_kernel(start, size, n_src, bound_ref, x_hbm, w1_hbm, w3_hbm, w2_hbm, out_ref, x_ref, w1, w3, w2, xbuf, hbuf, list_ref, low_ref, high_ref, used_ref, sems, x_sems):
    n_loc, _, ff = w1.shape
    n_f = ff // WIDE
    per = size // TILE

    def copy(e, which, f):
        cut = pl.ds(f * WIDE, WIDE)
        at = (e, cut) if which == 2 else (e, slice(None), cut)
        src, dst = ((w1_hbm, w1), (w3_hbm, w3), (w2_hbm, w2))[which]
        return pltpu.make_async_copy(src.at[at], dst.at[at], sems.at[e, which, f])

    quarter = x_ref.shape[0] // 4

    def row_copy(q):
        at = pl.ds(q * quarter, quarter)
        return pltpu.make_async_copy(x_hbm.at[at], x_ref.at[at], x_sems.at[q])

    for q in range(4):
        row_copy(q).start()

    @pl.loop(0, n_loc)
    def _(e):
        def need(s, any_):
            lo, hi = bound_ref[e, s], bound_ref[e + 1, s]
            return any_ | ((lo < start + size) & (hi > start) & (hi > lo)).astype(I32)

        used = lax.fori_loop(0, n_src, need, jnp.int32(0))
        used_ref[e] = used

        @pl.when(used > 0)
        def _():
            @pl.loop(0, n_f)
            def _(f):
                copy(e, 0, f).start()
                copy(e, 1, f).start()

            @pl.loop(0, n_f)
            def _(f):
                copy(e, 2, f).start()

    out_ref[...] = jnp.zeros_like(out_ref)
    for q in range(4):
        row_copy(q).wait()

    @pl.loop(0, n_loc)
    def _(e):
        @pl.when(used_ref[e] > 0)
        def _():
            def collect(s, cnt):
                lo = jnp.clip(bound_ref[e, s] - start, 0, size)
                hi = jnp.clip(bound_ref[e + 1, s] - start, 0, size)
                t_lo = lo // TILE
                t_hi = jnp.where(hi > lo, (hi + TILE - 1) // TILE, t_lo)

                def add(t, k):
                    list_ref[k] = s * per + t
                    low_ref[k] = lo - t * TILE
                    high_ref[k] = hi - t * TILE
                    return k + 1

                return lax.fori_loop(t_lo, t_hi, add, cnt)

            cnt = lax.fori_loop(0, n_src, collect, jnp.int32(0))
            groups = (cnt + GROUP - 1) // GROUP

            @pl.loop(cnt, groups * GROUP)
            def _(k):
                list_ref[k] = 0
                low_ref[k] = 0
                high_ref[k] = 0

            def tile_of(g, j):
                return pl.ds(pl.multiple_of(list_ref[g * GROUP + j] * TILE, TILE), TILE)

            def columns(f):
                cut = pl.ds(f * WIDE if isinstance(f, int) else pl.multiple_of(f * WIDE, WIDE), WIDE)
                xb = xbuf[...]
                u = _dot(xb, w1[e, :, cut])
                v = _dot(xb, w3[e, :, cut])
                hbuf[:, cut] = (u * jax.nn.sigmoid(u) * v).astype(BF16)

            @pl.loop(0, groups)
            def _(g):
                for j in range(GROUP):
                    xbuf[j * TILE : (j + 1) * TILE, :] = x_ref[tile_of(g, j), :]

                @pl.when(g == 0)
                def _():
                    @pl.loop(0, n_f)
                    def _(f):
                        copy(e, 0, f).wait()
                        copy(e, 1, f).wait()
                        columns(f)

                    @pl.loop(0, n_f)
                    def _(f):
                        copy(e, 2, f).wait()

                @pl.when(g > 0)
                def _():
                    for f in range(n_f):
                        columns(f)

                y = _dot(hbuf[...], w2[e]).astype(BF16)
                row = lax.broadcasted_iota(I32, (TILE, 1), 0)
                for j in range(GROUP):
                    own = (row >= low_ref[g * GROUP + j]) & (row < high_ref[g * GROUP + j])
                    at = tile_of(g, j)
                    out_ref[at, :] = jnp.where(own, y[j * TILE : (j + 1) * TILE], out_ref[at, :])


def gated(cols, ids, rows):
    add = 0.0
    for k in range(2):
        pick = jnp.where(ids == cols[:, k : k + 1], 1.0, 0.0).astype(BF16)
        add = add + cols[:, 2 + k : 3 + k] * _dot(pick, rows)
    return add


def bring_kernel(row_cap, n_dev, chunks, made_ref, back_hbm, cols_ref, out_ref, back, got, acc, send_sems, recv_sems, own_sem, back_sems):
    me = lax.axis_index("ep")
    (start, size), (start1, size1) = chunks
    tok = cols_ref.shape[0]
    block = 512

    def send(k):
        return pltpu.make_async_remote_copy(
            src_ref=made_ref.at[partner(me, k)],
            dst_ref=got.at[me],
            send_sem=send_sems.at[k],
            recv_sem=recv_sems.at[k],
            device_id=(partner(me, k),),
            device_id_type=MESH,
        )

    def fetch(g):
        at = pl.ds(pl.multiple_of(g * 2 * size, 2 * size), 2 * size)
        return pltpu.make_async_copy(back_hbm.at[at], back.at[at], back_sems.at[g])

    def slots_of(chip, first, rows):
        lane = lax.broadcasted_iota(I32, (1, 2 * rows), 1)
        return ((2 * chip + lane // rows) * row_cap + first + lane % rows).astype(F32)

    def each_block(body):
        @pl.loop(0, tok // block)
        def _(t):
            body(pl.ds(pl.multiple_of(t * block, block), block))

    def first_group(g):
        fetch(g).wait()
        rows = back[pl.ds(pl.multiple_of(g * 2 * size, 2 * size), 2 * size), :]
        ids = slots_of(g, start, size)

        def add(at):
            acc[at, :] += gated(cols_ref[at, :], ids, rows)

        each_block(add)

    def arrived(k):
        chip = partner(me, k) // 2
        rows = got[pl.ds(2 * chip, 2)].reshape(2 * size1, got.shape[2])
        return rows, slots_of(chip, start1, size1)

    def second_group(k):
        rows, ids = arrived(k)

        def add(at):
            acc[at, :] += gated(cols_ref[at, :], ids, rows)

        each_block(add)

    barrier = pltpu.get_barrier_semaphore()
    for k in range(1, n_dev):
        pl.semaphore_signal(barrier, inc=1, device_id=(partner(me, k),), device_id_type=MESH)
    groups = n_dev // 2

    @pl.loop(0, groups)
    def _(g):
        fetch(g).start()

    acc[...] = jnp.zeros_like(acc)
    pl.semaphore_wait(barrier, n_dev - 1)
    send(14).start()
    send(15).start()
    send(1).start()
    own = pltpu.make_async_copy(made_ref.at[me], got.at[me], own_sem)
    own.start()

    @pl.loop(1, 7)
    def _(p):
        k0, k1 = pair_of(p)

        @pl.when(p <= 2)
        def _():
            send(13 + p).wait_send()

        @pl.when(p >= 3)
        def _():
            for k in pair_of(p - 2):
                send(k).wait_send()

        send(k0).start()
        send(k1).start()

        @pl.loop((groups * (p - 1)) // 6, (groups * p) // 6)
        def _(g):
            first_group(g)

        @pl.when((p >= 3) & (p <= 5))
        def _():
            base = jnp.where(p == 3, 14, jnp.where(p == 4, 6, 8))
            send(base).wait_recv()
            send(base + 1).wait_recv()
            second_group(base)

    own.wait()
    send(1).wait_recv()

    @pl.loop(0, 3)
    def _(q):
        base = jnp.where(q == 0, 0, jnp.where(q == 1, 10, 4))

        @pl.when(q > 0)
        def _():
            send(base).wait_recv()
            send(base + 1).wait_recv()

        second_group(base)

    for k in (12, 13, 2, 3):
        send(k).wait_recv()
    rows_a, ids_a = arrived(12)
    rows_b, ids_b = arrived(2)

    def finish(at):
        cols = cols_ref[at, :]
        total = acc[at, :] + gated(cols, ids_a, rows_a) + gated(cols, ids_b, rows_b)
        out_ref[at, :] = total.astype(BF16)

    each_block(finish)
    for p in (5, 6):
        for k in pair_of(p):
            send(k).wait_send()
    send(1).wait_send()


def _params(vmem_limit_bytes=VMEM_BYTES):
    return pltpu.CompilerParams(vmem_limit_bytes=vmem_limit_bytes)


def solution(mesh):
    n = mesh.shape["ep"]

    def body(x, w_router, ids, w1, w3, w2):
        tok, dim = x.shape
        local = w1.shape[0]
        ff = w1.shape[2]
        n_exp = n * local
        cap = 4 * tok // n
        slots, cols, counts = pl.pallas_call(
            functools.partial(route_kernel, local, cap),
            out_shape=(
                jax.ShapeDtypeStruct((8, tok), I32),
                jax.ShapeDtypeStruct((tok, 8), F32),
                jax.ShapeDtypeStruct((n_exp, 128), I32),
            ),
            compiler_params=_params(),
            name="route",
        )(x, w_router.T, ids.T)
        smem = pl.BlockSpec(memory_space=pltpu.SMEM)
        vmem = pl.BlockSpec(memory_space=pltpu.VMEM)
        hbm = pl.BlockSpec(memory_space=pl.ANY)
        ship = pl.pallas_call(
            functools.partial(ship_kernel, cap, n, CHUNKS),
            in_specs=[vmem, vmem, vmem],
            out_specs=[hbm, hbm, hbm],
            out_shape=[jax.ShapeDtypeStruct((n, size, dim), BF16) for _, size in CHUNKS]
            + [jax.ShapeDtypeStruct((n,) + counts.shape, I32)],
            scratch_shapes=[
                pltpu.VMEM((n, CHUNKS[0][1], dim), BF16),
                pltpu.VMEM((n, CHUNKS[1][1], dim), BF16),
                pltpu.SemaphoreType.DMA((n,)),
                pltpu.SemaphoreType.DMA((n,)),
                pltpu.SemaphoreType.DMA,
                pltpu.SemaphoreType.DMA((n,)),
                pltpu.SemaphoreType.DMA((n,)),
                pltpu.SemaphoreType.DMA((n,)),
                pltpu.SemaphoreType.DMA,
            ],
            compiler_params=pltpu.CompilerParams(
                vmem_limit_bytes=VMEM_BYTES, collective_id=0, has_side_effects=True
            ),
            cost_estimate=pl.CostEstimate(flops=10**11, bytes_accessed=1, transcendentals=0),
            name="ship",
        )
        first_rows, second_rows, every = ship(slots, counts, x)
        at = lax.axis_index("ep") * local
        per_exp = lax.dynamic_slice(every, (0, at, 0), (n, local, 1))[:, :, 0]
        ends = jnp.cumsum(per_exp, axis=1).T
        bounds = jnp.concatenate([jnp.zeros((1, n), I32), ends], axis=0)
        for index, (start, size) in enumerate(CHUNKS):
            if index == 0:
                got = first_rows
            else:
                got = lax.all_to_all(second_rows, "ep", 0, 0, tiled=True)
            rows = n * size
            made = pl.pallas_call(
                functools.partial(ffn_kernel, start, size, n),
                in_specs=[smem, hbm, hbm, hbm, hbm],
                out_specs=vmem,
                scratch_shapes=[
                    pltpu.VMEM((rows, dim), BF16),
                    pltpu.VMEM((local, dim, ff), BF16),
                    pltpu.VMEM((local, dim, ff), BF16),
                    pltpu.VMEM((local, ff, dim), BF16),
                    pltpu.VMEM((STEP, dim), BF16),
                    pltpu.VMEM((STEP, ff), BF16),
                    pltpu.SMEM((rows // TILE + GROUP,), I32),
                    pltpu.SMEM((rows // TILE + GROUP,), I32),
                    pltpu.SMEM((rows // TILE + GROUP,), I32),
                    pltpu.SMEM((local,), I32),
                    pltpu.SemaphoreType.DMA((local, 3, ff // WIDE)),
                    pltpu.SemaphoreType.DMA((4,)),
                ],
                out_shape=jax.ShapeDtypeStruct((rows, dim), BF16),
                compiler_params=_params(),
                cost_estimate=pl.CostEstimate(flops=6 * rows * dim * ff, bytes_accessed=1, transcendentals=0),
            )
            made = made(bounds, got.reshape(rows, dim), w1, w3, w2)
            if index == 0:
                back = lax.all_to_all(made.reshape(n, size, dim), "ep", 0, 0, tiled=True)
        return pl.pallas_call(
            functools.partial(bring_kernel, cap, n, CHUNKS),
            in_specs=[hbm, hbm, vmem],
            out_specs=vmem,
            out_shape=jax.ShapeDtypeStruct((tok, dim), BF16),
            scratch_shapes=[
                pltpu.VMEM((n * CHUNKS[0][1], dim), BF16),
                pltpu.VMEM((n, CHUNKS[1][1], dim), BF16),
                pltpu.VMEM((tok, dim), F32),
                pltpu.SemaphoreType.DMA((n,)),
                pltpu.SemaphoreType.DMA((n,)),
                pltpu.SemaphoreType.DMA,
                pltpu.SemaphoreType.DMA((n // 2,)),
            ],
            compiler_params=pltpu.CompilerParams(
                vmem_limit_bytes=VMEM_BYTES, collective_id=1, has_side_effects=True
            ),
            cost_estimate=pl.CostEstimate(flops=10**11, bytes_accessed=1, transcendentals=0),
            name="bring",
        )(made.reshape(n, CHUNKS[1][1], dim), back.reshape(n * CHUNKS[0][1], dim), cols)

    return jax.shard_map(
        body,
        mesh=mesh,
        in_specs=(P("ep", None), P(None, None), P("ep", None), P("ep", None, None), P("ep", None, None), P("ep", None, None)),
        out_specs=P("ep", None),
        check_vma=False,
    )
```

```python
import functools

import jax
import jax.numpy as jnp
from jax import lax
from jax.experimental import pallas as pl
from jax.experimental.pallas import tpu as pltpu
from jax.sharding import PartitionSpec as P


F32 = jnp.float32
BF16 = jnp.bfloat16
I32 = jnp.int32
TILE = 16
CHUNKS = ((0, 256), (256, 256))
VMEM_BYTES = 60 * 1024 * 1024


def _dot(a, b):
    return jnp.dot(a, b, preferred_element_type=F32)


def route_kernel(local_count, row_cap, x_ref, wr_ref, ids_ref, slot_ref, cols_ref, cnt_ref):
    tok = x_ref.shape[0]
    n_exp = wr_ref.shape[0]
    w = wr_ref[...]
    w_hi = w.astype(BF16)
    rest = w - w_hi.astype(F32)
    w_mid = rest.astype(BF16)
    w_lo = (rest - w_mid.astype(F32)).astype(BF16)
    x = x_ref[...]
    nt = (((1,), (1,)), ((), ()))
    w_all = jnp.concatenate([w_hi, w_mid, w_lo], axis=0)
    parts = lax.dot_general(w_all, x, nt, preferred_element_type=F32)
    logits = parts[:n_exp] + (parts[n_exp : 2 * n_exp] + parts[2 * n_exp :])
    ids = ids_ref[...]
    id_a, id_b = ids[0:1], ids[1:2]
    row = lax.broadcasted_iota(I32, (n_exp, tok), 0)
    oh_a, oh_b = row == id_a, row == id_b
    zero = jnp.zeros((), F32)
    l_a = jnp.sum(jnp.where(oh_a, logits, zero), axis=0, keepdims=True)
    l_b = jnp.sum(jnp.where(oh_b, logits, zero), axis=0, keepdims=True)
    top = jnp.maximum(l_a, l_b)
    e_a, e_b = jnp.exp(l_a - top), jnp.exp(l_b - top)
    g_a, g_b = e_a / (e_a + e_b), e_b / (e_a + e_b)
    chosen = jnp.where(oh_a | oh_b, 1.0, 0.0).astype(F32)
    width = 256
    tri = (lax.broadcasted_iota(I32, (width, width), 0) < lax.broadcasted_iota(I32, (width, width), 1))
    tri = jnp.where(tri, 1.0, 0.0).astype(BF16)
    before = jnp.zeros((n_exp, 1), F32)
    ranks = []
    for k in range(tok // width):
        blk = chosen[:, k * width : (k + 1) * width]
        ranks.append(_dot(blk.astype(BF16), tri) + before)
        before = before + jnp.sum(blk, axis=1, keepdims=True)
    rank = jnp.concatenate(ranks, axis=1)
    cnt_ref[...] = jnp.broadcast_to(before, cnt_ref.shape).astype(I32)

    def slot_of(ident, onehot):
        here = jnp.sum(jnp.where(onehot, rank, zero), axis=0, keepdims=True)
        dev = ident // local_count
        lower = (row < ident) & (row >= dev * local_count)
        base = jnp.sum(jnp.where(lower, jnp.broadcast_to(before, (n_exp, tok)), zero), axis=0, keepdims=True)
        return dev.astype(F32) * row_cap + here + base

    s_a, s_b = slot_of(id_a, oh_a), slot_of(id_b, oh_b)
    both = jnp.concatenate([s_a, s_b, g_a, g_b, s_a, s_b, g_a, g_b], axis=0)
    slot_ref[...] = both.astype(I32)
    cols_ref[...] = both.T


WIDE = 512
GROUP = 16
STEP = GROUP * TILE


MESH = pl.DeviceIdType.MESH


def partner(me, offset):
    other = me
    for bit in (1, 2, 4, 8):
        other = other + ((offset // bit) % 2) * (bit - 2 * bit * ((me // bit) % 2))
    return other


def pair_of(p):
    j, r = (p - 1) // 2, (p - 1) % 2
    near = 8 - 4 * j + 2 * (j // 2)
    return 14 - near + r, near + r


def ship_kernel(row_cap, n_dev, chunks, slot_ref, cnt_ref, x_ref, got_ref, next_ref, all_ref, sbuf, vbuf, send_sems, recv_sems, own_sem, next_sems, cs_sems, cr_sems, co_sem):
    me = lax.axis_index("ep")
    tok = x_ref.shape[0]
    (start, size), (start1, size1) = chunks

    def pack(dev, first, rows):
        want = lax.broadcasted_iota(I32, (rows, tok), 0) + (dev * row_cap + first)
        hit = (want == slot_ref[0:1, :]) | (want == slot_ref[1:2, :])
        pick = jnp.where(hit, 1.0, 0.0).astype(BF16)
        return _dot(pick, x_ref[...]).astype(BF16)

    def send(k):
        return pltpu.make_async_remote_copy(
            src_ref=sbuf.at[k],
            dst_ref=got_ref.at[me],
            send_sem=send_sems.at[k],
            recv_sem=recv_sems.at[k],
            device_id=(partner(me, k),),
            device_id_type=MESH,
        )

    def tell(k):
        return pltpu.make_async_remote_copy(
            src_ref=cnt_ref,
            dst_ref=all_ref.at[me],
            send_sem=cs_sems.at[k],
            recv_sem=cr_sems.at[k],
            device_id=(partner(me, k),),
            device_id_type=MESH,
        )

    own_counts = pltpu.make_async_copy(cnt_ref, all_ref.at[me], co_sem)

    def keep(d):
        return pltpu.make_async_copy(vbuf.at[d], next_ref.at[d], next_sems.at[d])

    def pack_first(k0, k1):
        @pl.loop(0, 2)
        def _(r):
            k = k0 + r * (k1 - k0)
            sbuf[k] = pack(partner(me, k), start, size)

    barrier = pltpu.get_barrier_semaphore()
    for k in range(1, n_dev):
        pl.semaphore_signal(barrier, inc=1, device_id=(partner(me, k),), device_id_type=MESH)
    pack_first(14, 15)
    pl.semaphore_wait(barrier, n_dev - 1)
    send(14).start()
    send(15).start()
    own_counts.start()

    @pl.loop(1, n_dev)
    def _(k):
        tell(k).start()

    pack_first(6, 8)
    pack_first(0, 1)

    @pl.loop(1, 7)
    def _(p):
        k0, k1 = pair_of(p)

        @pl.when(p <= 2)
        def _():
            send(13 + p).wait_send()

        @pl.when(p >= 3)
        def _():
            for k in pair_of(p - 2):
                send(k).wait_send()

        send(k0).start()
        send(k1).start()

        @pl.when(p < 6)
        def _():
            pack_first(*pair_of(p + 1))

        @pl.loop((n_dev * (p - 1)) // 6, (n_dev * p) // 6)
        def _(d):
            vbuf[d] = pack(d, start1, size1)

            @pl.when(d > 0)
            def _():
                keep(d - 1).start()

    keep(n_dev - 1).start()
    send(1).start()
    own = pltpu.make_async_copy(sbuf.at[0], got_ref.at[me], own_sem)
    own.start()
    for p in (5, 6):
        for k in pair_of(p):
            send(k).wait_send()
    send(1).wait_send()
    own.wait()
    own_counts.wait()

    @pl.loop(0, n_dev)
    def _(d):
        keep(d).wait()

    @pl.loop(1, n_dev)
    def _(k):
        tell(k).wait_send()
        tell(k).wait_recv()
        send(k).wait_recv()


def ffn_kernel(start, size, n_src, bound_ref, x_hbm, w1_hbm, w3_hbm, w2_hbm, out_ref, x_ref, w1, w3, w2, xbuf, hbuf, list_ref, low_ref, high_ref, used_ref, sems, x_sems):
    n_loc, _, ff = w1.shape
    n_f = ff // WIDE
    per = size // TILE

    def copy(e, which, f):
        cut = pl.ds(f * WIDE, WIDE)
        at = (e, cut) if which == 2 else (e, slice(None), cut)
        src, dst = ((w1_hbm, w1), (w3_hbm, w3), (w2_hbm, w2))[which]
        return pltpu.make_async_copy(src.at[at], dst.at[at], sems.at[e, which, f])

    quarter = x_ref.shape[0] // 4

    def row_copy(q):
        at = pl.ds(q * quarter, quarter)
        return pltpu.make_async_copy(x_hbm.at[at], x_ref.at[at], x_sems.at[q])

    for q in range(4):
        row_copy(q).start()

    @pl.loop(0, n_loc)
    def _(e):
        def need(s, any_):
            lo, hi = bound_ref[e, s], bound_ref[e + 1, s]
            return any_ | ((lo < start + size) & (hi > start) & (hi > lo)).astype(I32)

        used = lax.fori_loop(0, n_src, need, jnp.int32(0))
        used_ref[e] = used

        @pl.when(used > 0)
        def _():
            @pl.loop(0, n_f)
            def _(f):
                copy(e, 0, f).start()
                copy(e, 1, f).start()

            @pl.loop(0, n_f)
            def _(f):
                copy(e, 2, f).start()

    out_ref[...] = jnp.zeros_like(out_ref)
    for q in range(4):
        row_copy(q).wait()

    @pl.loop(0, n_loc)
    def _(e):
        @pl.when(used_ref[e] > 0)
        def _():
            def collect(s, cnt):
                lo = jnp.clip(bound_ref[e, s] - start, 0, size)
                hi = jnp.clip(bound_ref[e + 1, s] - start, 0, size)
                t_lo = lo // TILE
                t_hi = jnp.where(hi > lo, (hi + TILE - 1) // TILE, t_lo)

                def add(t, k):
                    list_ref[k] = s * per + t
                    low_ref[k] = lo - t * TILE
                    high_ref[k] = hi - t * TILE
                    return k + 1

                return lax.fori_loop(t_lo, t_hi, add, cnt)

            cnt = lax.fori_loop(0, n_src, collect, jnp.int32(0))
            groups = (cnt + GROUP - 1) // GROUP

            @pl.loop(cnt, groups * GROUP)
            def _(k):
                list_ref[k] = 0
                low_ref[k] = 0
                high_ref[k] = 0

            def tile_of(g, j):
                return pl.ds(pl.multiple_of(list_ref[g * GROUP + j] * TILE, TILE), TILE)

            def columns(f):
                cut = pl.ds(f * WIDE if isinstance(f, int) else pl.multiple_of(f * WIDE, WIDE), WIDE)
                xb = xbuf[...]
                u = _dot(xb, w1[e, :, cut])
                v = _dot(xb, w3[e, :, cut])
                hbuf[:, cut] = (u * jax.nn.sigmoid(u) * v).astype(BF16)

            @pl.loop(0, groups)
            def _(g):
                for j in range(GROUP):
                    xbuf[j * TILE : (j + 1) * TILE, :] = x_ref[tile_of(g, j), :]

                @pl.when(g == 0)
                def _():
                    @pl.loop(0, n_f)
                    def _(f):
                        copy(e, 0, f).wait()
                        copy(e, 1, f).wait()
                        columns(f)

                    @pl.loop(0, n_f)
                    def _(f):
                        copy(e, 2, f).wait()

                @pl.when(g > 0)
                def _():
                    for f in range(n_f):
                        columns(f)

                y = _dot(hbuf[...], w2[e]).astype(BF16)
                row = lax.broadcasted_iota(I32, (TILE, 1), 0)
                for j in range(GROUP):
                    own = (row >= low_ref[g * GROUP + j]) & (row < high_ref[g * GROUP + j])
                    at = tile_of(g, j)
                    out_ref[at, :] = jnp.where(own, y[j * TILE : (j + 1) * TILE], out_ref[at, :])


def gated(cols, ids, rows):
    add = 0.0
    for k in range(2):
        pick = jnp.where(ids == cols[:, k : k + 1], 1.0, 0.0).astype(BF16)
        add = add + cols[:, 2 + k : 3 + k] * _dot(pick, rows)
    return add


def bring_kernel(row_cap, n_dev, chunks, made_ref, back_hbm, cols_ref, out_ref, back, got, acc, rows_ref, send_sems, recv_sems, own_sem, back_sems):
    me = lax.axis_index("ep")
    (start, size), (start1, size1) = chunks
    tok = cols_ref.shape[0]
    block = 512

    def send(k):
        return pltpu.make_async_remote_copy(
            src_ref=made_ref.at[partner(me, k)],
            dst_ref=got.at[me],
            send_sem=send_sems.at[k],
            recv_sem=recv_sems.at[k],
            device_id=(partner(me, k),),
            device_id_type=MESH,
        )

    def fetch(g):
        at = pl.ds(pl.multiple_of(g * 2 * size, 2 * size), 2 * size)
        return pltpu.make_async_copy(back_hbm.at[at], back.at[at], back_sems.at[g])

    barrier = pltpu.get_barrier_semaphore()
    for k in range(1, n_dev):
        pl.semaphore_signal(barrier, inc=1, device_id=(partner(me, k),), device_id_type=MESH)
    groups = n_dev // 2

    @pl.loop(0, groups)
    def _(g):
        fetch(g).start()

    acc[...] = jnp.zeros_like(acc)
    pl.semaphore_wait(barrier, n_dev - 1)
    send(14).start()
    send(15).start()
    send(1).start()
    own = pltpu.make_async_copy(made_ref.at[me], got.at[me], own_sem)
    own.start()
    lane = lax.broadcasted_iota(I32, (1, 2 * size), 1)

    @pl.loop(1, 9)
    def _(p):
        @pl.when(p <= 2)
        def _():
            send(13 + p).wait_send()

        @pl.when(p >= 3)
        def _():
            for k in pair_of(p - 2):
                send(k).wait_send()

        @pl.when(p <= 6)
        def _():
            for k in pair_of(p):
                send(k).start()

        low = jnp.minimum((groups * (p - 1)) // 6, groups)
        high = jnp.minimum((groups * p) // 6, groups)
        near, far = pair_of(p - 2)
        k0 = jnp.where(p == 1, 0, jnp.where(p == 2, 14, near))
        k1 = jnp.where(p == 1, 1, jnp.where(p == 2, 15, far))
        d0, d1 = partner(me, k0), partner(me, k1)

        @pl.loop(low, high + 1)
        def _(g):
            @pl.when(g < high)
            def _():
                fetch(g).wait()
                rows_ref[...] = back[pl.ds(pl.multiple_of(g * 2 * size, 2 * size), 2 * size), :]

            @pl.when(g == high)
            def _():
                @pl.when(p == 1)
                def _():
                    own.wait()

                @pl.when(p > 1)
                def _():
                    send(k0).wait_recv()

                send(k1).wait_recv()
                rows_ref[:size1, :] = got[d0]
                rows_ref[size1:, :] = got[d1]

            at0 = jnp.where(g < high, 2 * g * row_cap + start, d0 * row_cap + start1)
            at1 = jnp.where(g < high, (2 * g + 1) * row_cap + start, d1 * row_cap + start1)
            ids = jnp.where(lane < size, at0 + lane, at1 + lane - size).astype(F32)
            rows = rows_ref[...]
            for t in range(tok // block):
                at = slice(t * block, (t + 1) * block)
                acc[at, :] += gated(cols_ref[at, :], ids, rows)

    out_ref[...] = acc[...].astype(BF16)
    send(1).wait_send()


def _params(vmem_limit_bytes=VMEM_BYTES):
    return pltpu.CompilerParams(vmem_limit_bytes=vmem_limit_bytes)


def solution(mesh):
    n = mesh.shape["ep"]

    def body(x, w_router, ids, w1, w3, w2):
        tok, dim = x.shape
        local = w1.shape[0]
        ff = w1.shape[2]
        n_exp = n * local
        cap = 4 * tok // n
        slots, cols, counts = pl.pallas_call(
            functools.partial(route_kernel, local, cap),
            out_shape=(
                jax.ShapeDtypeStruct((8, tok), I32),
                jax.ShapeDtypeStruct((tok, 8), F32),
                jax.ShapeDtypeStruct((n_exp, 128), I32),
            ),
            compiler_params=_params(),
            name="route",
        )(x, w_router.T, ids.T)
        smem = pl.BlockSpec(memory_space=pltpu.SMEM)
        vmem = pl.BlockSpec(memory_space=pltpu.VMEM)
        hbm = pl.BlockSpec(memory_space=pl.ANY)
        ship = pl.pallas_call(
            functools.partial(ship_kernel, cap, n, CHUNKS),
            in_specs=[vmem, vmem, vmem],
            out_specs=[hbm, hbm, hbm],
            out_shape=[jax.ShapeDtypeStruct((n, size, dim), BF16) for _, size in CHUNKS]
            + [jax.ShapeDtypeStruct((n,) + counts.shape, I32)],
            scratch_shapes=[
                pltpu.VMEM((n, CHUNKS[0][1], dim), BF16),
                pltpu.VMEM((n, CHUNKS[1][1], dim), BF16),
                pltpu.SemaphoreType.DMA((n,)),
                pltpu.SemaphoreType.DMA((n,)),
                pltpu.SemaphoreType.DMA,
                pltpu.SemaphoreType.DMA((n,)),
                pltpu.SemaphoreType.DMA((n,)),
                pltpu.SemaphoreType.DMA((n,)),
                pltpu.SemaphoreType.DMA,
            ],
            compiler_params=pltpu.CompilerParams(
                vmem_limit_bytes=VMEM_BYTES, collective_id=0, has_side_effects=True
            ),
            cost_estimate=pl.CostEstimate(flops=10**11, bytes_accessed=1, transcendentals=0),
            name="ship",
        )
        first_rows, second_rows, every = ship(slots, counts, x)
        at = lax.axis_index("ep") * local
        per_exp = lax.dynamic_slice(every, (0, at, 0), (n, local, 1))[:, :, 0]
        ends = jnp.cumsum(per_exp, axis=1).T
        bounds = jnp.concatenate([jnp.zeros((1, n), I32), ends], axis=0)
        for index, (start, size) in enumerate(CHUNKS):
            if index == 0:
                got = first_rows
            else:
                got = lax.all_to_all(second_rows, "ep", 0, 0, tiled=True)
            rows = n * size
            made = pl.pallas_call(
                functools.partial(ffn_kernel, start, size, n),
                in_specs=[smem, hbm, hbm, hbm, hbm],
                out_specs=vmem,
                scratch_shapes=[
                    pltpu.VMEM((rows, dim), BF16),
                    pltpu.VMEM((local, dim, ff), BF16),
                    pltpu.VMEM((local, dim, ff), BF16),
                    pltpu.VMEM((local, ff, dim), BF16),
                    pltpu.VMEM((STEP, dim), BF16),
                    pltpu.VMEM((STEP, ff), BF16),
                    pltpu.SMEM((rows // TILE + GROUP,), I32),
                    pltpu.SMEM((rows // TILE + GROUP,), I32),
                    pltpu.SMEM((rows // TILE + GROUP,), I32),
                    pltpu.SMEM((local,), I32),
                    pltpu.SemaphoreType.DMA((local, 3, ff // WIDE)),
                    pltpu.SemaphoreType.DMA((4,)),
                ],
                out_shape=jax.ShapeDtypeStruct((rows, dim), BF16),
                compiler_params=_params(),
                cost_estimate=pl.CostEstimate(flops=6 * rows * dim * ff, bytes_accessed=1, transcendentals=0),
            )
            made = made(bounds, got.reshape(rows, dim), w1, w3, w2)
            if index == 0:
                back = lax.all_to_all(made.reshape(n, size, dim), "ep", 0, 0, tiled=True)
        return pl.pallas_call(
            functools.partial(bring_kernel, cap, n, CHUNKS),
            in_specs=[hbm, hbm, vmem],
            out_specs=vmem,
            out_shape=jax.ShapeDtypeStruct((tok, dim), BF16),
            scratch_shapes=[
                pltpu.VMEM((n * CHUNKS[0][1], dim), BF16),
                pltpu.VMEM((n, CHUNKS[1][1], dim), BF16),
                pltpu.VMEM((tok, dim), F32),
                pltpu.VMEM((2 * CHUNKS[0][1], dim), BF16),
                pltpu.SemaphoreType.DMA((n,)),
                pltpu.SemaphoreType.DMA((n,)),
                pltpu.SemaphoreType.DMA,
                pltpu.SemaphoreType.DMA((n // 2,)),
            ],
            compiler_params=pltpu.CompilerParams(
                vmem_limit_bytes=VMEM_BYTES, collective_id=1, has_side_effects=True
            ),
            cost_estimate=pl.CostEstimate(flops=10**11, bytes_accessed=1, transcendentals=0),
            name="bring",
        )(made.reshape(n, CHUNKS[1][1], dim), back.reshape(n * CHUNKS[0][1], dim), cols)

    return jax.shard_map(
        body,
        mesh=mesh,
        in_specs=(P("ep", None), P(None, None), P("ep", None), P("ep", None, None), P("ep", None, None), P("ep", None, None)),
        out_specs=P("ep", None),
        check_vma=False,
    )
```

```python
import functools

import jax
import jax.numpy as jnp
from jax import lax
from jax.experimental import pallas as pl
from jax.experimental.pallas import tpu as pltpu
from jax.sharding import PartitionSpec as P


F32 = jnp.float32
BF16 = jnp.bfloat16
I32 = jnp.int32
TILE = 16
CHUNKS = ((0, 256), (256, 256))
VMEM_BYTES = 60 * 1024 * 1024


def _dot(a, b):
    return jnp.dot(a, b, preferred_element_type=F32)


def route_slots(local_count, row_cap, n_exp, ids_ref, slot_ref, cnt_ref):
    tok = ids_ref.shape[1]
    ids = ids_ref[...]
    id_a, id_b = ids[0:1], ids[1:2]
    row = lax.broadcasted_iota(I32, (n_exp, tok), 0)
    oh_a, oh_b = row == id_a, row == id_b
    zero = jnp.zeros((), F32)
    chosen = jnp.where(oh_a | oh_b, 1.0, 0.0).astype(F32)
    width = 256
    tri = lax.broadcasted_iota(I32, (width, width), 0) < lax.broadcasted_iota(I32, (width, width), 1)
    tri = jnp.where(tri, 1.0, 0.0).astype(BF16)
    before = jnp.zeros((n_exp, 1), F32)
    ranks = []
    for k in range(tok // width):
        blk = chosen[:, k * width : (k + 1) * width]
        ranks.append(_dot(blk.astype(BF16), tri) + before)
        before = before + jnp.sum(blk, axis=1, keepdims=True)
    rank = jnp.concatenate(ranks, axis=1)
    cnt_ref[...] = jnp.broadcast_to(before, cnt_ref.shape).astype(I32)

    def slot_of(ident, onehot):
        here = jnp.sum(jnp.where(onehot, rank, zero), axis=0, keepdims=True)
        dev = ident // local_count
        lower = (row < ident) & (row >= dev * local_count)
        base = jnp.sum(jnp.where(lower, jnp.broadcast_to(before, (n_exp, tok)), zero), axis=0, keepdims=True)
        return dev.astype(F32) * row_cap + here + base

    s_a, s_b = slot_of(id_a, oh_a), slot_of(id_b, oh_b)
    slot_ref[...] = jnp.concatenate([s_a, s_b] * 4, axis=0).astype(I32)


def route_gates(x_ref, wr_ref, ids_ref, slot_ref, cols_ref):
    tok = x_ref.shape[0]
    n_exp = wr_ref.shape[0]
    w = wr_ref[...]
    w_hi = w.astype(BF16)
    rest = w - w_hi.astype(F32)
    w_mid = rest.astype(BF16)
    w_lo = (rest - w_mid.astype(F32)).astype(BF16)
    nt = (((1,), (1,)), ((), ()))
    w_all = jnp.concatenate([w_hi, w_mid, w_lo], axis=0)
    parts = lax.dot_general(w_all, x_ref[...], nt, preferred_element_type=F32)
    logits = parts[:n_exp] + (parts[n_exp : 2 * n_exp] + parts[2 * n_exp :])
    ids = ids_ref[...]
    row = lax.broadcasted_iota(I32, (n_exp, tok), 0)
    zero = jnp.zeros((), F32)
    l_a = jnp.sum(jnp.where(row == ids[0:1], logits, zero), axis=0, keepdims=True)
    l_b = jnp.sum(jnp.where(row == ids[1:2], logits, zero), axis=0, keepdims=True)
    top = jnp.maximum(l_a, l_b)
    e_a, e_b = jnp.exp(l_a - top), jnp.exp(l_b - top)
    g_a, g_b = e_a / (e_a + e_b), e_b / (e_a + e_b)
    slots = slot_ref[0:2, :].astype(F32)
    cols_ref[...] = jnp.concatenate([slots, g_a, g_b, slots, g_a, g_b], axis=0).T


WIDE = 512
GROUP = 16
STEP = GROUP * TILE


MESH = pl.DeviceIdType.MESH


def partner(me, offset):
    other = me
    for bit in (1, 2, 4, 8):
        other = other + ((offset // bit) % 2) * (bit - 2 * bit * ((me // bit) % 2))
    return other


def pair_of(p):
    j, r = (p - 1) // 2, (p - 1) % 2
    near = 8 - 4 * j + 2 * (j // 2)
    return 14 - near + r, near + r


def ship_kernel(row_cap, n_dev, chunks, local, ids_ref, wr_ref, x_ref, got_ref, next_ref, all_ref, cols_ref, slot_ref, cnt_ref, sbuf, vbuf, send_sems, recv_sems, own_sem, next_sems, cs_sems, cr_sems, co_sem):
    me = lax.axis_index("ep")
    tok = x_ref.shape[0]
    (start, size), (start1, size1) = chunks

    def pack(dev, first, rows):
        want = lax.broadcasted_iota(I32, (rows, tok), 0) + (dev * row_cap + first)
        hit = (want == slot_ref[0:1, :]) | (want == slot_ref[1:2, :])
        pick = jnp.where(hit, 1.0, 0.0).astype(BF16)
        return _dot(pick, x_ref[...]).astype(BF16)

    def send(k):
        return pltpu.make_async_remote_copy(
            src_ref=sbuf.at[k],
            dst_ref=got_ref.at[me],
            send_sem=send_sems.at[k],
            recv_sem=recv_sems.at[k],
            device_id=(partner(me, k),),
            device_id_type=MESH,
        )

    def tell(k):
        return pltpu.make_async_remote_copy(
            src_ref=cnt_ref,
            dst_ref=all_ref.at[me],
            send_sem=cs_sems.at[k],
            recv_sem=cr_sems.at[k],
            device_id=(partner(me, k),),
            device_id_type=MESH,
        )

    own_counts = pltpu.make_async_copy(cnt_ref, all_ref.at[me], co_sem)

    def keep(d):
        return pltpu.make_async_copy(vbuf.at[d], next_ref.at[d], next_sems.at[d])

    def pack_first(k0, k1):
        @pl.loop(0, 2)
        def _(r):
            k = k0 + r * (k1 - k0)
            sbuf[k] = pack(partner(me, k), start, size)

    barrier = pltpu.get_barrier_semaphore()
    for k in range(1, n_dev):
        pl.semaphore_signal(barrier, inc=1, device_id=(partner(me, k),), device_id_type=MESH)
    route_slots(local, row_cap, wr_ref.shape[0], ids_ref, slot_ref, cnt_ref)
    pack_first(14, 15)
    pl.semaphore_wait(barrier, n_dev - 1)
    send(14).start()
    send(15).start()
    own_counts.start()

    @pl.loop(1, n_dev)
    def _(k):
        tell(k).start()

    pack_first(6, 8)

    @pl.loop(1, 7)
    def _(p):
        k0, k1 = pair_of(p)

        @pl.when(p <= 2)
        def _():
            send(13 + p).wait_send()

        @pl.when(p >= 3)
        def _():
            for k in pair_of(p - 2):
                send(k).wait_send()

        send(k0).start()
        send(k1).start()

        @pl.when(p < 6)
        def _():
            pack_first(*pair_of(p + 1))

        @pl.loop((n_dev * (p - 1)) // 6, (n_dev * p) // 6)
        def _(d):
            vbuf[d] = pack(d, start1, size1)

            @pl.when(d > 0)
            def _():
                keep(d - 1).start()

    pack_first(0, 1)
    keep(n_dev - 1).start()
    route_gates(x_ref, wr_ref, ids_ref, slot_ref, cols_ref)
    send(1).start()
    own = pltpu.make_async_copy(sbuf.at[0], got_ref.at[me], own_sem)
    own.start()
    for p in (5, 6):
        for k in pair_of(p):
            send(k).wait_send()
    send(1).wait_send()
    own.wait()
    own_counts.wait()

    @pl.loop(0, n_dev)
    def _(d):
        keep(d).wait()

    @pl.loop(1, n_dev)
    def _(k):
        tell(k).wait_send()
        tell(k).wait_recv()
        send(k).wait_recv()


def ffn_kernel(start, size, n_src, bound_ref, x_hbm, w1_hbm, w3_hbm, w2_hbm, out_ref, x_ref, w1, w3, w2, xbuf, hbuf, list_ref, low_ref, high_ref, used_ref, sems, x_sems):
    n_loc, _, ff = w1.shape
    n_f = ff // WIDE
    per = size // TILE

    def copy(e, which, f):
        cut = pl.ds(f * WIDE, WIDE)
        at = (e, cut) if which == 2 else (e, slice(None), cut)
        src, dst = ((w1_hbm, w1), (w3_hbm, w3), (w2_hbm, w2))[which]
        return pltpu.make_async_copy(src.at[at], dst.at[at], sems.at[e, which, f])

    quarter = x_ref.shape[0] // 4

    def row_copy(q):
        at = pl.ds(q * quarter, quarter)
        return pltpu.make_async_copy(x_hbm.at[at], x_ref.at[at], x_sems.at[q])

    for q in range(4):
        row_copy(q).start()

    @pl.loop(0, n_loc)
    def _(e):
        def need(s, any_):
            lo, hi = bound_ref[e, s], bound_ref[e + 1, s]
            return any_ | ((lo < start + size) & (hi > start) & (hi > lo)).astype(I32)

        used = lax.fori_loop(0, n_src, need, jnp.int32(0))
        used_ref[e] = used

        @pl.when(used > 0)
        def _():
            @pl.loop(0, n_f)
            def _(f):
                copy(e, 0, f).start()
                copy(e, 1, f).start()

            @pl.loop(0, n_f)
            def _(f):
                copy(e, 2, f).start()

    out_ref[...] = jnp.zeros_like(out_ref)
    for q in range(4):
        row_copy(q).wait()

    @pl.loop(0, n_loc)
    def _(e):
        @pl.when(used_ref[e] > 0)
        def _():
            def collect(s, cnt):
                lo = jnp.clip(bound_ref[e, s] - start, 0, size)
                hi = jnp.clip(bound_ref[e + 1, s] - start, 0, size)
                t_lo = lo // TILE
                t_hi = jnp.where(hi > lo, (hi + TILE - 1) // TILE, t_lo)

                def add(t, k):
                    list_ref[k] = s * per + t
                    low_ref[k] = lo - t * TILE
                    high_ref[k] = hi - t * TILE
                    return k + 1

                return lax.fori_loop(t_lo, t_hi, add, cnt)

            cnt = lax.fori_loop(0, n_src, collect, jnp.int32(0))
            groups = (cnt + GROUP - 1) // GROUP

            @pl.loop(cnt, groups * GROUP)
            def _(k):
                list_ref[k] = 0
                low_ref[k] = 0
                high_ref[k] = 0

            def tile_of(g, j):
                return pl.ds(pl.multiple_of(list_ref[g * GROUP + j] * TILE, TILE), TILE)

            def columns(f):
                cut = pl.ds(f * WIDE if isinstance(f, int) else pl.multiple_of(f * WIDE, WIDE), WIDE)
                xb = xbuf[...]
                u = _dot(xb, w1[e, :, cut])
                v = _dot(xb, w3[e, :, cut])
                hbuf[:, cut] = (u * jax.nn.sigmoid(u) * v).astype(BF16)

            @pl.loop(0, groups)
            def _(g):
                for j in range(GROUP):
                    xbuf[j * TILE : (j + 1) * TILE, :] = x_ref[tile_of(g, j), :]

                @pl.when(g == 0)
                def _():
                    @pl.loop(0, n_f)
                    def _(f):
                        copy(e, 0, f).wait()
                        copy(e, 1, f).wait()
                        columns(f)

                    @pl.loop(0, n_f)
                    def _(f):
                        copy(e, 2, f).wait()

                @pl.when(g > 0)
                def _():
                    for f in range(n_f):
                        columns(f)

                y = _dot(hbuf[...], w2[e]).astype(BF16)
                row = lax.broadcasted_iota(I32, (TILE, 1), 0)
                for j in range(GROUP):
                    own = (row >= low_ref[g * GROUP + j]) & (row < high_ref[g * GROUP + j])
                    at = tile_of(g, j)
                    out_ref[at, :] = jnp.where(own, y[j * TILE : (j + 1) * TILE], out_ref[at, :])


def gated(cols, ids, rows):
    add = 0.0
    for k in range(2):
        pick = jnp.where(ids == cols[:, k : k + 1], 1.0, 0.0).astype(BF16)
        add = add + cols[:, 2 + k : 3 + k] * _dot(pick, rows)
    return add


def bring_kernel(row_cap, n_dev, chunks, made_ref, back_hbm, cols_ref, out_ref, back, got, acc, rows_ref, send_sems, recv_sems, own_sem, back_sems):
    me = lax.axis_index("ep")
    (start, size), (start1, size1) = chunks
    tok = cols_ref.shape[0]
    block = 512

    def send(k):
        return pltpu.make_async_remote_copy(
            src_ref=made_ref.at[partner(me, k)],
            dst_ref=got.at[me],
            send_sem=send_sems.at[k],
            recv_sem=recv_sems.at[k],
            device_id=(partner(me, k),),
            device_id_type=MESH,
        )

    def fetch(g):
        at = pl.ds(pl.multiple_of(g * 2 * size, 2 * size), 2 * size)
        return pltpu.make_async_copy(back_hbm.at[at], back.at[at], back_sems.at[g])

    barrier = pltpu.get_barrier_semaphore()
    for k in range(1, n_dev):
        pl.semaphore_signal(barrier, inc=1, device_id=(partner(me, k),), device_id_type=MESH)
    groups = n_dev // 2

    @pl.loop(0, groups)
    def _(g):
        fetch(g).start()

    acc[...] = jnp.zeros_like(acc)
    pl.semaphore_wait(barrier, n_dev - 1)
    send(14).start()
    send(15).start()
    send(1).start()
    own = pltpu.make_async_copy(made_ref.at[me], got.at[me], own_sem)
    own.start()
    lane = lax.broadcasted_iota(I32, (1, 2 * size), 1)

    @pl.loop(1, 9)
    def _(p):
        @pl.when(p <= 2)
        def _():
            send(13 + p).wait_send()

        @pl.when(p >= 3)
        def _():
            for k in pair_of(p - 2):
                send(k).wait_send()

        @pl.when(p <= 6)
        def _():
            for k in pair_of(p):
                send(k).start()

        low = jnp.minimum((groups * (p - 1)) // 6, groups)
        high = jnp.minimum((groups * p) // 6, groups)
        near, far = pair_of(p - 2)
        k0 = jnp.where(p == 1, 0, jnp.where(p == 2, 14, near))
        k1 = jnp.where(p == 1, 1, jnp.where(p == 2, 15, far))
        d0, d1 = partner(me, k0), partner(me, k1)

        @pl.loop(low, high + 1)
        def _(g):
            @pl.when(g < high)
            def _():
                fetch(g).wait()
                rows_ref[...] = back[pl.ds(pl.multiple_of(g * 2 * size, 2 * size), 2 * size), :]

            @pl.when(g == high)
            def _():
                @pl.when(p == 1)
                def _():
                    own.wait()

                @pl.when(p > 1)
                def _():
                    send(k0).wait_recv()

                send(k1).wait_recv()
                rows_ref[:size1, :] = got[d0]
                rows_ref[size1:, :] = got[d1]

            at0 = jnp.where(g < high, 2 * g * row_cap + start, d0 * row_cap + start1)
            at1 = jnp.where(g < high, (2 * g + 1) * row_cap + start, d1 * row_cap + start1)
            ids = jnp.where(lane < size, at0 + lane, at1 + lane - size).astype(F32)
            rows = rows_ref[...]
            for t in range(tok // block):
                at = slice(t * block, (t + 1) * block)
                acc[at, :] += gated(cols_ref[at, :], ids, rows)

    out_ref[...] = acc[...].astype(BF16)
    send(1).wait_send()


def _params(vmem_limit_bytes=VMEM_BYTES):
    return pltpu.CompilerParams(vmem_limit_bytes=vmem_limit_bytes)


def solution(mesh):
    n = mesh.shape["ep"]

    def body(x, w_router, ids, w1, w3, w2):
        tok, dim = x.shape
        local = w1.shape[0]
        ff = w1.shape[2]
        n_exp = n * local
        cap = 4 * tok // n
        smem = pl.BlockSpec(memory_space=pltpu.SMEM)
        vmem = pl.BlockSpec(memory_space=pltpu.VMEM)
        hbm = pl.BlockSpec(memory_space=pl.ANY)
        ship = pl.pallas_call(
            functools.partial(ship_kernel, cap, n, CHUNKS, local),
            in_specs=[vmem, vmem, vmem],
            out_specs=[hbm, hbm, hbm, vmem],
            out_shape=[jax.ShapeDtypeStruct((n, size, dim), BF16) for _, size in CHUNKS]
            + [jax.ShapeDtypeStruct((n, n_exp, 128), I32), jax.ShapeDtypeStruct((tok, 8), F32)],
            scratch_shapes=[
                pltpu.VMEM((8, tok), I32),
                pltpu.VMEM((n_exp, 128), I32),
                pltpu.VMEM((n, CHUNKS[0][1], dim), BF16),
                pltpu.VMEM((n, CHUNKS[1][1], dim), BF16),
                pltpu.SemaphoreType.DMA((n,)),
                pltpu.SemaphoreType.DMA((n,)),
                pltpu.SemaphoreType.DMA,
                pltpu.SemaphoreType.DMA((n,)),
                pltpu.SemaphoreType.DMA((n,)),
                pltpu.SemaphoreType.DMA((n,)),
                pltpu.SemaphoreType.DMA,
            ],
            compiler_params=pltpu.CompilerParams(
                vmem_limit_bytes=VMEM_BYTES, collective_id=0, has_side_effects=True
            ),
            cost_estimate=pl.CostEstimate(flops=10**11, bytes_accessed=1, transcendentals=0),
            name="ship",
        )
        first_rows, second_rows, every, cols = ship(ids.T, w_router.T, x)
        at = lax.axis_index("ep") * local
        per_exp = lax.dynamic_slice(every, (0, at, 0), (n, local, 1))[:, :, 0]
        ends = jnp.cumsum(per_exp, axis=1).T
        bounds = jnp.concatenate([jnp.zeros((1, n), I32), ends], axis=0)
        for index, (start, size) in enumerate(CHUNKS):
            if index == 0:
                got = first_rows
            else:
                got = lax.all_to_all(second_rows, "ep", 0, 0, tiled=True)
            rows = n * size
            made = pl.pallas_call(
                functools.partial(ffn_kernel, start, size, n),
                in_specs=[smem, hbm, hbm, hbm, hbm],
                out_specs=vmem,
                scratch_shapes=[
                    pltpu.VMEM((rows, dim), BF16),
                    pltpu.VMEM((local, dim, ff), BF16),
                    pltpu.VMEM((local, dim, ff), BF16),
                    pltpu.VMEM((local, ff, dim), BF16),
                    pltpu.VMEM((STEP, dim), BF16),
                    pltpu.VMEM((STEP, ff), BF16),
                    pltpu.SMEM((rows // TILE + GROUP,), I32),
                    pltpu.SMEM((rows // TILE + GROUP,), I32),
                    pltpu.SMEM((rows // TILE + GROUP,), I32),
                    pltpu.SMEM((local,), I32),
                    pltpu.SemaphoreType.DMA((local, 3, ff // WIDE)),
                    pltpu.SemaphoreType.DMA((4,)),
                ],
                out_shape=jax.ShapeDtypeStruct((rows, dim), BF16),
                compiler_params=_params(),
                cost_estimate=pl.CostEstimate(flops=6 * rows * dim * ff, bytes_accessed=1, transcendentals=0),
            )
            made = made(bounds, got.reshape(rows, dim), w1, w3, w2)
            if index == 0:
                back = lax.all_to_all(made.reshape(n, size, dim), "ep", 0, 0, tiled=True)
        return pl.pallas_call(
            functools.partial(bring_kernel, cap, n, CHUNKS),
            in_specs=[hbm, hbm, vmem],
            out_specs=vmem,
            out_shape=jax.ShapeDtypeStruct((tok, dim), BF16),
            scratch_shapes=[
                pltpu.VMEM((n * CHUNKS[0][1], dim), BF16),
                pltpu.VMEM((n, CHUNKS[1][1], dim), BF16),
                pltpu.VMEM((tok, dim), F32),
                pltpu.VMEM((2 * CHUNKS[0][1], dim), BF16),
                pltpu.SemaphoreType.DMA((n,)),
                pltpu.SemaphoreType.DMA((n,)),
                pltpu.SemaphoreType.DMA,
                pltpu.SemaphoreType.DMA((n // 2,)),
            ],
            compiler_params=pltpu.CompilerParams(
                vmem_limit_bytes=VMEM_BYTES, collective_id=1, has_side_effects=True
            ),
            cost_estimate=pl.CostEstimate(flops=10**11, bytes_accessed=1, transcendentals=0),
            name="bring",
        )(made.reshape(n, CHUNKS[1][1], dim), back.reshape(n * CHUNKS[0][1], dim), cols)

    return jax.shard_map(
        body,
        mesh=mesh,
        in_specs=(P("ep", None), P(None, None), P("ep", None), P("ep", None, None), P("ep", None, None), P("ep", None, None)),
        out_specs=P("ep", None),
        check_vma=False,
    )
```

```python
import functools

import jax
import jax.numpy as jnp
from jax import lax
from jax.experimental import pallas as pl
from jax.experimental.pallas import tpu as pltpu
from jax.sharding import PartitionSpec as P


F32 = jnp.float32
BF16 = jnp.bfloat16
I32 = jnp.int32
TILE = 16
CHUNKS = ((0, 256), (256, 256))
VMEM_BYTES = 60 * 1024 * 1024


def _dot(a, b):
    return jnp.dot(a, b, preferred_element_type=F32)


def route_slots(local_count, row_cap, n_exp, ids_ref, slot_ref, cnt_ref):
    tok = ids_ref.shape[1]
    ids = ids_ref[...]
    id_a, id_b = ids[0:1], ids[1:2]
    row = lax.broadcasted_iota(I32, (n_exp, tok), 0)
    oh_a, oh_b = row == id_a, row == id_b
    zero = jnp.zeros((), F32)
    chosen = jnp.where(oh_a | oh_b, 1.0, 0.0).astype(F32)
    width = 256
    tri = lax.broadcasted_iota(I32, (width, width), 0) < lax.broadcasted_iota(I32, (width, width), 1)
    tri = jnp.where(tri, 1.0, 0.0).astype(BF16)
    before = jnp.zeros((n_exp, 1), F32)
    ranks = []
    for k in range(tok // width):
        blk = chosen[:, k * width : (k + 1) * width]
        ranks.append(_dot(blk.astype(BF16), tri) + before)
        before = before + jnp.sum(blk, axis=1, keepdims=True)
    rank = jnp.concatenate(ranks, axis=1)
    cnt_ref[...] = jnp.broadcast_to(before, cnt_ref.shape).astype(I32)

    def slot_of(ident, onehot):
        here = jnp.sum(jnp.where(onehot, rank, zero), axis=0, keepdims=True)
        dev = ident // local_count
        lower = (row < ident) & (row >= dev * local_count)
        base = jnp.sum(jnp.where(lower, jnp.broadcast_to(before, (n_exp, tok)), zero), axis=0, keepdims=True)
        return dev.astype(F32) * row_cap + here + base

    s_a, s_b = slot_of(id_a, oh_a), slot_of(id_b, oh_b)
    slot_ref[...] = jnp.concatenate([s_a, s_b] * 4, axis=0).astype(I32)


def route_gates(x_ref, wr_ref, ids_ref, slot_ref, cols_ref):
    tok = x_ref.shape[0]
    n_exp = wr_ref.shape[0]
    w = wr_ref[...]
    w_hi = w.astype(BF16)
    rest = w - w_hi.astype(F32)
    w_mid = rest.astype(BF16)
    w_lo = (rest - w_mid.astype(F32)).astype(BF16)
    nt = (((1,), (1,)), ((), ()))
    w_all = jnp.concatenate([w_hi, w_mid, w_lo], axis=0)
    parts = lax.dot_general(w_all, x_ref[...], nt, preferred_element_type=F32)
    logits = parts[:n_exp] + (parts[n_exp : 2 * n_exp] + parts[2 * n_exp :])
    ids = ids_ref[...]
    row = lax.broadcasted_iota(I32, (n_exp, tok), 0)
    zero = jnp.zeros((), F32)
    l_a = jnp.sum(jnp.where(row == ids[0:1], logits, zero), axis=0, keepdims=True)
    l_b = jnp.sum(jnp.where(row == ids[1:2], logits, zero), axis=0, keepdims=True)
    top = jnp.maximum(l_a, l_b)
    e_a, e_b = jnp.exp(l_a - top), jnp.exp(l_b - top)
    g_a, g_b = e_a / (e_a + e_b), e_b / (e_a + e_b)
    slots = slot_ref[0:2, :].astype(F32)
    cols_ref[...] = jnp.concatenate([slots, g_a, g_b, slots, g_a, g_b], axis=0).T


WIDE = 512
GROUP = 16
STEP = GROUP * TILE


MESH = pl.DeviceIdType.MESH


def partner(me, offset):
    other = me
    for bit in (1, 2, 4, 8):
        other = other + ((offset // bit) % 2) * (bit - 2 * bit * ((me // bit) % 2))
    return other


def pair_of(p):
    j, r = (p - 1) // 2, (p - 1) % 2
    near = 8 - 4 * j + 2 * (j // 2)
    return 14 - near + r, near + r


def ship_kernel(row_cap, n_dev, chunks, slot_ref, cnt_ref, ids_ref, wr_ref, x_ref, got_ref, next_ref, all_ref, cols_ref, sbuf, vbuf, send_sems, recv_sems, own_sem, next_sems, cs_sems, cr_sems, co_sem):
    me = lax.axis_index("ep")
    tok = x_ref.shape[0]
    (start, size), (start1, size1) = chunks

    def pack(dev, first, rows):
        want = lax.broadcasted_iota(I32, (rows, tok), 0) + (dev * row_cap + first)
        hit = (want == slot_ref[0:1, :]) | (want == slot_ref[1:2, :])
        pick = jnp.where(hit, 1.0, 0.0).astype(BF16)
        return _dot(pick, x_ref[...]).astype(BF16)

    def send(k):
        return pltpu.make_async_remote_copy(
            src_ref=sbuf.at[k],
            dst_ref=got_ref.at[me],
            send_sem=send_sems.at[k],
            recv_sem=recv_sems.at[k],
            device_id=(partner(me, k),),
            device_id_type=MESH,
        )

    def tell(k):
        return pltpu.make_async_remote_copy(
            src_ref=cnt_ref,
            dst_ref=all_ref.at[me],
            send_sem=cs_sems.at[k],
            recv_sem=cr_sems.at[k],
            device_id=(partner(me, k),),
            device_id_type=MESH,
        )

    own_counts = pltpu.make_async_copy(cnt_ref, all_ref.at[me], co_sem)

    def keep(d):
        return pltpu.make_async_copy(vbuf.at[d], next_ref.at[d], next_sems.at[d])

    def pack_first(k0, k1):
        @pl.loop(0, 2)
        def _(r):
            k = k0 + r * (k1 - k0)
            sbuf[k] = pack(partner(me, k), start, size)

    barrier = pltpu.get_barrier_semaphore()
    for k in range(1, n_dev):
        pl.semaphore_signal(barrier, inc=1, device_id=(partner(me, k),), device_id_type=MESH)
    pack_first(14, 15)
    pl.semaphore_wait(barrier, n_dev - 1)
    send(14).start()
    send(15).start()
    own_counts.start()

    @pl.loop(1, n_dev)
    def _(k):
        tell(k).start()

    pack_first(6, 8)

    @pl.loop(1, 7)
    def _(p):
        k0, k1 = pair_of(p)

        @pl.when(p <= 2)
        def _():
            send(13 + p).wait_send()

        @pl.when(p >= 3)
        def _():
            for k in pair_of(p - 2):
                send(k).wait_send()

        send(k0).start()
        send(k1).start()

        @pl.when(p < 6)
        def _():
            pack_first(*pair_of(p + 1))

        @pl.when(p == 6)
        def _():
            pack_first(0, 1)

        @pl.loop((n_dev * (p - 1)) // 6, (n_dev * p) // 6)
        def _(d):
            vbuf[d] = pack(d, start1, size1)

            @pl.when(d > 0)
            def _():
                keep(d - 1).start()

    send(1).start()
    own = pltpu.make_async_copy(sbuf.at[0], got_ref.at[me], own_sem)
    own.start()
    route_gates(x_ref, wr_ref, ids_ref, slot_ref, cols_ref)
    keep(n_dev - 1).start()
    for p in (5, 6):
        for k in pair_of(p):
            send(k).wait_send()
    send(1).wait_send()
    own.wait()
    own_counts.wait()

    @pl.loop(0, n_dev)
    def _(d):
        keep(d).wait()

    @pl.loop(1, n_dev)
    def _(k):
        tell(k).wait_send()
        tell(k).wait_recv()
        send(k).wait_recv()


def ffn_kernel(start, size, n_src, bound_ref, x_hbm, w1_hbm, w3_hbm, w2_hbm, out_ref, x_ref, w1, w3, w2, xbuf, hbuf, list_ref, low_ref, high_ref, used_ref, sems, x_sems):
    n_loc, _, ff = w1.shape
    n_f = ff // WIDE
    per = size // TILE

    def copy(e, which, f):
        cut = pl.ds(f * WIDE, WIDE)
        at = (e, cut) if which == 2 else (e, slice(None), cut)
        src, dst = ((w1_hbm, w1), (w3_hbm, w3), (w2_hbm, w2))[which]
        return pltpu.make_async_copy(src.at[at], dst.at[at], sems.at[e, which, f])

    quarter = x_ref.shape[0] // 4

    def row_copy(q):
        at = pl.ds(q * quarter, quarter)
        return pltpu.make_async_copy(x_hbm.at[at], x_ref.at[at], x_sems.at[q])

    for q in range(4):
        row_copy(q).start()

    @pl.loop(0, n_loc)
    def _(e):
        def need(s, any_):
            lo, hi = bound_ref[e, s], bound_ref[e + 1, s]
            return any_ | ((lo < start + size) & (hi > start) & (hi > lo)).astype(I32)

        used = lax.fori_loop(0, n_src, need, jnp.int32(0))
        used_ref[e] = used

        @pl.when(used > 0)
        def _():
            @pl.loop(0, n_f)
            def _(f):
                copy(e, 0, f).start()
                copy(e, 1, f).start()

            @pl.loop(0, n_f)
            def _(f):
                copy(e, 2, f).start()

    out_ref[...] = jnp.zeros_like(out_ref)
    for q in range(4):
        row_copy(q).wait()

    @pl.loop(0, n_loc)
    def _(e):
        @pl.when(used_ref[e] > 0)
        def _():
            def collect(s, cnt):
                lo = jnp.clip(bound_ref[e, s] - start, 0, size)
                hi = jnp.clip(bound_ref[e + 1, s] - start, 0, size)
                t_lo = lo // TILE
                t_hi = jnp.where(hi > lo, (hi + TILE - 1) // TILE, t_lo)

                def add(t, k):
                    list_ref[k] = s * per + t
                    low_ref[k] = lo - t * TILE
                    high_ref[k] = hi - t * TILE
                    return k + 1

                return lax.fori_loop(t_lo, t_hi, add, cnt)

            cnt = lax.fori_loop(0, n_src, collect, jnp.int32(0))
            groups = (cnt + GROUP - 1) // GROUP

            @pl.loop(cnt, groups * GROUP)
            def _(k):
                list_ref[k] = 0
                low_ref[k] = 0
                high_ref[k] = 0

            def tile_of(g, j):
                return pl.ds(pl.multiple_of(list_ref[g * GROUP + j] * TILE, TILE), TILE)

            def columns(f):
                cut = pl.ds(f * WIDE if isinstance(f, int) else pl.multiple_of(f * WIDE, WIDE), WIDE)
                xb = xbuf[...]
                u = _dot(xb, w1[e, :, cut])
                v = _dot(xb, w3[e, :, cut])
                hbuf[:, cut] = (u * jax.nn.sigmoid(u) * v).astype(BF16)

            @pl.loop(0, groups)
            def _(g):
                for j in range(GROUP):
                    xbuf[j * TILE : (j + 1) * TILE, :] = x_ref[tile_of(g, j), :]

                @pl.when(g == 0)
                def _():
                    @pl.loop(0, n_f)
                    def _(f):
                        copy(e, 0, f).wait()
                        copy(e, 1, f).wait()
                        columns(f)

                    @pl.loop(0, n_f)
                    def _(f):
                        copy(e, 2, f).wait()

                @pl.when(g > 0)
                def _():
                    for f in range(n_f):
                        columns(f)

                y = _dot(hbuf[...], w2[e]).astype(BF16)
                row = lax.broadcasted_iota(I32, (TILE, 1), 0)
                for j in range(GROUP):
                    own = (row >= low_ref[g * GROUP + j]) & (row < high_ref[g * GROUP + j])
                    at = tile_of(g, j)
                    out_ref[at, :] = jnp.where(own, y[j * TILE : (j + 1) * TILE], out_ref[at, :])


def gated(cols, ids, rows):
    add = 0.0
    for k in range(2):
        pick = jnp.where(ids == cols[:, k : k + 1], 1.0, 0.0).astype(BF16)
        add = add + cols[:, 2 + k : 3 + k] * _dot(pick, rows)
    return add


def bring_kernel(row_cap, n_dev, chunks, made_ref, back_hbm, cols_ref, out_ref, back, got, acc, rows_ref, send_sems, recv_sems, own_sem, back_sems):
    me = lax.axis_index("ep")
    (start, size), (start1, size1) = chunks
    tok = cols_ref.shape[0]
    block = 512

    def send(k):
        return pltpu.make_async_remote_copy(
            src_ref=made_ref.at[partner(me, k)],
            dst_ref=got.at[me],
            send_sem=send_sems.at[k],
            recv_sem=recv_sems.at[k],
            device_id=(partner(me, k),),
            device_id_type=MESH,
        )

    def fetch(g):
        at = pl.ds(pl.multiple_of(g * 2 * size, 2 * size), 2 * size)
        return pltpu.make_async_copy(back_hbm.at[at], back.at[at], back_sems.at[g])

    barrier = pltpu.get_barrier_semaphore()
    for k in range(1, n_dev):
        pl.semaphore_signal(barrier, inc=1, device_id=(partner(me, k),), device_id_type=MESH)
    groups = n_dev // 2

    @pl.loop(0, groups)
    def _(g):
        fetch(g).start()

    acc[...] = jnp.zeros_like(acc)
    pl.semaphore_wait(barrier, n_dev - 1)
    send(14).start()
    send(15).start()
    send(1).start()
    own = pltpu.make_async_copy(made_ref.at[me], got.at[me], own_sem)
    own.start()
    lane = lax.broadcasted_iota(I32, (1, 2 * size), 1)

    @pl.loop(1, 9)
    def _(p):
        @pl.when(p <= 2)
        def _():
            send(13 + p).wait_send()

        @pl.when(p >= 3)
        def _():
            for k in pair_of(p - 2):
                send(k).wait_send()

        @pl.when(p <= 6)
        def _():
            for k in pair_of(p):
                send(k).start()

        low = jnp.minimum((groups * (p - 1)) // 6, groups)
        high = jnp.minimum((groups * p) // 6, groups)
        near, far = pair_of(p - 2)
        k0 = jnp.where(p == 1, 0, jnp.where(p == 2, 14, near))
        k1 = jnp.where(p == 1, 1, jnp.where(p == 2, 15, far))
        d0, d1 = partner(me, k0), partner(me, k1)

        @pl.loop(low, high + 1)
        def _(g):
            @pl.when(g < high)
            def _():
                fetch(g).wait()
                rows_ref[...] = back[pl.ds(pl.multiple_of(g * 2 * size, 2 * size), 2 * size), :]

            @pl.when(g == high)
            def _():
                @pl.when(p == 1)
                def _():
                    own.wait()

                @pl.when(p > 1)
                def _():
                    send(k0).wait_recv()

                send(k1).wait_recv()
                rows_ref[:size1, :] = got[d0]
                rows_ref[size1:, :] = got[d1]

            at0 = jnp.where(g < high, 2 * g * row_cap + start, d0 * row_cap + start1)
            at1 = jnp.where(g < high, (2 * g + 1) * row_cap + start, d1 * row_cap + start1)
            ids = jnp.where(lane < size, at0 + lane, at1 + lane - size).astype(F32)
            rows = rows_ref[...]
            for t in range(tok // block):
                at = slice(t * block, (t + 1) * block)
                acc[at, :] += gated(cols_ref[at, :], ids, rows)

    out_ref[...] = acc[...].astype(BF16)
    send(1).wait_send()


def _params(vmem_limit_bytes=VMEM_BYTES):
    return pltpu.CompilerParams(vmem_limit_bytes=vmem_limit_bytes)


def solution(mesh):
    n = mesh.shape["ep"]

    def body(x, w_router, ids, w1, w3, w2):
        tok, dim = x.shape
        local = w1.shape[0]
        ff = w1.shape[2]
        n_exp = n * local
        cap = 4 * tok // n
        slots, counts = pl.pallas_call(
            functools.partial(route_slots, local, cap, n_exp),
            out_shape=(jax.ShapeDtypeStruct((8, tok), I32), jax.ShapeDtypeStruct((n_exp, 128), I32)),
            compiler_params=_params(),
            name="route",
        )(ids.T)
        smem = pl.BlockSpec(memory_space=pltpu.SMEM)
        vmem = pl.BlockSpec(memory_space=pltpu.VMEM)
        hbm = pl.BlockSpec(memory_space=pl.ANY)
        ship = pl.pallas_call(
            functools.partial(ship_kernel, cap, n, CHUNKS),
            in_specs=[vmem] * 5,
            out_specs=[hbm, hbm, hbm, vmem],
            out_shape=[jax.ShapeDtypeStruct((n, size, dim), BF16) for _, size in CHUNKS]
            + [jax.ShapeDtypeStruct((n, n_exp, 128), I32), jax.ShapeDtypeStruct((tok, 8), F32)],
            scratch_shapes=[
                pltpu.VMEM((n, CHUNKS[0][1], dim), BF16),
                pltpu.VMEM((n, CHUNKS[1][1], dim), BF16),
                pltpu.SemaphoreType.DMA((n,)),
                pltpu.SemaphoreType.DMA((n,)),
                pltpu.SemaphoreType.DMA,
                pltpu.SemaphoreType.DMA((n,)),
                pltpu.SemaphoreType.DMA((n,)),
                pltpu.SemaphoreType.DMA((n,)),
                pltpu.SemaphoreType.DMA,
            ],
            compiler_params=pltpu.CompilerParams(
                vmem_limit_bytes=VMEM_BYTES, collective_id=0, has_side_effects=True
            ),
            cost_estimate=pl.CostEstimate(flops=10**11, bytes_accessed=1, transcendentals=0),
            name="ship",
        )
        first_rows, second_rows, every, cols = ship(slots, counts, ids.T, w_router.T, x)
        at = lax.axis_index("ep") * local
        per_exp = lax.dynamic_slice(every, (0, at, 0), (n, local, 1))[:, :, 0]
        ends = jnp.cumsum(per_exp, axis=1).T
        bounds = jnp.concatenate([jnp.zeros((1, n), I32), ends], axis=0)
        for index, (start, size) in enumerate(CHUNKS):
            if index == 0:
                got = first_rows
            else:
                got = lax.all_to_all(second_rows, "ep", 0, 0, tiled=True)
            rows = n * size
            made = pl.pallas_call(
                functools.partial(ffn_kernel, start, size, n),
                in_specs=[smem, hbm, hbm, hbm, hbm],
                out_specs=vmem,
                scratch_shapes=[
                    pltpu.VMEM((rows, dim), BF16),
                    pltpu.VMEM((local, dim, ff), BF16),
                    pltpu.VMEM((local, dim, ff), BF16),
                    pltpu.VMEM((local, ff, dim), BF16),
                    pltpu.VMEM((STEP, dim), BF16),
                    pltpu.VMEM((STEP, ff), BF16),
                    pltpu.SMEM((rows // TILE + GROUP,), I32),
                    pltpu.SMEM((rows // TILE + GROUP,), I32),
                    pltpu.SMEM((rows // TILE + GROUP,), I32),
                    pltpu.SMEM((local,), I32),
                    pltpu.SemaphoreType.DMA((local, 3, ff // WIDE)),
                    pltpu.SemaphoreType.DMA((4,)),
                ],
                out_shape=jax.ShapeDtypeStruct((rows, dim), BF16),
                compiler_params=_params(),
                cost_estimate=pl.CostEstimate(flops=6 * rows * dim * ff, bytes_accessed=1, transcendentals=0),
            )
            made = made(bounds, got.reshape(rows, dim), w1, w3, w2)
            if index == 0:
                back = lax.all_to_all(made.reshape(n, size, dim), "ep", 0, 0, tiled=True)
        return pl.pallas_call(
            functools.partial(bring_kernel, cap, n, CHUNKS),
            in_specs=[hbm, hbm, vmem],
            out_specs=vmem,
            out_shape=jax.ShapeDtypeStruct((tok, dim), BF16),
            scratch_shapes=[
                pltpu.VMEM((n * CHUNKS[0][1], dim), BF16),
                pltpu.VMEM((n, CHUNKS[1][1], dim), BF16),
                pltpu.VMEM((tok, dim), F32),
                pltpu.VMEM((2 * CHUNKS[0][1], dim), BF16),
                pltpu.SemaphoreType.DMA((n,)),
                pltpu.SemaphoreType.DMA((n,)),
                pltpu.SemaphoreType.DMA,
                pltpu.SemaphoreType.DMA((n // 2,)),
            ],
            compiler_params=pltpu.CompilerParams(
                vmem_limit_bytes=VMEM_BYTES, collective_id=1, has_side_effects=True
            ),
            cost_estimate=pl.CostEstimate(flops=10**11, bytes_accessed=1, transcendentals=0),
            name="bring",
        )(made.reshape(n, CHUNKS[1][1], dim), back.reshape(n * CHUNKS[0][1], dim), cols)

    return jax.shard_map(
        body,
        mesh=mesh,
        in_specs=(P("ep", None), P(None, None), P("ep", None), P("ep", None, None), P("ep", None, None), P("ep", None, None)),
        out_specs=P("ep", None),
        check_vma=False,
    )
```
